128 devices in a mesh: ga: 16 (over y, x), band: 4 (over z), pool: 2 (over core).
Axes of the slice: x: 4, y: 4, z: 4, core: 2. Of those that a mesh axis runs over, the one named last changes fastest.
Arguments:
- psi_occ: bfloat16 [512, 64, 64, 128], P(('pool', 'band'), 'ga'), parts along dimension 0, may hold values from -9 to 9
- energies: float32 [32], P(('pool', 'band')), parts along dimension 0, may hold values from -0.8 to 0.6
- k_point: float32 [6], P('pool'), parts along dimension 0, may hold values from -0.5 to 0.5, as said below
- g_mask: int32 [128, 4096], P(('pool', 'ga')), parts along dimension 0, may hold values from 0 to 1, as said below
- v_local: float32 [64, 4096], P(None, 'ga'), may hold values from 1 to 4
- dv: float32 [3, 64, 4096], P(None, None, 'ga'), may hold values from -6 to 6
Outputs:
- response: float32 [32, 3, 64, 64, 128], P(('pool', 'band'), None, 'ga'), parts along dimension 0
- residual: float32 [32, 3, 64, 64, 128], P(('pool', 'band'), None, 'ga'), parts along dimension 0
The draws below stay inside these ranges and needn't reach their ends.
There are 2 independent parts, one for each index of `pool`. The reference program is written for one: setup_inputs(seed, part) draws one part's arguments, and reference() takes and returns one part's arrays. A program takes and returns all parts, laid end to end along the dimension named above; an argument that names none is the same for every part. Nothing has to cross between parts.
Inputs may be any that keep to these rules, and one draw needn't show every extreme that they name: `k_point`: each component is a nonzero multiple of 0.25. `g_mask`: 1 exactly where the distance of (f(g1), f(g2), f(g3)) + k_point from the anchor is below 21, with f the signed frequency; so no 1 stands where |f(g2)| > 21 or |f(g3)| > 21, and in every draw some 1 stands where |f(g2)| = 21.
All inputs are finite; a program needn't handle non-finite values.
Results may differ from the reference program's by a relative error of at most 0.0044.
Values may be sent and summed in bfloat16 or wider, within the bound.
A program may use at most 128 MiB of HBM per device.

```python
import math
import jax
import jax.numpy as jnp
from jax import lax

BOX = 64
GCUT = 21
NOCC = 256
NSOLVE = 16
NPERT = 3
ITERS = 2
STRIDE = 16


def offset_steps(key):
    picks = jax.random.randint(jax.random.fold_in(key, 11), (3,), 0, 4)
    return jnp.where(picks < 2, picks - 2, picks - 1).astype(jnp.int32)


def draw_k_point(key, part):
    return offset_steps(key).astype(jnp.float32) * 0.25


def draw_g_mask(key, part):
    shifts = offset_steps(key)
    indices = jnp.arange(BOX, dtype=jnp.int32)
    signed = jnp.where(indices < BOX // 2, indices, indices - BOX)
    first = 4 * signed[:, None, None] + shifts[0]
    second = 4 * signed[None, :, None] + shifts[1]
    third = 4 * signed[None, None, :] + shifts[2]
    total = first * first + second * second + third * third
    inside = (total < 16 * GCUT * GCUT).astype(jnp.int32)
    return inside.reshape(BOX, BOX * BOX)


def shard_levels(rng, extent, split, smallest, largest):
    gain, own = 1.0, jax.random.fold_in(rng, 6)
    for position, blocks in split:
        steps = jnp.exp(jax.random.uniform(jax.random.fold_in(own, position), (blocks,), jnp.float32, smallest / len(split), largest / len(split)))
        gain = gain * jnp.repeat(steps, extent[position] // blocks).reshape([-1 if axis == position else 1 for axis in range(len(extent))])
    return gain


def centred(stream_key, shape, scale, most, pieces=(), held_as=jnp.bfloat16):
    factor_of = shard_levels(stream_key, shape, pieces, -0.22, 0.18) if pieces else 1.0
    array = jax.random.normal(stream_key, shape, jnp.float32) * scale * factor_of
    return jnp.minimum(jnp.maximum(array, -most), most).astype(held_as)


def setup_inputs(seed: int = 0, part: int = 0) -> dict:
    splits = jax.random.split(jax.random.key(seed), 7)
    part_keys = jax.random.split(jax.random.fold_in(splits[6], part), 7)
    psi_occ = centred(part_keys[0], (NOCC, BOX, BOX, 2 * BOX), 1.8, 9.0, ((0, 4), (1, 16)))
    energies = jnp.clip(-0.8 + 1.40000004 * jax.random.uniform(part_keys[1], (NSOLVE,), jnp.float32) ** shard_levels(part_keys[1], (NSOLVE,), ((0, 4),), -0.2, 0.2), -0.8, 0.6)
    k_point = draw_k_point(jax.random.fold_in(jax.random.fold_in(splits[6], part), 71), part)
    g_mask = draw_g_mask(jax.random.fold_in(jax.random.fold_in(splits[6], part), 71), part)
    v_local = jnp.clip(1.0 + 3.0 * jax.random.uniform(splits[4], (BOX, BOX * BOX), jnp.float32) ** shard_levels(splits[4], (BOX, BOX * BOX), ((1, 16),), -0.2, 0.2), 1.0, 4.0)
    dv = centred(splits[5], (NPERT, BOX, BOX * BOX), 1.0, 6.0, ((2, 16),), jnp.float32)
    return dict(psi_occ=psi_occ, energies=energies, k_point=k_point, g_mask=g_mask, v_local=v_local, dv=dv)


cell_length = 16.5
shift_weight = 8.0


def rounded(values):
    return lax.optimization_barrier(values.astype(jnp.bfloat16)).astype(jnp.float32)


def complex_form(halves):
    return halves[..., :BOX] + 1j * halves[..., BOX:]


def signed_freq():
    indices = jnp.arange(BOX, dtype=jnp.int32)
    return jnp.where(indices < BOX // 2, indices, indices - BOX).astype(jnp.float32)


def kept_indices():
    return jnp.concatenate([jnp.arange(GCUT + 1, dtype=jnp.int32), jnp.arange(BOX - GCUT, BOX, dtype=jnp.int32)]).astype(jnp.int32)


def cube_of(values):
    keep = kept_indices()
    values = jnp.take(values, keep, axis=values.ndim - 3)
    values = jnp.take(values, keep, axis=values.ndim - 2)
    return jnp.take(values, keep, axis=values.ndim - 1)


def spread_axis(values, which):
    lead = lax.slice_in_dim(values, 0, GCUT + 1, axis=which)
    tail = lax.slice_in_dim(values, GCUT + 1, 2 * GCUT + 1, axis=which)
    shape = list(values.shape)
    shape[which] = BOX - 2 * GCUT - 1
    return jnp.concatenate([lead, jnp.zeros(shape, values.dtype), tail], axis=which)


def box_of(values):
    for which in (values.ndim - 3, values.ndim - 2, values.ndim - 1):
        values = spread_axis(values, which)
    return values


def reference(psi_occ, energies, k_point, g_mask, v_local, dv):
    sphere = g_mask.reshape(BOX, BOX, BOX).astype(jnp.float32)
    occupied = complex_form(psi_occ.astype(jnp.float32)) * sphere
    occupied_cube = cube_of(occupied)
    solved = occupied[::STRIDE]
    freq = signed_freq()
    factor = 0.5 * (2.0 * math.pi / cell_length) ** 2
    kinetic = factor * ((freq[:, None, None] + k_point[0]) ** 2 + (freq[None, :, None] + k_point[1]) ** 2 + (freq[None, None, :] + k_point[2]) ** 2)
    potential = v_local.reshape(BOX, BOX, BOX)
    changes = dv.reshape(NPERT, BOX, BOX, BOX)
    grid_axes = (-3, -2, -1)

    def grid_apply(field, coeffs):
        real_space = jnp.fft.ifftn(coeffs, axes=grid_axes)
        return sphere * jnp.fft.fftn(field * real_space, axes=grid_axes)

    def project(values):
        part = cube_of(values)
        lowered = rounded(jnp.real(part)) + 1j * rounded(jnp.imag(part))
        correlation = jnp.einsum('mabc,sabc->ms', jnp.conj(occupied_cube), lowered, precision=lax.Precision.HIGHEST)
        low_correlation = rounded(jnp.real(correlation)) + 1j * rounded(jnp.imag(correlation))
        result = jnp.einsum('ms,mabc->sabc', low_correlation, occupied_cube, precision=lax.Precision.HIGHEST)
        return box_of(result) / BOX ** 3

    source = grid_apply(changes[None], solved[:, None]).reshape(NSOLVE * NPERT, BOX, BOX, BOX)
    right_side = project(source) - source
    shift = jnp.repeat(energies, NPERT)[:, None, None, None]

    def apply_operator(values):
        return (kinetic - shift) * values + grid_apply(potential, values) + shift_weight * project(values)

    def inner(first, second):
        total = jnp.real(first) * jnp.real(second) + jnp.imag(first) * jnp.imag(second)
        return jnp.sum(total, axis=(1, 2, 3)) / BOX ** 3

    response = jnp.zeros_like(right_side)
    residual = right_side
    direction = right_side
    norm_now = inner(residual, residual)
    for iteration in range(ITERS):
        image = apply_operator(direction)
        step_size = (norm_now / inner(direction, image))[:, None, None, None]
        response = response + step_size * direction
        residual = residual - step_size * image
        fresh = inner(residual, residual)
        direction = residual + (fresh / norm_now)[:, None, None, None] * direction
        norm_now = fresh

    def halves(values):
        joined = jnp.concatenate([jnp.real(values), jnp.imag(values)], axis=-1)
        return joined.reshape(NSOLVE, NPERT, BOX, BOX, 2 * BOX).astype(jnp.float32)

    return halves(response), halves(residual)
```

```python
import functools
import math

import jax
import jax.numpy as jnp
import numpy as np
from jax import lax
from jax.experimental import pallas as pl
from jax.experimental.pallas import tpu as pltpu
from jax.sharding import PartitionSpec as P

BOX = 64
GCUT = 21
KEPT = 2 * GCUT + 1
NPERT = 3
STRIDE = 16
BASE_ROW = 13
SHIFT = 16.0
ROWS = 2 * BASE_ROW + 1

cell_length = 16.5
shift_weight = 8.0

kept_freqs = list(range(GCUT + 1)) + list(range(-GCUT, 0))
place_of = {f: i for i, f in enumerate(kept_freqs)}
base_freqs = list(range(BASE_ROW + 1)) + list(range(-BASE_ROW, 0))
wide_freqs = [f for m in range(14, 19) for f in (m, -m)]
narrow_freqs = [f for m in range(19, 22) for f in (m, -m)]
WIDE = len(wide_freqs)
F32 = jnp.float32
BF16 = jnp.bfloat16


def add(a, b):
    if a is None:
        return b
    if b is None:
        return a
    return (a[0] + b[0], a[1] + b[1])


def sub(a, b):
    if b is None:
        return a
    if a is None:
        return (-b[0], -b[1])
    return (a[0] - b[0], a[1] - b[1])


def times_phase(a, turns, sign):
    if a is None:
        return None
    turns = turns % 1.0
    re, im = a
    if turns == 0.0:
        return a
    if turns == 0.5:
        return (-re, -im)
    if turns in (0.25, 0.75):
        if (turns == 0.25) == (sign > 0):
            return (-im, re)
        return (im, -re)
    c, s = math.cos(2 * math.pi * turns), sign * math.sin(2 * math.pi * turns)
    if turns in (0.125, 0.375, 0.625, 0.875):
        h = abs(c)
        if (c > 0) == (s > 0):
            pair = ((re - im) * h, (re + im) * h)
        else:
            pair = ((re + im) * h, (im - re) * h)
        return pair if c > 0 else (-pair[0], -pair[1])
    return (re * c - im * s, im * c + re * s)


def small_dft(xs, sign):
    n = len(xs)
    if n == 1:
        return xs
    even, odd = small_dft(xs[0::2], sign), small_dft(xs[1::2], sign)
    turned = [times_phase(o, k / n, sign) for k, o in enumerate(odd)]
    return [add(e, o) for e, o in zip(even, turned)] + [sub(e, o) for e, o in zip(even, turned)]


def dft64(load, keep, tmp, store, sign):
    for n2 in range(8):
        out = small_dft([load(8 * n1 + n2) for n1 in range(8)], sign)
        for k1 in range(8):
            re, im = times_phase(out[k1], n2 * k1 / 64.0, sign)
            tmp[8 * n2 + k1, 0:8] = re
            tmp[8 * n2 + k1, 8:16] = im
    for k1 in range(8):
        if not any((k1 + 8 * k2) in keep for k2 in range(8)):
            continue
        out = small_dft([(tmp[8 * n2 + k1, 0:8], tmp[8 * n2 + k1, 8:16]) for n2 in range(8)], sign)
        for k2 in range(8):
            if (k1 + 8 * k2) in keep:
                store(k1 + 8 * k2, out[k2])


def corner_turn(block):
    front = lax.broadcasted_iota(jnp.int32, (8, 2 * BOX), 1) < BOX
    top = lax.broadcasted_iota(jnp.int32, (8, 2 * BOX), 0) < 4
    half = []
    for h in range(2):
        a, b = block[2 * h], block[2 * h + 1]
        half.append(
            (
                jnp.where(front, a, pltpu.roll(b, BOX, 1)),
                jnp.where(front, pltpu.roll(a, BOX, 1), b),
            )
        )
    out = [None] * 4
    for i in range(2):
        a, b = half[0][i], half[1][i]
        out[i] = jnp.where(top, a, pltpu.roll(b, 4, 0))
        out[2 + i] = jnp.where(top, pltpu.roll(a, 4, 0), b)
    return out


def turn_in(src, rows, dst):
    for s in range(16):
        tiles = [src[4 * s + c, rows].astype(F32) for c in range(4)]
        re = corner_turn([t[0:8] for t in tiles])
        im = corner_turn([t[8:16] for t in tiles])
        for c in range(4):
            dst[4 * s + c, 0:8] = re[c]
            dst[4 * s + c, 8:16] = im[c]


def pair(ref):
    return lambda n: (ref[n, 0:8], ref[n, 8:16])


def put_pair(ref, rows, dtype):
    def store(n, value):
        ref[n, rows] = jnp.concatenate([value[0], value[1]], axis=0).astype(dtype)

    return store


def split_dot(x, high, low):
    hi = x.astype(BF16)
    lo = (x - hi.astype(F32)).astype(BF16)
    dot = functools.partial(jnp.dot, preferred_element_type=F32)
    return dot(hi, high) + dot(lo, high) + dot(hi, low)


def lanes_forward(src, first_row, high, low, dst):
    a = src[:, pl.ds(first_row, 8), :].reshape(KEPT * 8, 2 * BOX)
    b = src[:, pl.ds(first_row + 8, 8), :].reshape(KEPT * 8, 2 * BOX)
    out = split_dot(jnp.concatenate([a, b], axis=1), high, low)
    dst[0:KEPT, 0:8, :] = out[:, : 2 * BOX].reshape(KEPT, 8, 2 * BOX)
    dst[0:KEPT, 8:16, :] = out[:, 2 * BOX :].reshape(KEPT, 8, 2 * BOX)


def lanes_back(src, high, low):
    x = jnp.concatenate(
        [
            src[0:KEPT, 0:8, :].reshape(KEPT * 8, 2 * BOX),
            src[0:KEPT, 8:16, :].reshape(KEPT * 8, 2 * BOX),
        ],
        axis=1,
    )
    out = split_dot(x, high, low)
    return (
        out[:, : 2 * BOX].reshape(KEPT, 8, 2 * BOX),
        out[:, 2 * BOX :].reshape(KEPT, 8, 2 * BOX),
    )


def lane_tables():
    index = np.arange(BOX)
    angle = (index[:, None] * index[None, :] % BOX) * (2.0 * np.pi / BOX)
    c, s, z = np.cos(angle), np.sin(angle), np.zeros((BOX, BOX))
    forward = np.block([[c, z, s, z], [-s, z, c, z], [z, c, z, s], [z, -s, z, c]])
    s = -s
    back = np.block([[c, s, z, z], [z, z, c, s], [-s, c, z, z], [z, z, -s, c]])
    out = []
    for w in (forward, back):
        w = jnp.asarray(w, F32)
        high = w.astype(BF16)
        out += [high, (w - high.astype(F32)).astype(BF16)]
    return out


kept_place = lambda n: n if n <= GCUT else (n - (BOX - KEPT) if n >= BOX - GCUT else None)
KEPT_SET = frozenset(f % BOX for f in kept_freqs)
ALL_SET = frozenset(range(BOX))


def load_kept(ref):
    def load(n):
        place = kept_place(n)
        return None if place is None else (ref[place, 0:8], ref[place, 8:16])

    return load


def forward_tile(src, first_row, high, low, near, tmp, store):
    lanes_forward(src, first_row, high, low, near)
    dft64(load_kept(near), ALL_SET, tmp, store, 1)


def back_tile(src, rows, high, low, near, tmp):
    turn_in(src, rows, near)

    def store(n, value):
        tmp2 = near
        tmp2[kept_place(n), 0:8] = value[0]
        tmp2[kept_place(n), 8:16] = value[1]

    dft64(pair(near), KEPT_SET, tmp, store, -1)
    return lanes_back(near, high, low)


def front_lanes(shape):
    return lax.broadcasted_iota(jnp.int32, shape, len(shape) - 1) % BOX < BOX // 2


def pack_row(get, r):
    value = get(base_freqs[r])
    front = front_lanes(value.shape)
    axis = value.ndim - 1
    if r < WIDE:
        guest = jnp.where(front, get(wide_freqs[r]), 0.0)
        value = value + pltpu.roll(guest, GCUT + 1, axis)
    elif r < 2 * WIDE:
        guest = jnp.where(front, 0.0, get(wide_freqs[r - WIDE]))
        value = value + pltpu.roll(guest, 2 * BOX - GCUT, axis)
    elif r < 2 * WIDE + 6:
        guest = get(narrow_freqs[r - 2 * WIDE])
        value = value + pltpu.roll(jnp.where(front, guest, 0.0), BOX // 2, axis)
        value = value + pltpu.roll(jnp.where(front, 0.0, guest), 3 * BOX // 2, axis)
    return value


def unpack_row(get, f):
    if f in base_freqs:
        return get(base_freqs.index(f))
    if f in wide_freqs:
        r = wide_freqs.index(f)
        up, down = get(r), get(WIDE + r)
        axis = up.ndim - 1
        return jnp.where(
            front_lanes(up.shape),
            pltpu.roll(up, 2 * BOX - GCUT - 1, axis),
            pltpu.roll(down, GCUT, axis),
        )
    value = get(2 * WIDE + narrow_freqs.index(f))
    axis = value.ndim - 1
    return jnp.where(
        front_lanes(value.shape),
        pltpu.roll(value, 3 * BOX // 2, axis),
        pltpu.roll(value, BOX // 2, axis),
    )


def lane_sign(shape):
    return jnp.where(lax.broadcasted_iota(jnp.int32, shape, len(shape) - 1) < BOX, 1.0, -1.0)


def panel_rows(panel, r, p):
    return jnp.concatenate([panel[b, r, p] for b in range(4)], axis=0)


def correlate(values, panel, fold, packed):
    for r in range(ROWS):
        straight = pack_row(lambda f: values[place_of[f]], r)
        turned = pack_row(
            lambda f: pltpu.roll(values[place_of[f]], BOX, 1) * lane_sign((48, 2 * BOX)), r
        )
        packed[r] = jnp.concatenate([straight, turned], axis=0).astype(BF16)
    total = [None] * 4
    for r in range(0, ROWS, 2):
        both = r + 1 < ROWS
        y = jnp.concatenate([packed[r], packed[r + 1]], axis=1) if both else packed[r]
        for p in range(4):
            o = panel_rows(panel, r, p)
            if both:
                o = jnp.concatenate([o, panel_rows(panel, r + 1, p)], axis=1)
            part = lax.dot_general(o, y, (((1,), (1,)), ((), ())), preferred_element_type=F32)
            total[p] = part if total[p] is None else total[p] + part
    column = lax.broadcasted_iota(jnp.int32, (256, 96), 1) % 16 // 4
    chosen = total[0]
    for p in range(1, 4):
        chosen = jnp.where(column == 2 * (p % 2) + p // 2, total[p], chosen)
    hi = chosen.astype(BF16)
    lo = (chosen - hi.astype(F32)).astype(BF16)
    nt = (((1,), (1,)), ((), ()))
    return lax.dot_general(fold, hi, nt, preferred_element_type=F32) + lax.dot_general(
        fold, lo, nt, preferred_element_type=F32
    )


def fold_table():
    f = np.zeros((2, 3, 4, 2, 3, 4, 4), np.float32)
    for a in range(2):
        for t in range(3):
            for q in range(4):
                f[a, t, q, a, t, :, q] = 1.0
    return f.reshape(24, 96)


def spread_table():
    f = np.zeros((4, 2, 3, 2, 2, 4, 2, 3, 4), np.float32)
    for p in range(4):
        for a in range(2):
            for t in range(3):
                for q in range(4):
                    f[p, a, t, p % 2, p // 2, q, a, t, q] = 1.0
    return f.reshape(384, 24)


def combine(corr, panel, spread, product, finish):
    rows = jnp.dot(spread[...], corr, preferred_element_type=F32).astype(BF16)
    sign = -lane_sign((48, 2 * BOX))
    for r in range(0, ROWS, 2):
        both = r + 1 < ROWS
        total = None
        for p in range(4):
            o = panel_rows(panel, r, p)
            if both:
                o = jnp.concatenate([o, panel_rows(panel, r + 1, p)], axis=1)
            part = jnp.dot(rows[96 * p : 96 * p + 96], o, preferred_element_type=F32)
            total = part if total is None else total + part
        for c in range(2 if both else 1):
            lanes = slice(2 * BOX * c, 2 * BOX * (c + 1))
            product[r + c] = (
                total[:48, lanes] + pltpu.roll(total[48:, lanes], BOX, 1) * sign
            )
    for f in kept_freqs:
        finish(place_of[f], unpack_row(lambda r: product[r], f))


VMEM_LIMIT = 60 * 1024 * 1024
vmem = pl.BlockSpec(memory_space=pltpu.VMEM)
TILE = pltpu.VMEM((BOX, 16, 2 * BOX), F32)


def call(body, outs, args, scratch=(), flops=10**9):
    return pl.pallas_call(
        body,
        out_shape=outs,
        in_specs=[vmem] * len(args),
        out_specs=jax.tree.map(lambda _: vmem, outs),
        scratch_shapes=list(scratch),
        compiler_params=pltpu.CompilerParams(vmem_limit_bytes=VMEM_LIMIT),
        cost_estimate=pl.CostEstimate(flops=flops, bytes_accessed=4 * 10**6, transcendentals=0),
    )(*args)


def shape(dims, dtype=F32):
    return jax.ShapeDtypeStruct(dims, dtype)


def pack_body(psi, mask, out):
    for r in range(ROWS):
        get = lambda f: psi[0, f % BOX].astype(F32) * mask[0, f % BOX]
        out[r, 0] = pack_row(get, r).astype(BF16)


def pack_panel(psi, mask):
    bands = psi.shape[2]
    return pl.pallas_call(
        pack_body,
        grid=(4,),
        out_shape=shape((ROWS, 4, bands, 2 * BOX), BF16),
        in_specs=[
            pl.BlockSpec((1, BOX, bands, 2 * BOX), lambda p: (p, 0, 0, 0)),
            pl.BlockSpec((1, BOX, 1, 2 * BOX), lambda p: (p, 0, 0, 0)),
        ],
        out_specs=pl.BlockSpec((ROWS, 1, bands, 2 * BOX), lambda p: (0, p, 0, 0)),
    )(psi, mask)


def source_forward_body(solved, high, low, out, near, tmp):
    forward_tile(solved, 0, high[...], low[...], near, tmp, put_pair(out, slice(0, 16), F32))


def source_middle_body(came, changes, out, near, tmp, space):
    turn_in(came, slice(0, 16), near)

    def keep(n, value):
        space[n, 0:8] = value[0]
        space[n, 8:16] = value[1]

    dft64(pair(near), ALL_SET, tmp, keep, 1)

    def each(p, carry):
        def load(n):
            d = changes[p, n]
            return (space[n, 0:8] * d, space[n, 8:16] * d)

        rows = pl.ds(pl.multiple_of(16 * p, 16), 16)
        dft64(load, ALL_SET, tmp, put_pair(out, rows, F32), -1)
        return carry

    lax.fori_loop(0, NPERT, each, 0)


def back_body(came, high, low, mask, out, near, tmp):
    def each(t, carry):
        start = pl.multiple_of(16 * t, 16)
        a, b = back_tile(came, pl.ds(start, 16), high[...], low[...], near, tmp)
        out[:, pl.ds(start, 8), :] = a * mask[:, 0:8, :]
        out[:, pl.ds(start + 8, 8), :] = b * mask[:, 8:16, :]
        return carry

    lax.fori_loop(0, 3, each, 0)


def forward_body(values, high, low, out, near, tmp):
    def each(t, carry):
        start = pl.multiple_of(16 * t, 16)
        forward_tile(values, start, high[...], low[...], near, tmp, put_pair(out, pl.ds(start, 16), BF16))
        return carry

    lax.fori_loop(0, 3, each, 0)


def middle_body(came, potential, out, near, tmp):
    def each(t, carry):
        rows = pl.ds(pl.multiple_of(16 * t, 16), 16)
        turn_in(came, rows, near)

        def keep(n, value):
            v = potential[n]
            near[n, 0:8] = value[0] * v
            near[n, 8:16] = value[1] * v

        dft64(pair(near), ALL_SET, tmp, keep, 1)
        dft64(pair(near), ALL_SET, tmp, put_pair(out, rows, BF16), -1)
        return carry

    lax.fori_loop(0, 3, each, 0)


def correlate_body(values, panel, fold, out, packed):
    out[...] = correlate(values, panel, fold[...], packed).astype(BF16)


def combine_body(shares, panel, spread, mask, out, product):
    total = shares[0].astype(F32)
    for s in range(1, 16):
        total = total + shares[s].astype(F32)

    def finish(place, row):
        for t in range(3):
            out[place, 16 * t : 16 * t + 16] = row[16 * t : 16 * t + 16] * mask[place]

    combine(total.astype(BF16), panel, spread, product, finish)


def copy_for_each(shard, axis):
    size = lax.axis_size(axis)
    return lax.all_to_all(
        jnp.broadcast_to(shard[None], (size, *shard.shape)), axis, 0, 0, tiled=True
    )


def swap(values):
    return lax.all_to_all(values, "ga", split_axis=0, concat_axis=0, tiled=True)


def rows_of_planes(values):
    values = values.reshape(2, 2, BOX, 2 * BOX).transpose(2, 1, 0, 3).reshape(BOX, 4, 2 * BOX)
    return jnp.concatenate([values[: GCUT + 1], values[BOX - GCUT :]], axis=0)


def on_device(psi_occ, energies, k_point, g_mask, v_local, dv):
    planes = psi_occ.shape[1]
    ga_index = lax.axis_index("ga")
    indices = jnp.arange(BOX, dtype=jnp.int32)
    signed = jnp.where(indices < BOX // 2, indices, indices - BOX).astype(F32)
    owned = ga_index * planes + jnp.arange(planes, dtype=jnp.int32)
    freq_first = jnp.where(owned < BOX // 2, owned, owned - BOX).astype(F32)
    factor = 0.5 * (2.0 * math.pi / cell_length) ** 2
    kinetic = factor * (
        (freq_first[:, None, None] + k_point[0]) ** 2
        + (signed[None, :, None] + k_point[1]) ** 2
        + (signed[None, None, :] + k_point[2]) ** 2
    )
    kinetic = jnp.concatenate([kinetic, kinetic], axis=-1)
    sphere = g_mask.reshape(planes, BOX, BOX).astype(F32)
    sphere = jnp.concatenate([sphere, sphere], axis=-1)
    tables = lane_tables()
    fold = jnp.asarray(fold_table(), BF16)
    spread = jnp.asarray(spread_table(), BF16)

    packed = pack_panel(psi_occ.transpose(1, 2, 0, 3), sphere[:, :, None, :])
    panel = lax.all_gather(packed, "band", axis=0, tiled=False)

    mask4 = rows_of_planes(sphere)
    mask = jnp.repeat(mask4, 4, axis=1)
    level = (rows_of_planes(kinetic)[:, :, None, :] - energies[None, None, :, None]).reshape(
        KEPT, 16, 2 * BOX
    ) * mask
    mask_scaled = mask / BOX**3
    solved = psi_occ[::STRIDE].astype(F32) * sphere[None]
    solved = solved.reshape(4, 2, 2, BOX, 2 * BOX).transpose(3, 2, 1, 0, 4).reshape(BOX, 16, 2 * BOX)
    solved = jnp.concatenate([solved[: GCUT + 1], solved[BOX - GCUT :]], axis=0)
    potential = jnp.repeat(v_local.reshape(BOX, 2, 2 * BOX), 4, axis=1)
    changes = jnp.repeat(dv.reshape(NPERT, BOX, 2, 2 * BOX), 4, axis=2)

    grid_bf = shape((BOX, 48, 2 * BOX), BF16)
    grid_f = shape((BOX, 48, 2 * BOX), F32)
    natural = shape((KEPT, 48, 2 * BOX))

    def project(values):
        share = call(
            correlate_body, shape((24, 256), BF16), (values, panel, fold),
            [pltpu.VMEM((ROWS, 96, 2 * BOX), BF16)],
        )
        return call(
            combine_body, natural, (copy_for_each(share, "ga"), panel, spread, mask_scaled),
            [pltpu.VMEM((ROWS, 48, 2 * BOX), F32)],
        )

    def grid_potential(values):
        sent = call(forward_body, grid_bf, (values, tables[0], tables[1]), [TILE, TILE])
        sent = call(middle_body, grid_bf, (swap(sent), potential), [TILE, TILE])
        return call(back_body, natural, (swap(sent), tables[2], tables[3], mask_scaled), [TILE, TILE])

    sent = call(source_forward_body, shape((BOX, 16, 2 * BOX)), (solved, tables[0], tables[1]), [TILE, TILE])
    sent = call(source_middle_body, grid_f, (swap(sent), changes), [TILE, TILE, TILE])
    source = call(back_body, natural, (swap(sent), tables[2], tables[3], mask_scaled), [TILE, TILE])

    def by_tile(values):
        return values.reshape(KEPT, 3, 16, 2 * BOX)

    def apply(values):
        local = grid_potential(values)
        return (
            (by_tile(values) * level[:, None]).reshape(values.shape)
            + local
            + shift_weight * project(values)
        )

    def inner(a, b):
        total = jnp.sum(a * b, axis=(0, 2)).reshape(3, 4, 4)
        return jnp.sum(total, axis=1) / BOX**3

    first = project(source) - source
    image = apply(first)
    second = image - SHIFT * first
    other = apply(second)
    sums = jnp.stack([inner(first, first), inner(first, image), inner(image, image), inner(second, other)])
    m0, m1, m2, m3 = jnp.sum(copy_for_each(sums, "ga"), axis=0)
    step0 = m0 / m1
    fresh = m0 - 2.0 * step0 * m1 + step0 * step0 * m2
    u = 1.0 + fresh / m0 - step0 * SHIFT
    curve = u * u * m1 - 2.0 * u * step0 * (m2 - SHIFT * m1) + step0 * step0 * m3
    step1 = fresh / curve

    def each(v):
        return jnp.repeat(v[:, None, :], 4, axis=1).reshape(48)[None, :, None]

    response = each(step0 + step1 * u) * first - each(step1 * step0) * second
    residual = first - each(step0 + step1 * u) * image + each(step1 * step0) * other

    def placed(values):
        values = values.reshape(KEPT, 3, 2, 2, 4, 2 * BOX).transpose(4, 1, 3, 2, 0, 5)
        values = values.reshape(4, NPERT, 4, KEPT, 2 * BOX)
        gap = jnp.zeros((4, NPERT, 4, BOX - KEPT, 2 * BOX), F32)
        return jnp.concatenate([values[..., : GCUT + 1, :], gap, values[..., GCUT + 1 :, :]], axis=3)

    return placed(response), placed(residual)


def solution(mesh):
    placed = (
        P(("pool", "band"), "ga", None, None),
        P(("pool", "band")),
        P("pool"),
        P(("pool", "ga"), None),
        P(None, "ga"),
        P(None, None, "ga"),
    )
    return jax.shard_map(
        on_device,
        mesh=mesh,
        in_specs=placed,
        out_specs=(
            P(("pool", "band"), None, "ga", None, None),
            P(("pool", "band"), None, "ga", None, None),
        ),
        check_vma=False,
    )
```

```python
import functools
import math

import jax
import jax.numpy as jnp
import numpy as np
from jax import lax
from jax.experimental import pallas as pl
from jax.experimental.pallas import tpu as pltpu
from jax.sharding import PartitionSpec as P

BOX = 64
GCUT = 21
KEPT = 2 * GCUT + 1
NPERT = 3
STRIDE = 16
BASE_ROW = 13
SHIFT = 16.0
ROWS = 2 * BASE_ROW + 1

cell_length = 16.5
shift_weight = 8.0

kept_freqs = list(range(GCUT + 1)) + list(range(-GCUT, 0))
place_of = {f: i for i, f in enumerate(kept_freqs)}
base_freqs = list(range(BASE_ROW + 1)) + list(range(-BASE_ROW, 0))
wide_freqs = [f for m in range(14, 19) for f in (m, -m)]
narrow_freqs = [f for m in range(19, 22) for f in (m, -m)]
WIDE = len(wide_freqs)
F32 = jnp.float32
BF16 = jnp.bfloat16


def add(a, b):
    if a is None:
        return b
    if b is None:
        return a
    return (a[0] + b[0], a[1] + b[1])


def sub(a, b):
    if b is None:
        return a
    if a is None:
        return (-b[0], -b[1])
    return (a[0] - b[0], a[1] - b[1])


def times_phase(a, turns, sign):
    if a is None:
        return None
    turns = turns % 1.0
    re, im = a
    if turns == 0.0:
        return a
    if turns == 0.5:
        return (-re, -im)
    if turns in (0.25, 0.75):
        if (turns == 0.25) == (sign > 0):
            return (-im, re)
        return (im, -re)
    c, s = math.cos(2 * math.pi * turns), sign * math.sin(2 * math.pi * turns)
    if turns in (0.125, 0.375, 0.625, 0.875):
        h = abs(c)
        if (c > 0) == (s > 0):
            pair = ((re - im) * h, (re + im) * h)
        else:
            pair = ((re + im) * h, (im - re) * h)
        return pair if c > 0 else (-pair[0], -pair[1])
    return (re * c - im * s, im * c + re * s)


def small_dft(xs, sign):
    n = len(xs)
    if n == 1:
        return xs
    even, odd = small_dft(xs[0::2], sign), small_dft(xs[1::2], sign)
    turned = [times_phase(o, k / n, sign) for k, o in enumerate(odd)]
    return [add(e, o) for e, o in zip(even, turned)] + [sub(e, o) for e, o in zip(even, turned)]


def dft64(load, keep, tmp, store, sign):
    for n2 in range(8):
        out = small_dft([load(8 * n1 + n2) for n1 in range(8)], sign)
        for k1 in range(8):
            re, im = times_phase(out[k1], n2 * k1 / 64.0, sign)
            tmp[8 * n2 + k1, 0:8] = re
            tmp[8 * n2 + k1, 8:16] = im
    for k1 in range(8):
        if not any((k1 + 8 * k2) in keep for k2 in range(8)):
            continue
        out = small_dft([(tmp[8 * n2 + k1, 0:8], tmp[8 * n2 + k1, 8:16]) for n2 in range(8)], sign)
        for k2 in range(8):
            if (k1 + 8 * k2) in keep:
                store(k1 + 8 * k2, out[k2])


def corner_turn(block):
    front = lax.broadcasted_iota(jnp.int32, (8, 2 * BOX), 1) < BOX
    top = lax.broadcasted_iota(jnp.int32, (8, 2 * BOX), 0) < 4
    half = []
    for h in range(2):
        a, b = block[2 * h], block[2 * h + 1]
        half.append(
            (
                jnp.where(front, a, pltpu.roll(b, BOX, 1)),
                jnp.where(front, pltpu.roll(a, BOX, 1), b),
            )
        )
    out = [None] * 4
    for i in range(2):
        a, b = half[0][i], half[1][i]
        out[i] = jnp.where(top, a, pltpu.roll(b, 4, 0))
        out[2 + i] = jnp.where(top, pltpu.roll(a, 4, 0), b)
    return out


def turn_in(src, dst):
    for s in range(16):
        tiles = [src[4 * s + c].astype(F32) for c in range(4)]
        re = corner_turn([t[0:8] for t in tiles])
        im = corner_turn([t[8:16] for t in tiles])
        for c in range(4):
            dst[4 * s + c, 0:8] = re[c]
            dst[4 * s + c, 8:16] = im[c]


def pair(ref):
    return lambda n: (ref[n, 0:8], ref[n, 8:16])


def put_pair(ref, rows, dtype):
    def store(n, value):
        ref[n, rows] = jnp.concatenate([value[0], value[1]], axis=0).astype(dtype)

    return store


def split_dot(x, high, low):
    hi = x.astype(BF16)
    lo = (x - hi.astype(F32)).astype(BF16)
    dot = functools.partial(jnp.dot, preferred_element_type=F32)
    return dot(hi, high) + dot(lo, high) + dot(hi, low)


def lanes_forward(src, first_row, high, low, dst):
    a = src[:, pl.ds(first_row, 8), :].reshape(KEPT * 8, 2 * BOX)
    b = src[:, pl.ds(first_row + 8, 8), :].reshape(KEPT * 8, 2 * BOX)
    out = split_dot(jnp.concatenate([a, b], axis=1), high, low)
    dst[0:KEPT, 0:8, :] = out[:, : 2 * BOX].reshape(KEPT, 8, 2 * BOX)
    dst[0:KEPT, 8:16, :] = out[:, 2 * BOX :].reshape(KEPT, 8, 2 * BOX)


def lanes_back(src, high, low):
    x = jnp.concatenate(
        [
            src[0:KEPT, 0:8, :].reshape(KEPT * 8, 2 * BOX),
            src[0:KEPT, 8:16, :].reshape(KEPT * 8, 2 * BOX),
        ],
        axis=1,
    )
    out = split_dot(x, high, low)
    return (
        out[:, : 2 * BOX].reshape(KEPT, 8, 2 * BOX),
        out[:, 2 * BOX :].reshape(KEPT, 8, 2 * BOX),
    )


def lane_tables():
    index = np.arange(BOX)
    angle = (index[:, None] * index[None, :] % BOX) * (2.0 * np.pi / BOX)
    c, s, z = np.cos(angle), np.sin(angle), np.zeros((BOX, BOX))
    forward = np.block([[c, z, s, z], [-s, z, c, z], [z, c, z, s], [z, -s, z, c]])
    s = -s
    back = np.block([[c, s, z, z], [z, z, c, s], [-s, c, z, z], [z, z, -s, c]])
    out = []
    for w in (forward, back):
        w = jnp.asarray(w, F32)
        high = w.astype(BF16)
        out += [high, (w - high.astype(F32)).astype(BF16)]
    return out


kept_place = lambda n: n if n <= GCUT else (n - (BOX - KEPT) if n >= BOX - GCUT else None)
KEPT_SET = frozenset(f % BOX for f in kept_freqs)
ALL_SET = frozenset(range(BOX))


def load_kept(ref):
    def load(n):
        place = kept_place(n)
        return None if place is None else (ref[place, 0:8], ref[place, 8:16])

    return load


def forward_tile(src, first_row, high, low, near, tmp, store):
    lanes_forward(src, first_row, high, low, near)
    dft64(load_kept(near), ALL_SET, tmp, store, 1)


def back_tile(src, high, low, near, tmp):
    turn_in(src, near)

    def store(n, value):
        tmp2 = near
        tmp2[kept_place(n), 0:8] = value[0]
        tmp2[kept_place(n), 8:16] = value[1]

    dft64(pair(near), KEPT_SET, tmp, store, -1)
    return lanes_back(near, high, low)


def front_lanes(shape):
    return lax.broadcasted_iota(jnp.int32, shape, len(shape) - 1) % BOX < BOX // 2


def pack_row(get, r):
    value = get(base_freqs[r])
    front = front_lanes(value.shape)
    axis = value.ndim - 1
    if r < WIDE:
        guest = jnp.where(front, get(wide_freqs[r]), 0.0)
        value = value + pltpu.roll(guest, GCUT + 1, axis)
    elif r < 2 * WIDE:
        guest = jnp.where(front, 0.0, get(wide_freqs[r - WIDE]))
        value = value + pltpu.roll(guest, 2 * BOX - GCUT, axis)
    elif r < 2 * WIDE + 6:
        guest = get(narrow_freqs[r - 2 * WIDE])
        value = value + pltpu.roll(jnp.where(front, guest, 0.0), BOX // 2, axis)
        value = value + pltpu.roll(jnp.where(front, 0.0, guest), 3 * BOX // 2, axis)
    return value


def unpack_row(get, f):
    if f in base_freqs:
        return get(base_freqs.index(f))
    if f in wide_freqs:
        r = wide_freqs.index(f)
        up, down = get(r), get(WIDE + r)
        axis = up.ndim - 1
        return jnp.where(
            front_lanes(up.shape),
            pltpu.roll(up, 2 * BOX - GCUT - 1, axis),
            pltpu.roll(down, GCUT, axis),
        )
    value = get(2 * WIDE + narrow_freqs.index(f))
    axis = value.ndim - 1
    return jnp.where(
        front_lanes(value.shape),
        pltpu.roll(value, 3 * BOX // 2, axis),
        pltpu.roll(value, BOX // 2, axis),
    )


def lane_sign(shape):
    return jnp.where(lax.broadcasted_iota(jnp.int32, shape, len(shape) - 1) < BOX, 1.0, -1.0)


def panel_rows(panel, slots, r, p, both):
    rows = [jnp.concatenate([panel[d, p, r] for d in slots], axis=0)]
    if both:
        rows.append(jnp.concatenate([panel[d, p, r + 1] for d in slots], axis=0))
    return jnp.concatenate(rows, axis=1)


def pack_values(values, packed):
    sign = lane_sign((48, 2 * BOX))
    for r in range(ROWS):
        straight = pack_row(lambda f: values[place_of[f]], r)
        turned = pack_row(lambda f: pltpu.roll(values[place_of[f]], BOX, 1) * sign, r)
        packed[r] = jnp.concatenate([straight, turned], axis=0).astype(BF16)


def correlate(packed, panel, fold, slots):
    count = 64 * len(slots)
    nt = (((1,), (1,)), ((), ()))
    total = [None] * 4
    for r in range(0, ROWS, 2):
        both = r + 1 < ROWS
        y = jnp.concatenate([packed[r], packed[r + 1]], axis=1) if both else packed[r]
        for p in range(4):
            o = panel_rows(panel, slots, r, p, both)
            part = lax.dot_general(o, y, nt, preferred_element_type=F32)
            total[p] = part if total[p] is None else total[p] + part
    column = lax.broadcasted_iota(jnp.int32, (count, 96), 1) % 16 // 4
    chosen = total[0]
    for p in range(1, 4):
        chosen = jnp.where(column == 2 * (p % 2) + p // 2, total[p], chosen)
    hi = chosen.astype(BF16)
    lo = (chosen - hi.astype(F32)).astype(BF16)
    return lax.dot_general(fold, hi, nt, preferred_element_type=F32) + lax.dot_general(
        fold, lo, nt, preferred_element_type=F32
    )


def fold_table():
    f = np.zeros((2, 3, 4, 2, 3, 4, 4), np.float32)
    for a in range(2):
        for t in range(3):
            for q in range(4):
                f[a, t, q, a, t, :, q] = 1.0
    return f.reshape(24, 96)


def spread_table():
    f = np.zeros((4, 2, 3, 2, 2, 4, 2, 3, 4), np.float32)
    for p in range(4):
        for a in range(2):
            for t in range(3):
                for q in range(4):
                    f[p, a, t, p % 2, p // 2, q, a, t, q] = 1.0
    return f.reshape(384, 24)


def combine(corr, panel, spread, product, finish):
    rows = jnp.dot(spread[...], corr, preferred_element_type=F32).astype(BF16)
    sign = -lane_sign((48, 2 * BOX))
    for r in range(0, ROWS, 2):
        both = r + 1 < ROWS
        total = None
        for p in range(4):
            o = panel_rows(panel, SLOTS, r, p, both)
            part = jnp.dot(rows[96 * p : 96 * p + 96], o, preferred_element_type=F32)
            total = part if total is None else total + part
        for c in range(2 if both else 1):
            lanes = slice(2 * BOX * c, 2 * BOX * (c + 1))
            product[r + c] = (
                total[:48, lanes] + pltpu.roll(total[48:, lanes], BOX, 1) * sign
            )
    for f in kept_freqs:
        finish(place_of[f], unpack_row(lambda r: product[r], f))


VMEM_LIMIT = 62 * 1024 * 1024
MESH = pl.DeviceIdType.MESH
vmem = pl.BlockSpec(memory_space=pltpu.VMEM)
STEP = 72
SLOTS = (0, 1, 3, 2)


def shape(dims, dtype=F32):
    return jax.ShapeDtypeStruct(dims, dtype)


def remote(src, dst, send, recv, where):
    return pltpu.make_async_remote_copy(
        src_ref=src, dst_ref=dst, send_sem=send, recv_sem=recv, device_id=where, device_id_type=MESH
    )


def to_peers(me, src_of, dst, send, recv):
    def one(k, carry):
        g = lax.rem(me + k, 16)
        remote(src_of(g), dst, send, recv, {"ga": g}).start()
        return carry

    lax.fori_loop(1, 16, one, 0)


def kernel(
    psi, mask_rows, solved, fwd_hi, fwd_lo, back_hi, back_lo, changes, potential, mask, level,
    fold, spread,
    response, residual,
    raw, wide_rows, panel, near, tmp, space, send_a, came_a, send_b, came_b, send_1, send_2,
    came_1, came_2, packed, product, share, shares, source, vec, image, sums, all_sums,
    raw_sem, ring_send, ring_recv, a_sem, b_send, b_recv, s1, r1, s2, r2, c_send, c_recv, m_sem,
):
    me = lax.axis_index("ga")
    z = lax.axis_index("band")
    up, down = lax.rem(z + 1, 4), lax.rem(z + 3, 4)

    barrier = pltpu.get_barrier_semaphore()

    def greet(k, carry):
        pl.semaphore_signal(
            barrier, inc=1, device_id={"ga": lax.rem(me + k, 16)}, device_id_type=MESH
        )
        return carry

    lax.fori_loop(1, 16, greet, 0)
    for other in (up, down):
        pl.semaphore_signal(barrier, inc=1, device_id={"band": other}, device_id_type=MESH)

    def raw_copy(p):
        return pltpu.make_async_copy(psi.at[:, p], raw.at[p], raw_sem.at[p])

    for p in range(4):
        raw_copy(p).start()

    forward_tile(solved, 0, fwd_hi[...], fwd_lo[...], near, tmp, put_pair(send_a, slice(0, 16), F32))
    pl.semaphore_wait(barrier, 17)

    mine = pl.ds(4 * me, 4)
    to_peers(me, lambda g: send_a.at[pl.ds(4 * g, 4)], came_a.at[mine], a_sem.at[0], a_sem.at[1])
    came_a[mine] = send_a[mine]

    def ring(src_slot, dst_slot, p, where, n):
        return remote(
            panel.at[src_slot, p], panel.at[dst_slot, p], ring_send.at[n], ring_recv.at[dst_slot, p],
            {"band": where},
        )

    def ring_up(p):
        return ring(0, 3, p, up, p)

    def ring_down(p):
        return ring(0, 1, p, down, 4 + p)

    def pack_plane(u, carry):
        p = 2 * lax.rem(u, 2) + u // 2
        raw_copy(p).wait()

        def widen(m, c):
            wide_rows[pl.ds(pl.multiple_of(STEP * m, 8), BOX), :] = raw[p, m].astype(F32)
            return c

        lax.fori_loop(0, 64, widen, 0)

        def get(f):
            n = f % BOX
            return wide_rows[pl.ds(n, 64, stride=STEP), :] * mask_rows[p, n : n + 1]

        for r in range(ROWS):
            panel[0, p, r] = pack_row(get, r).astype(BF16)

        @pl.when(lax.rem(u, 2) == 0)
        def _():
            ring_up(p).start()

        @pl.when(lax.rem(u, 2) == 1)
        def _():
            ring_down(p).start()

        return carry

    lax.fori_loop(0, 4, pack_plane, 0)
    ring_up(2).start()
    ring_down(0).start()
    ring_up(3).start()
    ring_down(1).start()

    def wait_all(src, dst, send, recv):
        return remote(src, dst, send, recv, {"ga": lax.rem(me + 1, 16)})

    every = pl.ds(0, 60)
    wait_all(send_a.at[every], came_a.at[every], a_sem.at[0], a_sem.at[1]).wait()

    turn_in(came_a, near)

    def keep(n, value):
        space[n, 0:8] = value[0]
        space[n, 8:16] = value[1]

    dft64(pair(near), ALL_SET, tmp, keep, 1)

    def each_change(p, carry):
        def load(n):
            d = changes[p, n]
            return (space[n, 0:8] * d, space[n, 8:16] * d)

        dft64(load, ALL_SET, tmp, put_pair(send_b.at[p], slice(0, 16), F32), -1)
        to_peers(
            me, lambda g: send_b.at[p, pl.ds(4 * g, 4)], came_b.at[p, mine], b_send.at[p], b_recv.at[p]
        )
        came_b[p, mine] = send_b[p, mine]
        return carry

    lax.fori_loop(0, NPERT, each_change, 0)

    def pass_on(p_up, p_down):
        ring(0, 3, p_up, up, p_up).wait_recv()
        first = ring(3, 2, p_up, up, 8 + p_up)
        first.start()
        ring(0, 1, p_down, down, 4 + p_down).wait_recv()
        second = ring(1, 2, p_down, down, 8 + p_down)
        second.start()

    pass_on(0, 2)
    pass_on(1, 3)

    def back(came, dst_add):
        def each(t, carry):
            dst_add(t)
            return carry

        lax.fori_loop(0, 3, each, 0)

    def source_tile(t):
        wait_all(send_b.at[t, every], came_b.at[t, every], b_send.at[t], b_recv.at[t]).wait()
        start = pl.multiple_of(16 * t, 16)
        a, b = back_tile(came_b.at[t], back_hi[...], back_lo[...], near, tmp)
        source[:, pl.ds(start, 8), :] = a * mask[:, 0:8, :]
        source[:, pl.ds(start + 8, 8), :] = b * mask[:, 8:16, :]

    back(came_b, source_tile)

    def send_share(n, src):
        to_peers(me, lambda g: src, shares.at[n, me], c_send.at[n], c_recv.at[n])

    def total_share(n):
        first = pl.ds(0, 15)
        wait_all(shares.at[n, first], shares.at[n, first], c_send.at[n], c_recv.at[n]).wait()
        total = shares[n, 0].astype(F32)
        for g in range(1, 16):
            total = total + shares[n, g].astype(F32)
        return total.astype(BF16)

    pack_values(source, packed)
    for p in range(2, 4):
        ring(0, 3, p, up, p).wait_recv()
    for p in range(2):
        ring(0, 1, p, down, 4 + p).wait_recv()
    early = correlate(packed, panel, fold[...], SLOTS[:3])
    for p in range(2):
        ring(3, 2, p, up, 8 + p).wait_recv()
    for p in range(2, 4):
        ring(1, 2, p, down, 8 + p).wait_recv()
    late = correlate(packed, panel, fold[...], SLOTS[3:])
    share[0] = jnp.concatenate([early, late], axis=1).astype(BF16)
    shares[0, me] = share[0]
    send_share(0, share.at[0])

    def first_row(place, row):
        for t in range(3):
            rows = slice(16 * t, 16 * t + 16)
            vec[0, place, rows] = row[rows] * mask[place] - source[place, rows]

    combine(total_share(0), panel, spread, product, first_row)

    def apply(it, carry):
        def near_tile(t, c):
            start = pl.multiple_of(16 * t, 16)
            forward_tile(
                vec.at[it], start, fwd_hi[...], fwd_lo[...], near, tmp,
                put_pair(send_1.at[it, t], slice(0, 16), BF16),
            )
            to_peers(
                me, lambda g: send_1.at[it, t, pl.ds(4 * g, 4)], came_1.at[it, t, mine],
                s1.at[it, t], r1.at[it, t],
            )
            came_1[it, t, mine] = send_1[it, t, mine]
            return c

        lax.fori_loop(0, 3, near_tile, 0)

        pack_values(vec.at[it], packed)
        n = it + 1
        share[n] = correlate(packed, panel, fold[...], SLOTS).astype(BF16)
        shares[n, me] = share[n]
        send_share(n, share.at[n])

        def space_tile(t, c):
            wait_all(send_1.at[it, t, every], came_1.at[it, t, every], s1.at[it, t], r1.at[it, t]).wait()
            turn_in(came_1.at[it, t], near)

            def with_potential(k, value):
                v = potential[k]
                near[k, 0:8] = value[0] * v
                near[k, 8:16] = value[1] * v

            dft64(pair(near), ALL_SET, tmp, with_potential, 1)
            dft64(pair(near), ALL_SET, tmp, put_pair(send_2.at[it, t], slice(0, 16), BF16), -1)
            to_peers(
                me, lambda g: send_2.at[it, t, pl.ds(4 * g, 4)], came_2.at[it, t, mine],
                s2.at[it, t], r2.at[it, t],
            )
            came_2[it, t, mine] = send_2[it, t, mine]
            return c

        lax.fori_loop(0, 3, space_tile, 0)

        def with_level(place, row):
            for t in range(3):
                rows = slice(16 * t, 16 * t + 16)
                image[it, place, rows] = (
                    row[rows] * (shift_weight * mask[place])
                    + level[place] * vec[it, place, rows]
                )

        combine(total_share(n), panel, spread, product, with_level)

        def far_tile(t, c):
            wait_all(send_2.at[it, t, every], came_2.at[it, t, every], s2.at[it, t], r2.at[it, t]).wait()
            start = pl.multiple_of(16 * t, 16)
            a, b = back_tile(came_2.at[it, t], back_hi[...], back_lo[...], near, tmp)
            for half, value in ((0, a), (8, b)):
                rows = pl.ds(start + half, 8)
                total = image[it, :, rows, :] + value * mask[:, half : half + 8, :]
                image[it, :, rows, :] = total
                vec[it + 1, :, rows, :] = total - SHIFT * vec[it, :, rows, :]
            return c

        lax.fori_loop(0, 3, far_tile, 0)
        return carry

    lax.fori_loop(0, 2, apply, 0)

    def moments(place, totals):
        b, ab, w, aw = vec[0, place], image[0, place], vec[1, place], image[1, place]
        return tuple(x + y for x, y in zip(totals, (b * b, b * ab, ab * ab, w * aw)))

    zero = jnp.zeros((48, 2 * BOX), F32)
    totals = lax.fori_loop(0, KEPT, moments, (zero,) * 4)
    lane = lax.broadcasted_iota(jnp.int32, (8, 2 * BOX), 1)
    own = jnp.zeros((8, 2 * BOX), F32)
    for m, total in enumerate(totals):
        line = jnp.sum(total, axis=1, keepdims=True) / BOX**3
        for t in range(3):
            both = line[16 * t : 16 * t + 8] + line[16 * t + 8 : 16 * t + 16]
            own = jnp.where(lane == 4 * t + m, jnp.broadcast_to(both, own.shape), own)
    own = own + pltpu.roll(own, 4, 0)
    sums[...] = own
    all_sums[me] = own
    to_peers(me, lambda g: sums, all_sums.at[me], m_sem.at[0], m_sem.at[1])
    first = pl.ds(0, 15)
    wait_all(all_sums.at[first], all_sums.at[first], m_sem.at[0], m_sem.at[1]).wait()
    m0 = all_sums[0]
    for g in range(1, 16):
        m0 = m0 + all_sums[g]
    m1, m2, m3 = (pltpu.roll(m0, 2 * BOX - n, 1) for n in (1, 2, 3))
    step0 = m0 / m1
    fresh = m0 - 2.0 * step0 * m1 + step0 * step0 * m2
    u = 1.0 + fresh / m0 - step0 * SHIFT
    curve = u * u * m1 - 2.0 * u * step0 * (m2 - SHIFT * m1) + step0 * step0 * m3
    step1 = fresh / curve
    low_part, high_part = step0 + step1 * u, step1 * step0
    for t in range(3):
        a = jnp.broadcast_to(low_part[:, 4 * t : 4 * t + 1], (8, 2 * BOX))
        e = jnp.broadcast_to(high_part[:, 4 * t : 4 * t + 1], (8, 2 * BOX))
        for half in (0, 8):
            rows = slice(16 * t + half, 16 * t + half + 8)
            b, ab = vec[0, :, rows, :], image[0, :, rows, :]
            response[:, rows, :] = a * b - e * vec[1, :, rows, :]
            residual[:, rows, :] = b - a * ab + e * image[1, :, rows, :]

    for p in range(4):
        ring_up(p).wait_send()
        ring_down(p).wait_send()
    for p in range(2):
        ring(3, 2, p, up, 8 + p).wait_send()
    for p in range(2, 4):
        ring(1, 2, p, down, 8 + p).wait_send()


def run(*args):
    grid_f = pltpu.VMEM((BOX, 16, 2 * BOX), F32)
    three_f = pltpu.VMEM((3, BOX, 16, 2 * BOX), F32)
    six_b = pltpu.VMEM((2, 3, BOX, 16, 2 * BOX), BF16)
    natural = (KEPT, 48, 2 * BOX)
    dma = pltpu.SemaphoreType.DMA
    return pl.pallas_call(
        kernel,
        out_shape=(shape(natural), shape(natural)),
        in_specs=[pl.BlockSpec(memory_space=pl.ANY)] + [vmem] * (len(args) - 1),
        out_specs=(vmem, vmem),
        scratch_shapes=[
            pltpu.VMEM((4, 64, BOX, 2 * BOX), BF16),
            pltpu.VMEM((64 * STEP, 2 * BOX), F32),
            pltpu.VMEM((4, 4, ROWS, 64, 2 * BOX), BF16),
            grid_f, grid_f, grid_f,
            grid_f, grid_f, three_f, three_f, six_b, six_b, six_b, six_b,
            pltpu.VMEM((ROWS, 96, 2 * BOX), BF16),
            pltpu.VMEM((ROWS, 48, 2 * BOX), F32),
            pltpu.VMEM((3, 24, 256), BF16),
            pltpu.VMEM((3, 16, 24, 256), BF16),
            pltpu.VMEM(natural, F32),
            pltpu.VMEM((3, *natural), F32),
            pltpu.VMEM((2, *natural), F32),
            pltpu.VMEM((8, 2 * BOX), F32),
            pltpu.VMEM((16, 8, 2 * BOX), F32),
            dma((4,)), dma((12,)), dma((4, 4)), dma((2,)), dma((3,)), dma((3,)),
            dma((2, 3)), dma((2, 3)), dma((2, 3)), dma((2, 3)), dma((3,)), dma((3,)), dma((2,)),
        ],
        compiler_params=pltpu.CompilerParams(
            vmem_limit_bytes=VMEM_LIMIT, collective_id=0, has_side_effects=True
        ),
    )(*args)


def rows_of_planes(values):
    values = values.reshape(2, 2, BOX, 2 * BOX).transpose(2, 1, 0, 3).reshape(BOX, 4, 2 * BOX)
    return jnp.concatenate([values[: GCUT + 1], values[BOX - GCUT :]], axis=0)


def on_device(psi_occ, energies, k_point, g_mask, v_local, dv):
    planes = psi_occ.shape[1]
    ga_index = lax.axis_index("ga")
    indices = jnp.arange(BOX, dtype=jnp.int32)
    signed = jnp.where(indices < BOX // 2, indices, indices - BOX).astype(F32)
    owned = ga_index * planes + jnp.arange(planes, dtype=jnp.int32)
    freq_first = jnp.where(owned < BOX // 2, owned, owned - BOX).astype(F32)
    factor = 0.5 * (2.0 * math.pi / cell_length) ** 2
    kinetic = factor * (
        (freq_first[:, None, None] + k_point[0]) ** 2
        + (signed[None, :, None] + k_point[1]) ** 2
        + (signed[None, None, :] + k_point[2]) ** 2
    )
    kinetic = jnp.concatenate([kinetic, kinetic], axis=-1)
    sphere = g_mask.reshape(planes, BOX, BOX).astype(F32)
    sphere = jnp.concatenate([sphere, sphere], axis=-1)
    mask = jnp.repeat(rows_of_planes(sphere), 4, axis=1)
    level = (rows_of_planes(kinetic)[:, :, None, :] - energies[None, None, :, None]).reshape(
        KEPT, 16, 2 * BOX
    ) * mask
    solved = psi_occ[::STRIDE].astype(F32) * sphere[None]
    solved = solved.reshape(4, 2, 2, BOX, 2 * BOX).transpose(3, 2, 1, 0, 4).reshape(BOX, 16, 2 * BOX)
    solved = jnp.concatenate([solved[: GCUT + 1], solved[BOX - GCUT :]], axis=0)
    potential = jnp.repeat(v_local.reshape(BOX, 2, 2 * BOX), 4, axis=1)
    changes = jnp.repeat(dv.reshape(NPERT, BOX, 2, 2 * BOX), 4, axis=2)

    response, residual = run(
        psi_occ, sphere, solved, *lane_tables(), changes, potential, mask / BOX**3, level,
        jnp.asarray(fold_table(), BF16), jnp.asarray(spread_table(), BF16),
    )

    def placed(values):
        values = values.reshape(KEPT, 3, 2, 2, 4, 2 * BOX).transpose(4, 1, 3, 2, 0, 5)
        values = values.reshape(4, NPERT, 4, KEPT, 2 * BOX)
        gap = jnp.zeros((4, NPERT, 4, BOX - KEPT, 2 * BOX), F32)
        return jnp.concatenate([values[..., : GCUT + 1, :], gap, values[..., GCUT + 1 :, :]], axis=3)

    return placed(response), placed(residual)


def solution(mesh):
    placed = (
        P(("pool", "band"), "ga", None, None),
        P(("pool", "band")),
        P("pool"),
        P(("pool", "ga"), None),
        P(None, "ga"),
        P(None, None, "ga"),
    )
    return jax.shard_map(
        on_device,
        mesh=mesh,
        in_specs=placed,
        out_specs=(
            P(("pool", "band"), None, "ga", None, None),
            P(("pool", "band"), None, "ga", None, None),
        ),
        check_vma=False,
    )
```

```python
import functools
import math

import jax
import jax.numpy as jnp
import numpy as np
from jax import lax
from jax.experimental import pallas as pl
from jax.experimental.pallas import tpu as pltpu
from jax.sharding import PartitionSpec as P

BOX = 64
GCUT = 21
KEPT = 2 * GCUT + 1
NPERT = 3
STRIDE = 16
BASE_ROW = 13
SHIFT = 16.0
ROWS = 2 * BASE_ROW + 1

cell_length = 16.5
shift_weight = 8.0

kept_freqs = list(range(GCUT + 1)) + list(range(-GCUT, 0))
place_of = {f: i for i, f in enumerate(kept_freqs)}
base_freqs = list(range(BASE_ROW + 1)) + list(range(-BASE_ROW, 0))
wide_freqs = [f for m in range(14, 19) for f in (m, -m)]
narrow_freqs = [f for m in range(19, 22) for f in (m, -m)]
WIDE = len(wide_freqs)
F32 = jnp.float32
BF16 = jnp.bfloat16


def add(a, b):
    if a is None:
        return b
    if b is None:
        return a
    return (a[0] + b[0], a[1] + b[1])


def sub(a, b):
    if b is None:
        return a
    if a is None:
        return (-b[0], -b[1])
    return (a[0] - b[0], a[1] - b[1])


def times_phase(a, turns, sign):
    if a is None:
        return None
    turns = turns % 1.0
    re, im = a
    if turns == 0.0:
        return a
    if turns == 0.5:
        return (-re, -im)
    if turns in (0.25, 0.75):
        if (turns == 0.25) == (sign > 0):
            return (-im, re)
        return (im, -re)
    c, s = math.cos(2 * math.pi * turns), sign * math.sin(2 * math.pi * turns)
    if turns in (0.125, 0.375, 0.625, 0.875):
        h = abs(c)
        if (c > 0) == (s > 0):
            pair = ((re - im) * h, (re + im) * h)
        else:
            pair = ((re + im) * h, (im - re) * h)
        return pair if c > 0 else (-pair[0], -pair[1])
    return (re * c - im * s, im * c + re * s)


def small_dft(xs, sign):
    n = len(xs)
    if n == 1:
        return xs
    even, odd = small_dft(xs[0::2], sign), small_dft(xs[1::2], sign)
    turned = [times_phase(o, k / n, sign) for k, o in enumerate(odd)]
    return [add(e, o) for e, o in zip(even, turned)] + [sub(e, o) for e, o in zip(even, turned)]


def dft64(load, keep, tmp, store, sign):
    for n2 in range(8):
        out = small_dft([load(8 * n1 + n2) for n1 in range(8)], sign)
        for k1 in range(8):
            re, im = times_phase(out[k1], n2 * k1 / 64.0, sign)
            tmp[8 * n2 + k1, 0:8] = re
            tmp[8 * n2 + k1, 8:16] = im
    for k1 in range(8):
        if not any((k1 + 8 * k2) in keep for k2 in range(8)):
            continue
        out = small_dft([(tmp[8 * n2 + k1, 0:8], tmp[8 * n2 + k1, 8:16]) for n2 in range(8)], sign)
        for k2 in range(8):
            if (k1 + 8 * k2) in keep:
                store(k1 + 8 * k2, out[k2])


def corner_turn(block):
    front = lax.broadcasted_iota(jnp.int32, (8, 2 * BOX), 1) < BOX
    top = lax.broadcasted_iota(jnp.int32, (8, 2 * BOX), 0) < 4
    half = []
    for h in range(2):
        a, b = block[2 * h], block[2 * h + 1]
        half.append(
            (
                jnp.where(front, a, pltpu.roll(b, BOX, 1)),
                jnp.where(front, pltpu.roll(a, BOX, 1), b),
            )
        )
    out = [None] * 4
    for i in range(2):
        a, b = half[0][i], half[1][i]
        out[i] = jnp.where(top, a, pltpu.roll(b, 4, 0))
        out[2 + i] = jnp.where(top, pltpu.roll(a, 4, 0), b)
    return out


def turn_in(src, dst):
    for s in range(16):
        tiles = [src[4 * s + c].astype(F32) for c in range(4)]
        re = corner_turn([t[0:8] for t in tiles])
        im = corner_turn([t[8:16] for t in tiles])
        for c in range(4):
            dst[4 * s + c, 0:8] = re[c]
            dst[4 * s + c, 8:16] = im[c]


def pair(ref):
    return lambda n: (ref[n, 0:8], ref[n, 8:16])


def put_pair(ref, rows, dtype):
    def store(n, value):
        ref[n, rows] = jnp.concatenate([value[0], value[1]], axis=0).astype(dtype)

    return store


def split_dot(x, high, low):
    hi = x.astype(BF16)
    lo = (x - hi.astype(F32)).astype(BF16)
    dot = functools.partial(jnp.dot, preferred_element_type=F32)
    return dot(hi, high) + dot(lo, high) + dot(hi, low)


def lanes_forward(src, first_row, high, low, dst):
    a = src[:, pl.ds(first_row, 8), :].reshape(KEPT * 8, 2 * BOX)
    b = src[:, pl.ds(first_row + 8, 8), :].reshape(KEPT * 8, 2 * BOX)
    out = split_dot(jnp.concatenate([a, b], axis=1), high, low)
    dst[0:KEPT, 0:8, :] = out[:, : 2 * BOX].reshape(KEPT, 8, 2 * BOX)
    dst[0:KEPT, 8:16, :] = out[:, 2 * BOX :].reshape(KEPT, 8, 2 * BOX)


def lanes_back(src, high, low):
    x = jnp.concatenate(
        [
            src[0:KEPT, 0:8, :].reshape(KEPT * 8, 2 * BOX),
            src[0:KEPT, 8:16, :].reshape(KEPT * 8, 2 * BOX),
        ],
        axis=1,
    )
    out = split_dot(x, high, low)
    return (
        out[:, : 2 * BOX].reshape(KEPT, 8, 2 * BOX),
        out[:, 2 * BOX :].reshape(KEPT, 8, 2 * BOX),
    )


def lane_tables():
    index = np.arange(BOX)
    angle = (index[:, None] * index[None, :] % BOX) * (2.0 * np.pi / BOX)
    c, s, z = np.cos(angle), np.sin(angle), np.zeros((BOX, BOX))
    forward = np.block([[c, z, s, z], [-s, z, c, z], [z, c, z, s], [z, -s, z, c]])
    s = -s
    back = np.block([[c, s, z, z], [z, z, c, s], [-s, c, z, z], [z, z, -s, c]])
    out = []
    for w in (forward, back):
        w = jnp.asarray(w, F32)
        high = w.astype(BF16)
        out += [high, (w - high.astype(F32)).astype(BF16)]
    return out


kept_place = lambda n: n if n <= GCUT else (n - (BOX - KEPT) if n >= BOX - GCUT else None)
KEPT_SET = frozenset(f % BOX for f in kept_freqs)
ALL_SET = frozenset(range(BOX))


def load_kept(ref):
    def load(n):
        place = kept_place(n)
        return None if place is None else (ref[place, 0:8], ref[place, 8:16])

    return load


def forward_tile(src, first_row, high, low, near, tmp, store):
    lanes_forward(src, first_row, high, low, near)
    dft64(load_kept(near), ALL_SET, tmp, store, 1)


def back_tile(src, high, low, near, tmp):
    turn_in(src, near)

    def store(n, value):
        tmp2 = near
        tmp2[kept_place(n), 0:8] = value[0]
        tmp2[kept_place(n), 8:16] = value[1]

    dft64(pair(near), KEPT_SET, tmp, store, -1)
    return lanes_back(near, high, low)


def front_lanes(shape):
    return lax.broadcasted_iota(jnp.int32, shape, len(shape) - 1) % BOX < BOX // 2


def pack_row(get, r):
    value = get(base_freqs[r])
    front = front_lanes(value.shape)
    axis = value.ndim - 1
    if r < WIDE:
        guest = jnp.where(front, get(wide_freqs[r]), 0.0)
        value = value + pltpu.roll(guest, GCUT + 1, axis)
    elif r < 2 * WIDE:
        guest = jnp.where(front, 0.0, get(wide_freqs[r - WIDE]))
        value = value + pltpu.roll(guest, 2 * BOX - GCUT, axis)
    elif r < 2 * WIDE + 6:
        guest = get(narrow_freqs[r - 2 * WIDE])
        value = value + pltpu.roll(jnp.where(front, guest, 0.0), BOX // 2, axis)
        value = value + pltpu.roll(jnp.where(front, 0.0, guest), 3 * BOX // 2, axis)
    return value


def unpack_row(get, f):
    if f in base_freqs:
        return get(base_freqs.index(f))
    if f in wide_freqs:
        r = wide_freqs.index(f)
        up, down = get(r), get(WIDE + r)
        axis = up.ndim - 1
        return jnp.where(
            front_lanes(up.shape),
            pltpu.roll(up, 2 * BOX - GCUT - 1, axis),
            pltpu.roll(down, GCUT, axis),
        )
    value = get(2 * WIDE + narrow_freqs.index(f))
    axis = value.ndim - 1
    return jnp.where(
        front_lanes(value.shape),
        pltpu.roll(value, 3 * BOX // 2, axis),
        pltpu.roll(value, BOX // 2, axis),
    )


def lane_sign(shape):
    return jnp.where(lax.broadcasted_iota(jnp.int32, shape, len(shape) - 1) < BOX, 1.0, -1.0)


def panel_rows(panel, slots, r, p, both):
    rows = [jnp.concatenate([panel[d, p, r] for d in slots], axis=0)]
    if both:
        rows.append(jnp.concatenate([panel[d, p, r + 1] for d in slots], axis=0))
    return jnp.concatenate(rows, axis=1)


def pack_values(values, packed):
    sign = lane_sign((48, 2 * BOX))
    for r in range(ROWS):
        straight = pack_row(lambda f: values[place_of[f]], r)
        turned = pack_row(lambda f: pltpu.roll(values[place_of[f]], BOX, 1) * sign, r)
        packed[r] = jnp.concatenate([straight, turned], axis=0).astype(BF16)


def correlate(packed, panel, fold, slots):
    count = 64 * len(slots)
    nt = (((1,), (1,)), ((), ()))
    total = [None] * 4
    for r in range(0, ROWS, 2):
        both = r + 1 < ROWS
        y = jnp.concatenate([packed[r], packed[r + 1]], axis=1) if both else packed[r]
        for p in range(4):
            o = panel_rows(panel, slots, r, p, both)
            part = lax.dot_general(o, y, nt, preferred_element_type=F32)
            total[p] = part if total[p] is None else total[p] + part
    column = lax.broadcasted_iota(jnp.int32, (count, 96), 1) % 16 // 4
    chosen = total[0]
    for p in range(1, 4):
        chosen = jnp.where(column == 2 * (p % 2) + p // 2, total[p], chosen)
    hi = chosen.astype(BF16)
    lo = (chosen - hi.astype(F32)).astype(BF16)
    return lax.dot_general(fold, hi, nt, preferred_element_type=F32) + lax.dot_general(
        fold, lo, nt, preferred_element_type=F32
    )


def fold_table():
    f = np.zeros((2, 3, 4, 2, 3, 4, 4), np.float32)
    for a in range(2):
        for t in range(3):
            for q in range(4):
                f[a, t, q, a, t, :, q] = 1.0
    return f.reshape(24, 96)


def spread_table():
    f = np.zeros((4, 2, 3, 2, 2, 4, 2, 3, 4), np.float32)
    for p in range(4):
        for a in range(2):
            for t in range(3):
                for q in range(4):
                    f[p, a, t, p % 2, p // 2, q, a, t, q] = 1.0
    return f.reshape(384, 24)


def combine(corr, panel, spread, product, finish):
    rows = jnp.dot(spread[...], corr, preferred_element_type=F32).astype(BF16)
    sign = -lane_sign((48, 2 * BOX))
    for r in range(0, ROWS, 2):
        both = r + 1 < ROWS
        total = None
        for p in range(4):
            o = panel_rows(panel, SLOTS, r, p, both)
            part = jnp.dot(rows[96 * p : 96 * p + 96], o, preferred_element_type=F32)
            total = part if total is None else total + part
        for c in range(2 if both else 1):
            lanes = slice(2 * BOX * c, 2 * BOX * (c + 1))
            product[r + c] = (
                total[:48, lanes] + pltpu.roll(total[48:, lanes], BOX, 1) * sign
            )
    for f in kept_freqs:
        finish(place_of[f], unpack_row(lambda r: product[r], f))


VMEM_LIMIT = 62 * 1024 * 1024
MESH = pl.DeviceIdType.MESH
vmem = pl.BlockSpec(memory_space=pltpu.VMEM)
smem = pl.BlockSpec(memory_space=pltpu.SMEM)
STEP = 72
SLOTS = (0, 1, 3, 2)


def shape(dims, dtype=F32):
    return jax.ShapeDtypeStruct(dims, dtype)


def remote(src, dst, send, recv, where):
    return pltpu.make_async_remote_copy(
        src_ref=src, dst_ref=dst, send_sem=send, recv_sem=recv, device_id=where, device_id_type=MESH
    )


def to_peers(me, src_of, dst, send, recv):
    def one(k, carry):
        g = lax.rem(me + k, 16)
        remote(src_of(g), dst, send, recv, {"ga": g}).start()
        return carry

    lax.fori_loop(1, 16, one, 0)


def kernel(
    psi, g_mask, v_local, dv, energies, k_point, fwd_hi, fwd_lo, back_hi, back_lo, fold, spread,
    response, residual,
    raw, mask_rows, mask, level, solved, changes, potential, solved_rows, weights, wide_rows, panel, near, tmp, space, send_a, came_a, send_b, came_b, send_1, send_2,
    came_1, came_2, packed, product, share, shares, source, vec, image, sums, sums_here, all_sums,
    raw_sem, ring_send, ring_recv, a_sem, b_send, b_recv, s1, r1, s2, r2, c_send, c_recv, m_sem,
):
    me = lax.axis_index("ga")
    z = lax.axis_index("band")
    up, down = lax.rem(z + 1, 4), lax.rem(z + 3, 4)

    barrier = pltpu.get_barrier_semaphore()

    def greet(k, carry):
        pl.semaphore_signal(
            barrier, inc=1, device_id={"ga": lax.rem(me + k, 16)}, device_id_type=MESH
        )
        return carry

    lax.fori_loop(1, 16, greet, 0)
    for other in (up, down):
        pl.semaphore_signal(barrier, inc=1, device_id={"band": other}, device_id_type=MESH)

    def raw_copy(p):
        return pltpu.make_async_copy(psi.at[:, p], raw.at[p], raw_sem.at[p])

    for p in range(4):
        raw_copy(p).start()

    front = lax.broadcasted_iota(jnp.int32, (4, 2 * BOX), 1) < BOX
    top = lax.broadcasted_iota(jnp.int32, (8, 2 * BOX), 0) < 4
    for c in range(BOX // 2):
        both = g_mask[:, 2 * BOX * c : 2 * BOX * (c + 1)].astype(F32)
        turned = pltpu.roll(both, BOX, 1)
        for n, rows in ((2 * c, jnp.where(front, both, turned)), (2 * c + 1, jnp.where(front, turned, both))):
            for p in range(4):
                mask_rows[p, n : n + 1] = rows[p : p + 1]

    def spread_rows(first, second):
        return jnp.where(top, jnp.broadcast_to(first, (8, 2 * BOX)), jnp.broadcast_to(second, (8, 2 * BOX)))

    def pack_plane(u, carry):
        p = 2 * lax.rem(u, 2) + u // 2
        raw_copy(p).wait()

        def widen(m, c):
            wide_rows[pl.ds(pl.multiple_of(STEP * m, 8), BOX), :] = raw[p, m].astype(F32)
            return c

        lax.fori_loop(0, 64, widen, 0)

        def get(f):
            n = f % BOX
            return wide_rows[pl.ds(n, 64, stride=STEP), :] * mask_rows[p, n : n + 1]

        for r in range(ROWS):
            panel[0, p, r] = pack_row(get, r).astype(BF16)
        return carry

    lax.fori_loop(0, 2, pack_plane, 0)
    pl.semaphore_wait(barrier, 17)

    def ring(src_slot, dst_slot, p, where, n):
        return remote(
            panel.at[src_slot, p], panel.at[dst_slot, p], ring_send.at[n], ring_recv.at[dst_slot, p],
            {"band": where},
        )

    def ring_up(p):
        return ring(0, 3, p, up, p)

    def ring_down(p):
        return ring(0, 1, p, down, 4 + p)

    ring_up(0).start()
    ring_down(2).start()
    lax.fori_loop(2, 4, pack_plane, 0)
    ring_up(1).start()
    ring_down(3).start()
    ring_up(2).start()
    ring_down(0).start()
    ring_up(3).start()
    ring_down(1).start()

    for i in range(2):
        for k in range(2):
            for q in range(4):
                solved_rows[pl.ds(STEP * (8 * i + 4 * k + q), BOX), :] = raw[2 * k + i, STRIDE * q].astype(F32)
    for f in kept_freqs:
        n = f % BOX
        for i in range(2):
            rows = mask_rows[i, n : n + 1], mask_rows[2 + i, n : n + 1]
            mask[place_of[f], 8 * i : 8 * i + 8] = spread_rows(*rows)
        solved[place_of[f]] = solved_rows[pl.ds(n, 16, stride=STEP), :] * mask[place_of[f]]
    forward_tile(solved, 0, fwd_hi[...], fwd_lo[...], near, tmp, put_pair(send_a, slice(0, 16), F32))

    mine = pl.ds(4 * me, 4)
    to_peers(me, lambda g: send_a.at[pl.ds(4 * g, 4)], came_a.at[mine], a_sem.at[0], a_sem.at[1])
    came_a[mine] = send_a[mine]

    def spread_field(n, carry):
        line = v_local[pl.ds(n, 1), :]
        potential[n] = spread_rows(line[:, : 2 * BOX], line[:, 2 * BOX :])
        for p in range(NPERT):
            line = dv[p, pl.ds(n, 1), :]
            changes[p, n] = spread_rows(line[:, : 2 * BOX], line[:, 2 * BOX :])
        return carry

    lax.fori_loop(0, BOX, spread_field, 0)

    factor = 0.5 * (2.0 * math.pi / cell_length) ** 2
    row = lax.broadcasted_iota(jnp.int32, (8, 2 * BOX), 0)
    third = lax.broadcasted_iota(jnp.int32, (8, 2 * BOX), 1) % BOX
    third = jnp.where(third < BOX // 2, third, third - BOX).astype(F32)
    for i in range(2):
        first = 4 * me + 2 * (row // 4) + i
        first = jnp.where(first < BOX // 2, first, first - BOX).astype(F32)
        still = factor * ((first + k_point[0]) ** 2 + (third + k_point[2]) ** 2)
        for q in range(4):
            still = jnp.where(row % 4 == q, still - energies[q], still)
        for f in kept_freqs:
            here = mask[place_of[f], 8 * i : 8 * i + 8]
            rise = factor * (float(f) + k_point[1]) * (float(f) + k_point[1])
            level[place_of[f], 8 * i : 8 * i + 8] = (still + rise) * here
            mask[place_of[f], 8 * i : 8 * i + 8] = here * (1.0 / BOX**3)

    def wait_all(src, dst, send, recv):
        return remote(src, dst, send, recv, {"ga": lax.rem(me + 1, 16)})

    every = pl.ds(0, 60)
    wait_all(send_a.at[every], came_a.at[every], a_sem.at[0], a_sem.at[1]).wait()

    turn_in(came_a, near)

    def keep(n, value):
        space[n, 0:8] = value[0]
        space[n, 8:16] = value[1]

    dft64(pair(near), ALL_SET, tmp, keep, 1)

    def each_change(p, carry):
        def load(n):
            d = changes[p, n]
            return (space[n, 0:8] * d, space[n, 8:16] * d)

        dft64(load, ALL_SET, tmp, put_pair(send_b.at[p], slice(0, 16), F32), -1)
        to_peers(
            me, lambda g: send_b.at[p, pl.ds(4 * g, 4)], came_b.at[p, mine], b_send.at[p], b_recv.at[p]
        )
        came_b[p, mine] = send_b[p, mine]
        return carry

    lax.fori_loop(0, NPERT, each_change, 0)

    def pass_on(p_up, p_down):
        ring(0, 3, p_up, up, p_up).wait_recv()
        first = ring(3, 2, p_up, up, 8 + p_up)
        first.start()
        ring(0, 1, p_down, down, 4 + p_down).wait_recv()
        second = ring(1, 2, p_down, down, 8 + p_down)
        second.start()

    pass_on(0, 2)
    pass_on(1, 3)

    def back(came, dst_add):
        def each(t, carry):
            dst_add(t)
            return carry

        lax.fori_loop(0, 3, each, 0)

    def source_tile(t):
        wait_all(send_b.at[t, every], came_b.at[t, every], b_send.at[t], b_recv.at[t]).wait()
        start = pl.multiple_of(16 * t, 16)
        a, b = back_tile(came_b.at[t], back_hi[...], back_lo[...], near, tmp)
        source[:, pl.ds(start, 8), :] = a * mask[:, 0:8, :]
        source[:, pl.ds(start + 8, 8), :] = b * mask[:, 8:16, :]

    back(came_b, source_tile)

    def send_share(n, src):
        to_peers(me, lambda g: src, shares.at[n, me], c_send.at[n], c_recv.at[n])

    def total_share(n):
        first = pl.ds(0, 15)
        wait_all(shares.at[n, first], shares.at[n, first], c_send.at[n], c_recv.at[n]).wait()
        total = shares[n, 0].astype(F32)
        for g in range(1, 16):
            total = total + shares[n, g].astype(F32)
        return total.astype(BF16)

    pack_values(source, packed)
    for p in range(2, 4):
        ring(0, 3, p, up, p).wait_recv()
    for p in range(2):
        ring(0, 1, p, down, 4 + p).wait_recv()
    early = correlate(packed, panel, fold[...], SLOTS[:3])
    for p in range(2):
        ring(3, 2, p, up, 8 + p).wait_recv()
    for p in range(2, 4):
        ring(1, 2, p, down, 8 + p).wait_recv()
    late = correlate(packed, panel, fold[...], SLOTS[3:])
    share[0] = jnp.concatenate([early, late], axis=1).astype(BF16)
    shares[0, me] = share[0]
    send_share(0, share.at[0])

    def first_row(place, row):
        for t in range(3):
            rows = slice(16 * t, 16 * t + 16)
            vec[0, place, rows] = row[rows] * mask[place] - source[place, rows]

    combine(total_share(0), panel, spread, product, first_row)

    lane = lax.broadcasted_iota(jnp.int32, (8, 2 * BOX), 1)

    def apply(it, carry):
        def near_tile(t, c):
            start = pl.multiple_of(16 * t, 16)
            forward_tile(
                vec.at[it], start, fwd_hi[...], fwd_lo[...], near, tmp,
                put_pair(send_1.at[it, t], slice(0, 16), BF16),
            )
            to_peers(
                me, lambda g: send_1.at[it, t, pl.ds(4 * g, 4)], came_1.at[it, t, mine],
                s1.at[it, t], r1.at[it, t],
            )
            came_1[it, t, mine] = send_1[it, t, mine]
            return c

        lax.fori_loop(0, 3, near_tile, 0)

        pack_values(vec.at[it], packed)
        n = it + 1
        share[n] = correlate(packed, panel, fold[...], SLOTS).astype(BF16)
        shares[n, me] = share[n]
        send_share(n, share.at[n])

        def space_tile(t, c):
            wait_all(send_1.at[it, t, every], came_1.at[it, t, every], s1.at[it, t], r1.at[it, t]).wait()
            turn_in(came_1.at[it, t], near)

            weight = [jnp.zeros((8, 2 * BOX), F32)]

            def with_potential(k, value):
                v = potential[k]
                re, im = value[0] * v, value[1] * v
                near[k, 0:8] = re
                near[k, 8:16] = im
                weight[0] = weight[0] + (value[0] * re + value[1] * im)

            dft64(pair(near), ALL_SET, tmp, with_potential, 1)
            weights[t] = weight[0]
            dft64(pair(near), ALL_SET, tmp, put_pair(send_2.at[it, t], slice(0, 16), BF16), -1)
            to_peers(
                me, lambda g: send_2.at[it, t, pl.ds(4 * g, 4)], came_2.at[it, t, mine],
                s2.at[it, t], r2.at[it, t],
            )
            came_2[it, t, mine] = send_2[it, t, mine]
            return c

        lax.fori_loop(0, 3, space_tile, 0)

        def with_level(place, row):
            for t in range(3):
                rows = slice(16 * t, 16 * t + 16)
                image[it, place, rows] = (
                    row[rows] * (shift_weight * mask[place])
                    + level[place] * vec[it, place, rows]
                )

        corr = total_share(n)

        @pl.when(it == 1)
        def _():
            def moments(place, totals):
                b, ab, w = vec[0, place], image[0, place], vec[1, place]
                lift = jnp.concatenate([level[place]] * 3, axis=0)
                return tuple(x + y for x, y in zip(totals, (b * b, b * ab, ab * ab, lift * w * w)))

            zero = jnp.zeros((48, 2 * BOX), F32)
            totals = lax.fori_loop(0, KEPT, moments, (zero,) * 4)
            own = jnp.zeros((8, 2 * BOX), F32)
            for m, total in enumerate(totals):
                line = jnp.sum(total, axis=1, keepdims=True) * (1.0 / BOX**3)
                for t in range(3):
                    both = line[16 * t : 16 * t + 8] + line[16 * t + 8 : 16 * t + 16]
                    if m == 3:
                        both = both + jnp.sum(weights[t], axis=1, keepdims=True) * (1.0 / BOX**6)
                    own = jnp.where(lane == 4 * t + m, jnp.broadcast_to(both, own.shape), own)
            own = own + pltpu.roll(own, 4, 0)
            sums[...] = own
            all_sums[me] = own
            to_peers(me, lambda g: sums, all_sums.at[me], m_sem.at[0], m_sem.at[1])
            square = corr.astype(F32)
            square = jnp.sum(square * square, axis=1, keepdims=True) * (shift_weight / BOX**6)
            rest = jnp.zeros((8, 2 * BOX), F32)
            for t in range(3):
                four = square[4 * t : 4 * t + 4] + square[12 + 4 * t : 16 + 4 * t]
                eight = jnp.concatenate([four, four], axis=0)
                rest = jnp.where(lane == 4 * t + 3, jnp.broadcast_to(eight, rest.shape), rest)
            sums_here[...] = rest

        combine(corr, panel, spread, product, with_level)

        def far_tile(t, c):
            wait_all(send_2.at[it, t, every], came_2.at[it, t, every], s2.at[it, t], r2.at[it, t]).wait()
            start = pl.multiple_of(16 * t, 16)
            a, b = back_tile(came_2.at[it, t], back_hi[...], back_lo[...], near, tmp)
            for half, value in ((0, a), (8, b)):
                rows = pl.ds(start + half, 8)
                total = image[it, :, rows, :] + value * mask[:, half : half + 8, :]
                image[it, :, rows, :] = total
                vec[it + 1, :, rows, :] = total - SHIFT * vec[it, :, rows, :]
            return c

        lax.fori_loop(0, 3, far_tile, 0)
        return carry

    lax.fori_loop(0, 2, apply, 0)

    first = pl.ds(0, 15)
    wait_all(all_sums.at[first], all_sums.at[first], m_sem.at[0], m_sem.at[1]).wait()
    m0 = sums_here[...] + all_sums[0]
    for g in range(1, 16):
        m0 = m0 + all_sums[g]
    m1, m2, m3 = (pltpu.roll(m0, 2 * BOX - n, 1) for n in (1, 2, 3))
    step0 = m0 / m1
    fresh = m0 - 2.0 * step0 * m1 + step0 * step0 * m2
    u = 1.0 + fresh / m0 - step0 * SHIFT
    curve = u * u * m1 - 2.0 * u * step0 * (m2 - SHIFT * m1) + step0 * step0 * m3
    step1 = fresh / curve
    low_part, high_part = step0 + step1 * u, step1 * step0
    for t in range(3):
        a = jnp.broadcast_to(low_part[:, 4 * t : 4 * t + 1], (8, 2 * BOX))
        e = jnp.broadcast_to(high_part[:, 4 * t : 4 * t + 1], (8, 2 * BOX))
        for half in (0, 8):
            rows = slice(16 * t + half, 16 * t + half + 8)
            b, ab = vec[0, :, rows, :], image[0, :, rows, :]
            response[:, rows, :] = a * b - e * vec[1, :, rows, :]
            residual[:, rows, :] = b - a * ab + e * image[1, :, rows, :]

    for p in range(4):
        ring_up(p).wait_send()
        ring_down(p).wait_send()
    for p in range(2):
        ring(3, 2, p, up, 8 + p).wait_send()
    for p in range(2, 4):
        ring(1, 2, p, down, 8 + p).wait_send()


def run(*args):
    grid_f = pltpu.VMEM((BOX, 16, 2 * BOX), F32)
    three_f = pltpu.VMEM((3, BOX, 16, 2 * BOX), F32)
    six_b = pltpu.VMEM((2, 3, BOX, 16, 2 * BOX), BF16)
    natural = (KEPT, 48, 2 * BOX)
    dma = pltpu.SemaphoreType.DMA
    return pl.pallas_call(
        kernel,
        out_shape=(shape(natural), shape(natural)),
        in_specs=[pl.BlockSpec(memory_space=pl.ANY)] + [vmem] * 3 + [smem] * 2 + [vmem] * 6,
        out_specs=(vmem, vmem),
        scratch_shapes=[
            pltpu.VMEM((4, 64, BOX, 2 * BOX), BF16),
            pltpu.VMEM((4, BOX, 2 * BOX), F32),
            pltpu.VMEM((KEPT, 16, 2 * BOX), F32),
            pltpu.VMEM((KEPT, 16, 2 * BOX), F32),
            pltpu.VMEM((KEPT, 16, 2 * BOX), F32),
            pltpu.VMEM((NPERT, BOX, 8, 2 * BOX), F32),
            pltpu.VMEM((BOX, 8, 2 * BOX), F32),
            pltpu.VMEM((16 * STEP, 2 * BOX), F32),
            pltpu.VMEM((3, 8, 2 * BOX), F32),
            pltpu.VMEM((64 * STEP, 2 * BOX), F32),
            pltpu.VMEM((4, 4, ROWS, 64, 2 * BOX), BF16),
            grid_f, grid_f, grid_f,
            grid_f, grid_f, three_f, three_f, six_b, six_b, six_b, six_b,
            pltpu.VMEM((ROWS, 96, 2 * BOX), BF16),
            pltpu.VMEM((ROWS, 48, 2 * BOX), F32),
            pltpu.VMEM((3, 24, 256), BF16),
            pltpu.VMEM((3, 16, 24, 256), BF16),
            pltpu.VMEM(natural, F32),
            pltpu.VMEM((3, *natural), F32),
            pltpu.VMEM((2, *natural), F32),
            pltpu.VMEM((8, 2 * BOX), F32),
            pltpu.VMEM((8, 2 * BOX), F32),
            pltpu.VMEM((16, 8, 2 * BOX), F32),
            dma((4,)), dma((12,)), dma((4, 4)), dma((2,)), dma((3,)), dma((3,)),
            dma((2, 3)), dma((2, 3)), dma((2, 3)), dma((2, 3)), dma((3,)), dma((3,)), dma((2,)),
        ],
        compiler_params=pltpu.CompilerParams(
            vmem_limit_bytes=VMEM_LIMIT, collective_id=0, has_side_effects=True
        ),
    )(*args)


def on_device(psi_occ, energies, k_point, g_mask, v_local, dv):
    response, residual = run(
        psi_occ, g_mask, v_local, dv, energies, k_point, *lane_tables(),
        jnp.asarray(fold_table(), BF16), jnp.asarray(spread_table(), BF16),
    )

    def placed(values):
        values = values.reshape(KEPT, 3, 2, 2, 4, 2 * BOX).transpose(4, 1, 3, 2, 0, 5)
        values = values.reshape(4, NPERT, 4, KEPT, 2 * BOX)
        gap = jnp.zeros((4, NPERT, 4, BOX - KEPT, 2 * BOX), F32)
        return jnp.concatenate([values[..., : GCUT + 1, :], gap, values[..., GCUT + 1 :, :]], axis=3)

    return placed(response), placed(residual)


def solution(mesh):
    placed = (
        P(("pool", "band"), "ga", None, None),
        P(("pool", "band")),
        P("pool"),
        P(("pool", "ga"), None),
        P(None, "ga"),
        P(None, None, "ga"),
    )
    return jax.shard_map(
        on_device,
        mesh=mesh,
        in_specs=placed,
        out_specs=(
            P(("pool", "band"), None, "ga", None, None),
            P(("pool", "band"), None, "ga", None, None),
        ),
        check_vma=False,
    )
```

```python
import functools
import math

import jax
import jax.numpy as jnp
import numpy as np
from jax import lax
from jax.experimental import pallas as pl
from jax.experimental.pallas import tpu as pltpu
from jax.sharding import PartitionSpec as P

BOX = 64
GCUT = 21
KEPT = 2 * GCUT + 1
NPERT = 3
STRIDE = 16
SHIFT = 16.0
ROWS = 24

cell_length = 16.5
shift_weight = 8.0

kept_freqs = list(range(GCUT + 1)) + list(range(-GCUT, 0))
place_of = {f: i for i, f in enumerate(kept_freqs)}
F32 = jnp.float32
BF16 = jnp.bfloat16


def add(a, b):
    if a is None:
        return b
    if b is None:
        return a
    return (a[0] + b[0], a[1] + b[1])


def sub(a, b):
    if b is None:
        return a
    if a is None:
        return (-b[0], -b[1])
    return (a[0] - b[0], a[1] - b[1])


def times_phase(a, turns, sign):
    if a is None:
        return None
    turns = turns % 1.0
    re, im = a
    if turns == 0.0:
        return a
    if turns == 0.5:
        return (-re, -im)
    if turns in (0.25, 0.75):
        if (turns == 0.25) == (sign > 0):
            return (-im, re)
        return (im, -re)
    c, s = math.cos(2 * math.pi * turns), sign * math.sin(2 * math.pi * turns)
    if turns in (0.125, 0.375, 0.625, 0.875):
        h = abs(c)
        if (c > 0) == (s > 0):
            pair = ((re - im) * h, (re + im) * h)
        else:
            pair = ((re + im) * h, (im - re) * h)
        return pair if c > 0 else (-pair[0], -pair[1])
    return (re * c - im * s, im * c + re * s)


def small_dft(xs, sign):
    n = len(xs)
    if n == 1:
        return xs
    even, odd = small_dft(xs[0::2], sign), small_dft(xs[1::2], sign)
    turned = [times_phase(o, k / n, sign) for k, o in enumerate(odd)]
    return [add(e, o) for e, o in zip(even, turned)] + [sub(e, o) for e, o in zip(even, turned)]


def dft64(load, keep, tmp, store, sign):
    for n2 in range(8):
        out = small_dft([load(8 * n1 + n2) for n1 in range(8)], sign)
        for k1 in range(8):
            re, im = times_phase(out[k1], n2 * k1 / 64.0, sign)
            tmp[8 * n2 + k1, 0:8] = re
            tmp[8 * n2 + k1, 8:16] = im
    for k1 in range(8):
        if not any((k1 + 8 * k2) in keep for k2 in range(8)):
            continue
        out = small_dft([(tmp[8 * n2 + k1, 0:8], tmp[8 * n2 + k1, 8:16]) for n2 in range(8)], sign)
        for k2 in range(8):
            if (k1 + 8 * k2) in keep:
                store(k1 + 8 * k2, out[k2])


def corner_turn(block):
    front = lax.broadcasted_iota(jnp.int32, (8, 2 * BOX), 1) < BOX
    top = lax.broadcasted_iota(jnp.int32, (8, 2 * BOX), 0) < 4
    half = []
    for h in range(2):
        a, b = block[2 * h], block[2 * h + 1]
        half.append(
            (
                jnp.where(front, a, pltpu.roll(b, BOX, 1)),
                jnp.where(front, pltpu.roll(a, BOX, 1), b),
            )
        )
    out = [None] * 4
    for i in range(2):
        a, b = half[0][i], half[1][i]
        out[i] = jnp.where(top, a, pltpu.roll(b, 4, 0))
        out[2 + i] = jnp.where(top, pltpu.roll(a, 4, 0), b)
    return out


def turn_in(src, dst):
    for s in range(16):
        tiles = [src[4 * s + c].astype(F32) for c in range(4)]
        re = corner_turn([t[0:8] for t in tiles])
        im = corner_turn([t[8:16] for t in tiles])
        for c in range(4):
            dst[4 * s + c, 0:8] = re[c]
            dst[4 * s + c, 8:16] = im[c]


def pair(ref):
    return lambda n: (ref[n, 0:8], ref[n, 8:16])


def put_pair(ref, rows, dtype):
    def store(n, value):
        ref[n, rows] = jnp.concatenate([value[0], value[1]], axis=0).astype(dtype)

    return store


def split_dot(x, high, low):
    hi = x.astype(BF16)
    lo = (x - hi.astype(F32)).astype(BF16)
    dot = functools.partial(jnp.dot, preferred_element_type=F32)
    return dot(hi, high) + dot(lo, high) + dot(hi, low)


def lanes_forward(src, first_row, high, low, dst):
    a = src[:, pl.ds(first_row, 8), :].reshape(KEPT * 8, 2 * BOX)
    b = src[:, pl.ds(first_row + 8, 8), :].reshape(KEPT * 8, 2 * BOX)
    out = split_dot(jnp.concatenate([a, b], axis=1), high, low)
    dst[0:KEPT, 0:8, :] = out[:, : 2 * BOX].reshape(KEPT, 8, 2 * BOX)
    dst[0:KEPT, 8:16, :] = out[:, 2 * BOX :].reshape(KEPT, 8, 2 * BOX)


def lanes_back(src, high, low):
    x = jnp.concatenate(
        [
            src[0:KEPT, 0:8, :].reshape(KEPT * 8, 2 * BOX),
            src[0:KEPT, 8:16, :].reshape(KEPT * 8, 2 * BOX),
        ],
        axis=1,
    )
    out = split_dot(x, high, low)
    return (
        out[:, : 2 * BOX].reshape(KEPT, 8, 2 * BOX),
        out[:, 2 * BOX :].reshape(KEPT, 8, 2 * BOX),
    )


def lane_tables():
    index = np.arange(BOX)
    angle = (index[:, None] * index[None, :] % BOX) * (2.0 * np.pi / BOX)
    c, s, z = np.cos(angle), np.sin(angle), np.zeros((BOX, BOX))
    forward = np.block([[c, z, s, z], [-s, z, c, z], [z, c, z, s], [z, -s, z, c]])
    s = -s
    back = np.block([[c, s, z, z], [z, z, c, s], [-s, c, z, z], [z, z, -s, c]])
    out = []
    for w in (forward, back):
        w = jnp.asarray(w, F32)
        high = w.astype(BF16)
        out += [high, (w - high.astype(F32)).astype(BF16)]
    return out


kept_place = lambda n: n if n <= GCUT else (n - (BOX - KEPT) if n >= BOX - GCUT else None)
KEPT_SET = frozenset(f % BOX for f in kept_freqs)
ALL_SET = frozenset(range(BOX))


def load_kept(ref):
    def load(n):
        place = kept_place(n)
        return None if place is None else (ref[place, 0:8], ref[place, 8:16])

    return load


def forward_tile(src, first_row, high, low, near, tmp, store):
    lanes_forward(src, first_row, high, low, near)
    dft64(load_kept(near), ALL_SET, tmp, store, 1)


def back_tile(src, high, low, near, tmp):
    turn_in(src, near)

    def store(n, value):
        tmp2 = near
        tmp2[kept_place(n), 0:8] = value[0]
        tmp2[kept_place(n), 8:16] = value[1]

    dft64(pair(near), KEPT_SET, tmp, store, -1)
    return lanes_back(near, high, low)


def front_lanes(shape):
    return lax.broadcasted_iota(jnp.int32, shape, len(shape) - 1) % BOX < BOX // 2


def widest(f):
    return int(math.sqrt(GCUT**2 - max(abs(f) - 0.5, 0.0) ** 2) + 0.5)


def lay_rows():
    order = sorted(kept_freqs, key=lambda f: (abs(f), -f))
    hosts, others = order[:ROWS], order[ROWS:]
    room = [[widest(f) + 1, BOX - 1 - widest(f)] for f in hosts]
    pieces = sorted(
        [(widest(f) + 1, f, True) for f in others] + [(widest(f), f, False) for f in others],
        key=lambda piece: -piece[0],
    )
    guests, where = [[] for _ in hosts], {}
    for size, f, ahead in pieces:
        fits = [r for r in range(ROWS) if room[r][1] - room[r][0] + 1 >= size]
        r = min(fits, key=lambda n: (room[n][1] - room[n][0] + 1 - size, n))
        start = room[r][0]
        shift = start if ahead else start - (BOX - size)
        room[r][0] = start + size
        guests[r].append((f, ahead, shift % (2 * BOX)))
        where[f, ahead] = (r, shift % (2 * BOX))
    return hosts, guests, where


hosts, guests, where_laid = lay_rows()


def pack_row(get, r):
    value = get(hosts[r])
    front = front_lanes(value.shape)
    for f, ahead, shift in guests[r]:
        row = get(f)
        piece = jnp.where(front, row, 0.0) if ahead else jnp.where(front, 0.0, row)
        value = value + pltpu.roll(piece, shift, value.ndim - 1)
    return value


def unpack_row(get, f):
    if f in hosts:
        return get(hosts.index(f))
    (r, up), (n, down) = where_laid[f, True], where_laid[f, False]
    first, second = get(r), get(n)
    axis = first.ndim - 1
    return jnp.where(
        front_lanes(first.shape),
        pltpu.roll(first, (2 * BOX - up) % (2 * BOX), axis),
        pltpu.roll(second, (2 * BOX - down) % (2 * BOX), axis),
    )


def lane_sign(shape):
    return jnp.where(lax.broadcasted_iota(jnp.int32, shape, len(shape) - 1) < BOX, 1.0, -1.0)


def panel_rows(panel, slots, r, p, both):
    rows = [jnp.concatenate([panel[d, p, r] for d in slots], axis=0)]
    if both:
        rows.append(jnp.concatenate([panel[d, p, r + 1] for d in slots], axis=0))
    return jnp.concatenate(rows, axis=1)


def pack_values(values, packed):
    sign = lane_sign((48, 2 * BOX))
    for r in range(ROWS):
        straight = pack_row(lambda f: values[place_of[f]], r)
        turned = pack_row(lambda f: pltpu.roll(values[place_of[f]], BOX, 1) * sign, r)
        packed[r] = jnp.concatenate([straight, turned], axis=0).astype(BF16)


def correlate(packed, panel, fold, slots):
    count = 64 * len(slots)
    nt = (((1,), (1,)), ((), ()))
    total = [None] * 4
    for r in range(0, ROWS, 2):
        both = r + 1 < ROWS
        y = jnp.concatenate([packed[r], packed[r + 1]], axis=1) if both else packed[r]
        for p in range(4):
            o = panel_rows(panel, slots, r, p, both)
            part = lax.dot_general(o, y, nt, preferred_element_type=F32)
            total[p] = part if total[p] is None else total[p] + part
    column = lax.broadcasted_iota(jnp.int32, (count, 96), 1) % 16 // 4
    chosen = total[0]
    for p in range(1, 4):
        chosen = jnp.where(column == 2 * (p % 2) + p // 2, total[p], chosen)
    hi = chosen.astype(BF16)
    lo = (chosen - hi.astype(F32)).astype(BF16)
    return lax.dot_general(fold, hi, nt, preferred_element_type=F32) + lax.dot_general(
        fold, lo, nt, preferred_element_type=F32
    )


def fold_table():
    f = np.zeros((2, 3, 4, 2, 3, 4, 4), np.float32)
    for a in range(2):
        for t in range(3):
            for q in range(4):
                f[a, t, q, a, t, :, q] = 1.0
    return f.reshape(24, 96)


def spread_table():
    f = np.zeros((4, 2, 3, 2, 2, 4, 2, 3, 4), np.float32)
    for p in range(4):
        for a in range(2):
            for t in range(3):
                for q in range(4):
                    f[p, a, t, p % 2, p // 2, q, a, t, q] = 1.0
    return f.reshape(384, 24)


def combine(corr, panel, spread, product, finish):
    rows = jnp.dot(spread[...], corr, preferred_element_type=F32).astype(BF16)
    sign = -lane_sign((48, 2 * BOX))
    for r in range(0, ROWS, 2):
        both = r + 1 < ROWS
        total = None
        for p in range(4):
            o = panel_rows(panel, SLOTS, r, p, both)
            part = jnp.dot(rows[96 * p : 96 * p + 96], o, preferred_element_type=F32)
            total = part if total is None else total + part
        for c in range(2 if both else 1):
            lanes = slice(2 * BOX * c, 2 * BOX * (c + 1))
            product[r + c] = (
                total[:48, lanes] + pltpu.roll(total[48:, lanes], BOX, 1) * sign
            )
    for f in kept_freqs:
        finish(place_of[f], unpack_row(lambda r: product[r], f))


VMEM_LIMIT = 62 * 1024 * 1024
MESH = pl.DeviceIdType.MESH
vmem = pl.BlockSpec(memory_space=pltpu.VMEM)
smem = pl.BlockSpec(memory_space=pltpu.SMEM)
STEP = 72
SLOTS = (0, 1, 3, 2)


def shape(dims, dtype=F32):
    return jax.ShapeDtypeStruct(dims, dtype)


def remote(src, dst, send, recv, where):
    return pltpu.make_async_remote_copy(
        src_ref=src, dst_ref=dst, send_sem=send, recv_sem=recv, device_id=where, device_id_type=MESH
    )


def to_peers(me, src_of, dst, send, recv):
    def one(k, carry):
        g = lax.rem(me + k, 16)
        remote(src_of(g), dst, send, recv, {"ga": g}).start()
        return carry

    lax.fori_loop(1, 16, one, 0)


def kernel(
    psi, g_mask, v_local, dv, energies, k_point, fwd_hi, fwd_lo, back_hi, back_lo, fold, spread,
    response, residual,
    raw, mask_rows, mask, level, solved, changes, potential, solved_rows, weights, wide_rows, panel, near, tmp, space, send_a, came_a, send_b, came_b, send_1, send_2,
    came_1, came_2, packed, product, share, shares, source, vec, image, sums, sums_here, all_sums,
    raw_sem, ring_send, ring_recv, a_sem, b_send, b_recv, s1, r1, s2, r2, c_send, c_recv, m_sem,
):
    me = lax.axis_index("ga")
    z = lax.axis_index("band")
    up, down = lax.rem(z + 1, 4), lax.rem(z + 3, 4)

    barrier = pltpu.get_barrier_semaphore()

    def greet(k, carry):
        pl.semaphore_signal(
            barrier, inc=1, device_id={"ga": lax.rem(me + k, 16)}, device_id_type=MESH
        )
        return carry

    lax.fori_loop(1, 16, greet, 0)
    for other in (up, down):
        pl.semaphore_signal(barrier, inc=1, device_id={"band": other}, device_id_type=MESH)

    def raw_copy(p):
        return pltpu.make_async_copy(psi.at[:, p], raw.at[p], raw_sem.at[p])

    for p in range(4):
        raw_copy(p).start()

    front = lax.broadcasted_iota(jnp.int32, (4, 2 * BOX), 1) < BOX
    top = lax.broadcasted_iota(jnp.int32, (8, 2 * BOX), 0) < 4
    for c in range(BOX // 2):
        both = g_mask[:, 2 * BOX * c : 2 * BOX * (c + 1)].astype(F32)
        turned = pltpu.roll(both, BOX, 1)
        for n, rows in ((2 * c, jnp.where(front, both, turned)), (2 * c + 1, jnp.where(front, turned, both))):
            for p in range(4):
                mask_rows[p, n : n + 1] = rows[p : p + 1]

    def spread_rows(first, second):
        return jnp.where(top, jnp.broadcast_to(first, (8, 2 * BOX)), jnp.broadcast_to(second, (8, 2 * BOX)))

    def pack_plane(u, carry):
        p = 2 * lax.rem(u, 2) + u // 2
        raw_copy(p).wait()

        def widen(m, c):
            wide_rows[pl.ds(pl.multiple_of(STEP * m, 8), BOX), :] = raw[p, m].astype(F32)
            return c

        lax.fori_loop(0, 64, widen, 0)

        def get(f):
            n = f % BOX
            return wide_rows[pl.ds(n, 64, stride=STEP), :] * mask_rows[p, n : n + 1]

        for r in range(ROWS):
            panel[0, p, r] = pack_row(get, r).astype(BF16)
        return carry

    lax.fori_loop(0, 2, pack_plane, 0)
    pl.semaphore_wait(barrier, 17)

    def ring(src_slot, dst_slot, p, where, n):
        return remote(
            panel.at[src_slot, p], panel.at[dst_slot, p], ring_send.at[n], ring_recv.at[dst_slot, p],
            {"band": where},
        )

    def ring_up(p):
        return ring(0, 3, p, up, p)

    def ring_down(p):
        return ring(0, 1, p, down, 4 + p)

    ring_up(0).start()
    ring_down(2).start()
    lax.fori_loop(2, 4, pack_plane, 0)
    ring_up(1).start()
    ring_down(3).start()
    ring_up(2).start()
    ring_down(0).start()
    ring_up(3).start()
    ring_down(1).start()

    for i in range(2):
        for k in range(2):
            for q in range(4):
                solved_rows[pl.ds(STEP * (8 * i + 4 * k + q), BOX), :] = raw[2 * k + i, STRIDE * q].astype(F32)
    for f in kept_freqs:
        n = f % BOX
        for i in range(2):
            rows = mask_rows[i, n : n + 1], mask_rows[2 + i, n : n + 1]
            mask[place_of[f], 8 * i : 8 * i + 8] = spread_rows(*rows)
        solved[place_of[f]] = solved_rows[pl.ds(n, 16, stride=STEP), :] * mask[place_of[f]]
    forward_tile(solved, 0, fwd_hi[...], fwd_lo[...], near, tmp, put_pair(send_a, slice(0, 16), F32))

    mine = pl.ds(4 * me, 4)
    to_peers(me, lambda g: send_a.at[pl.ds(4 * g, 4)], came_a.at[mine], a_sem.at[0], a_sem.at[1])
    came_a[mine] = send_a[mine]

    def spread_field(n, carry):
        line = v_local[pl.ds(n, 1), :]
        potential[n] = spread_rows(line[:, : 2 * BOX], line[:, 2 * BOX :])
        for p in range(NPERT):
            line = dv[p, pl.ds(n, 1), :]
            changes[p, n] = spread_rows(line[:, : 2 * BOX], line[:, 2 * BOX :])
        return carry

    lax.fori_loop(0, BOX, spread_field, 0)

    factor = 0.5 * (2.0 * math.pi / cell_length) ** 2
    row = lax.broadcasted_iota(jnp.int32, (8, 2 * BOX), 0)
    third = lax.broadcasted_iota(jnp.int32, (8, 2 * BOX), 1) % BOX
    third = jnp.where(third < BOX // 2, third, third - BOX).astype(F32)
    for i in range(2):
        first = 4 * me + 2 * (row // 4) + i
        first = jnp.where(first < BOX // 2, first, first - BOX).astype(F32)
        still = factor * ((first + k_point[0]) ** 2 + (third + k_point[2]) ** 2)
        for q in range(4):
            still = jnp.where(row % 4 == q, still - energies[q], still)
        for f in kept_freqs:
            here = mask[place_of[f], 8 * i : 8 * i + 8]
            rise = factor * (float(f) + k_point[1]) * (float(f) + k_point[1])
            level[place_of[f], 8 * i : 8 * i + 8] = (still + rise) * here
            mask[place_of[f], 8 * i : 8 * i + 8] = here * (1.0 / BOX**3)

    def wait_all(src, dst, send, recv):
        return remote(src, dst, send, recv, {"ga": lax.rem(me + 1, 16)})

    every = pl.ds(0, 60)
    wait_all(send_a.at[every], came_a.at[every], a_sem.at[0], a_sem.at[1]).wait()

    turn_in(came_a, near)

    def keep(n, value):
        space[n, 0:8] = value[0]
        space[n, 8:16] = value[1]

    dft64(pair(near), ALL_SET, tmp, keep, 1)

    def each_change(p, carry):
        def load(n):
            d = changes[p, n]
            return (space[n, 0:8] * d, space[n, 8:16] * d)

        dft64(load, ALL_SET, tmp, put_pair(send_b.at[p], slice(0, 16), F32), -1)
        to_peers(
            me, lambda g: send_b.at[p, pl.ds(4 * g, 4)], came_b.at[p, mine], b_send.at[p], b_recv.at[p]
        )
        came_b[p, mine] = send_b[p, mine]
        return carry

    lax.fori_loop(0, NPERT, each_change, 0)

    def pass_on(p_up, p_down):
        ring(0, 3, p_up, up, p_up).wait_recv()
        first = ring(3, 2, p_up, up, 8 + p_up)
        first.start()
        ring(0, 1, p_down, down, 4 + p_down).wait_recv()
        second = ring(1, 2, p_down, down, 8 + p_down)
        second.start()

    pass_on(0, 2)
    pass_on(1, 3)

    def back(came, dst_add):
        def each(t, carry):
            dst_add(t)
            return carry

        lax.fori_loop(0, 3, each, 0)

    def source_tile(t):
        wait_all(send_b.at[t, every], came_b.at[t, every], b_send.at[t], b_recv.at[t]).wait()
        start = pl.multiple_of(16 * t, 16)
        a, b = back_tile(came_b.at[t], back_hi[...], back_lo[...], near, tmp)
        source[:, pl.ds(start, 8), :] = a * mask[:, 0:8, :]
        source[:, pl.ds(start + 8, 8), :] = b * mask[:, 8:16, :]

    back(came_b, source_tile)

    def send_share(n, src):
        to_peers(me, lambda g: src, shares.at[n, me], c_send.at[n], c_recv.at[n])

    def total_share(n):
        first = pl.ds(0, 15)
        wait_all(shares.at[n, first], shares.at[n, first], c_send.at[n], c_recv.at[n]).wait()
        total = shares[n, 0].astype(F32)
        for g in range(1, 16):
            total = total + shares[n, g].astype(F32)
        return total.astype(BF16)

    pack_values(source, packed)
    for p in range(2, 4):
        ring(0, 3, p, up, p).wait_recv()
    for p in range(2):
        ring(0, 1, p, down, 4 + p).wait_recv()
    early = correlate(packed, panel, fold[...], SLOTS[:3])
    for p in range(2):
        ring(3, 2, p, up, 8 + p).wait_recv()
    for p in range(2, 4):
        ring(1, 2, p, down, 8 + p).wait_recv()
    late = correlate(packed, panel, fold[...], SLOTS[3:])
    share[0] = jnp.concatenate([early, late], axis=1).astype(BF16)
    shares[0, me] = share[0]
    send_share(0, share.at[0])

    def first_row(place, row):
        for t in range(3):
            rows = slice(16 * t, 16 * t + 16)
            vec[0, place, rows] = row[rows] * mask[place] - source[place, rows]

    combine(total_share(0), panel, spread, product, first_row)

    lane = lax.broadcasted_iota(jnp.int32, (8, 2 * BOX), 1)

    def apply(it, carry):
        def near_tile(t, c):
            start = pl.multiple_of(16 * t, 16)
            forward_tile(
                vec.at[it], start, fwd_hi[...], fwd_lo[...], near, tmp,
                put_pair(send_1.at[it, t], slice(0, 16), BF16),
            )
            to_peers(
                me, lambda g: send_1.at[it, t, pl.ds(4 * g, 4)], came_1.at[it, t, mine],
                s1.at[it, t], r1.at[it, t],
            )
            came_1[it, t, mine] = send_1[it, t, mine]
            return c

        lax.fori_loop(0, 3, near_tile, 0)

        pack_values(vec.at[it], packed)
        n = it + 1
        share[n] = correlate(packed, panel, fold[...], SLOTS).astype(BF16)
        shares[n, me] = share[n]
        send_share(n, share.at[n])

        def space_tile(t, c):
            wait_all(send_1.at[it, t, every], came_1.at[it, t, every], s1.at[it, t], r1.at[it, t]).wait()
            turn_in(came_1.at[it, t], near)

            weight = [jnp.zeros((8, 2 * BOX), F32)]

            def with_potential(k, value):
                v = potential[k]
                re, im = value[0] * v, value[1] * v
                near[k, 0:8] = re
                near[k, 8:16] = im
                weight[0] = weight[0] + (value[0] * re + value[1] * im)

            dft64(pair(near), ALL_SET, tmp, with_potential, 1)
            weights[t] = weight[0]
            dft64(pair(near), ALL_SET, tmp, put_pair(send_2.at[it, t], slice(0, 16), BF16), -1)
            to_peers(
                me, lambda g: send_2.at[it, t, pl.ds(4 * g, 4)], came_2.at[it, t, mine],
                s2.at[it, t], r2.at[it, t],
            )
            came_2[it, t, mine] = send_2[it, t, mine]
            return c

        lax.fori_loop(0, 3, space_tile, 0)

        def with_level(place, row):
            for t in range(3):
                rows = slice(16 * t, 16 * t + 16)
                image[it, place, rows] = (
                    row[rows] * (shift_weight * mask[place])
                    + level[place] * vec[it, place, rows]
                )

        corr = total_share(n)

        @pl.when(it == 1)
        def _():
            def moments(place, totals):
                b, ab, w = vec[0, place], image[0, place], vec[1, place]
                lift = jnp.concatenate([level[place]] * 3, axis=0)
                return tuple(x + y for x, y in zip(totals, (b * b, b * ab, ab * ab, lift * w * w)))

            zero = jnp.zeros((48, 2 * BOX), F32)
            totals = lax.fori_loop(0, KEPT, moments, (zero,) * 4)
            own = jnp.zeros((8, 2 * BOX), F32)
            for m, total in enumerate(totals):
                line = jnp.sum(total, axis=1, keepdims=True) * (1.0 / BOX**3)
                for t in range(3):
                    both = line[16 * t : 16 * t + 8] + line[16 * t + 8 : 16 * t + 16]
                    if m == 3:
                        both = both + jnp.sum(weights[t], axis=1, keepdims=True) * (1.0 / BOX**6)
                    own = jnp.where(lane == 4 * t + m, jnp.broadcast_to(both, own.shape), own)
            own = own + pltpu.roll(own, 4, 0)
            sums[...] = own
            all_sums[me] = own
            to_peers(me, lambda g: sums, all_sums.at[me], m_sem.at[0], m_sem.at[1])
            square = corr.astype(F32)
            square = jnp.sum(square * square, axis=1, keepdims=True) * (shift_weight / BOX**6)
            rest = jnp.zeros((8, 2 * BOX), F32)
            for t in range(3):
                four = square[4 * t : 4 * t + 4] + square[12 + 4 * t : 16 + 4 * t]
                eight = jnp.concatenate([four, four], axis=0)
                rest = jnp.where(lane == 4 * t + 3, jnp.broadcast_to(eight, rest.shape), rest)
            sums_here[...] = rest

        combine(corr, panel, spread, product, with_level)

        def far_tile(t, c):
            wait_all(send_2.at[it, t, every], came_2.at[it, t, every], s2.at[it, t], r2.at[it, t]).wait()
            start = pl.multiple_of(16 * t, 16)
            a, b = back_tile(came_2.at[it, t], back_hi[...], back_lo[...], near, tmp)
            for half, value in ((0, a), (8, b)):
                rows = pl.ds(start + half, 8)
                total = image[it, :, rows, :] + value * mask[:, half : half + 8, :]
                image[it, :, rows, :] = total
                vec[it + 1, :, rows, :] = total - SHIFT * vec[it, :, rows, :]
            return c

        lax.fori_loop(0, 3, far_tile, 0)
        return carry

    lax.fori_loop(0, 2, apply, 0)

    first = pl.ds(0, 15)
    wait_all(all_sums.at[first], all_sums.at[first], m_sem.at[0], m_sem.at[1]).wait()
    m0 = sums_here[...] + all_sums[0]
    for g in range(1, 16):
        m0 = m0 + all_sums[g]
    m1, m2, m3 = (pltpu.roll(m0, 2 * BOX - n, 1) for n in (1, 2, 3))
    step0 = m0 / m1
    fresh = m0 - 2.0 * step0 * m1 + step0 * step0 * m2
    u = 1.0 + fresh / m0 - step0 * SHIFT
    curve = u * u * m1 - 2.0 * u * step0 * (m2 - SHIFT * m1) + step0 * step0 * m3
    step1 = fresh / curve
    low_part, high_part = step0 + step1 * u, step1 * step0
    for t in range(3):
        a = jnp.broadcast_to(low_part[:, 4 * t : 4 * t + 1], (8, 2 * BOX))
        e = jnp.broadcast_to(high_part[:, 4 * t : 4 * t + 1], (8, 2 * BOX))
        for half in (0, 8):
            rows = slice(16 * t + half, 16 * t + half + 8)
            b, ab = vec[0, :, rows, :], image[0, :, rows, :]
            response[:, rows, :] = a * b - e * vec[1, :, rows, :]
            residual[:, rows, :] = b - a * ab + e * image[1, :, rows, :]

    for p in range(4):
        ring_up(p).wait_send()
        ring_down(p).wait_send()
    for p in range(2):
        ring(3, 2, p, up, 8 + p).wait_send()
    for p in range(2, 4):
        ring(1, 2, p, down, 8 + p).wait_send()


def run(*args):
    grid_f = pltpu.VMEM((BOX, 16, 2 * BOX), F32)
    three_f = pltpu.VMEM((3, BOX, 16, 2 * BOX), F32)
    six_b = pltpu.VMEM((2, 3, BOX, 16, 2 * BOX), BF16)
    natural = (KEPT, 48, 2 * BOX)
    dma = pltpu.SemaphoreType.DMA
    return pl.pallas_call(
        kernel,
        out_shape=(shape(natural), shape(natural)),
        in_specs=[pl.BlockSpec(memory_space=pl.ANY)] + [vmem] * 3 + [smem] * 2 + [vmem] * 6,
        out_specs=(vmem, vmem),
        scratch_shapes=[
            pltpu.VMEM((4, 64, BOX, 2 * BOX), BF16),
            pltpu.VMEM((4, BOX, 2 * BOX), F32),
            pltpu.VMEM((KEPT, 16, 2 * BOX), F32),
            pltpu.VMEM((KEPT, 16, 2 * BOX), F32),
            pltpu.VMEM((KEPT, 16, 2 * BOX), F32),
            pltpu.VMEM((NPERT, BOX, 8, 2 * BOX), F32),
            pltpu.VMEM((BOX, 8, 2 * BOX), F32),
            pltpu.VMEM((16 * STEP, 2 * BOX), F32),
            pltpu.VMEM((3, 8, 2 * BOX), F32),
            pltpu.VMEM((64 * STEP, 2 * BOX), F32),
            pltpu.VMEM((4, 4, ROWS, 64, 2 * BOX), BF16),
            grid_f, grid_f, grid_f,
            grid_f, grid_f, three_f, three_f, six_b, six_b, six_b, six_b,
            pltpu.VMEM((ROWS, 96, 2 * BOX), BF16),
            pltpu.VMEM((ROWS, 48, 2 * BOX), F32),
            pltpu.VMEM((3, 24, 256), BF16),
            pltpu.VMEM((3, 16, 24, 256), BF16),
            pltpu.VMEM(natural, F32),
            pltpu.VMEM((3, *natural), F32),
            pltpu.VMEM((2, *natural), F32),
            pltpu.VMEM((8, 2 * BOX), F32),
            pltpu.VMEM((8, 2 * BOX), F32),
            pltpu.VMEM((16, 8, 2 * BOX), F32),
            dma((4,)), dma((12,)), dma((4, 4)), dma((2,)), dma((3,)), dma((3,)),
            dma((2, 3)), dma((2, 3)), dma((2, 3)), dma((2, 3)), dma((3,)), dma((3,)), dma((2,)),
        ],
        compiler_params=pltpu.CompilerParams(
            vmem_limit_bytes=VMEM_LIMIT, collective_id=0, has_side_effects=True
        ),
    )(*args)


def place_body(response, residual, *outs):
    for src, out in zip((response, residual), outs):
        flat = src.reshape(KEPT * 16, 2 * BOX)
        for i in range(2):
            for k in range(2):
                for q in range(4):
                    line = flat[pl.ds(8 * i + 4 * k + q, KEPT, stride=16), :]
                    out[q, 0, 2 * k + i, 0 : GCUT + 1] = line[: GCUT + 1]
                    out[q, 0, 2 * k + i, GCUT + 1 : BOX - GCUT] = jnp.zeros((BOX - KEPT, 2 * BOX), F32)
                    out[q, 0, 2 * k + i, BOX - GCUT :] = line[GCUT + 1 :]


def place(*values):
    out = shape((4, NPERT, 4, BOX, 2 * BOX))
    return pl.pallas_call(
        place_body,
        grid=(NPERT,),
        out_shape=(out, out),
        in_specs=[pl.BlockSpec((KEPT, 16, 2 * BOX), lambda t: (0, t, 0))] * 2,
        out_specs=(pl.BlockSpec((4, 1, 4, BOX, 2 * BOX), lambda t: (0, t, 0, 0, 0)),) * 2,
    )(*values)


def on_device(psi_occ, energies, k_point, g_mask, v_local, dv):
    response, residual = run(
        psi_occ, g_mask, v_local, dv, energies, k_point, *lane_tables(),
        jnp.asarray(fold_table(), BF16), jnp.asarray(spread_table(), BF16),
    )

    return place(response, residual)


def solution(mesh):
    placed = (
        P(("pool", "band"), "ga", None, None),
        P(("pool", "band")),
        P("pool"),
        P(("pool", "ga"), None),
        P(None, "ga"),
        P(None, None, "ga"),
    )
    return jax.shard_map(
        on_device,
        mesh=mesh,
        in_specs=placed,
        out_specs=(
            P(("pool", "band"), None, "ga", None, None),
            P(("pool", "band"), None, "ga", None, None),
        ),
        check_vma=False,
    )
```

```python
import functools
import math

import jax
import jax.numpy as jnp
import numpy as np
from jax import lax
from jax.experimental import pallas as pl
from jax.experimental.pallas import tpu as pltpu
from jax.sharding import PartitionSpec as P

BOX = 64
GCUT = 21
KEPT = 2 * GCUT + 1
NPERT = 3
STRIDE = 16
SHIFT = 16.0
ROWS = 24

cell_length = 16.5
shift_weight = 8.0

kept_freqs = list(range(GCUT + 1)) + list(range(-GCUT, 0))
place_of = {f: i for i, f in enumerate(kept_freqs)}
F32 = jnp.float32
BF16 = jnp.bfloat16


def add(a, b):
    if a is None:
        return b
    if b is None:
        return a
    return (a[0] + b[0], a[1] + b[1])


def sub(a, b):
    if b is None:
        return a
    if a is None:
        return (-b[0], -b[1])
    return (a[0] - b[0], a[1] - b[1])


def times_phase(a, turns, sign):
    if a is None:
        return None
    turns = turns % 1.0
    re, im = a
    if turns == 0.0:
        return a
    if turns == 0.5:
        return (-re, -im)
    if turns in (0.25, 0.75):
        if (turns == 0.25) == (sign > 0):
            return (-im, re)
        return (im, -re)
    c, s = math.cos(2 * math.pi * turns), sign * math.sin(2 * math.pi * turns)
    if turns in (0.125, 0.375, 0.625, 0.875):
        h = abs(c)
        if (c > 0) == (s > 0):
            pair = ((re - im) * h, (re + im) * h)
        else:
            pair = ((re + im) * h, (im - re) * h)
        return pair if c > 0 else (-pair[0], -pair[1])
    return (re * c - im * s, im * c + re * s)


def small_dft(xs, sign):
    n = len(xs)
    if n == 1:
        return xs
    even, odd = small_dft(xs[0::2], sign), small_dft(xs[1::2], sign)
    turned = [times_phase(o, k / n, sign) for k, o in enumerate(odd)]
    return [add(e, o) for e, o in zip(even, turned)] + [sub(e, o) for e, o in zip(even, turned)]


def dft64(load, keep, tmp, store, sign):
    for n2 in range(8):
        out = small_dft([load(8 * n1 + n2) for n1 in range(8)], sign)
        for k1 in range(8):
            re, im = times_phase(out[k1], n2 * k1 / 64.0, sign)
            tmp[8 * n2 + k1, 0:8] = re
            tmp[8 * n2 + k1, 8:16] = im
    for k1 in range(8):
        if not any((k1 + 8 * k2) in keep for k2 in range(8)):
            continue
        out = small_dft([(tmp[8 * n2 + k1, 0:8], tmp[8 * n2 + k1, 8:16]) for n2 in range(8)], sign)
        for k2 in range(8):
            if (k1 + 8 * k2) in keep:
                store(k1 + 8 * k2, out[k2])


def corner_turn(block):
    front = lax.broadcasted_iota(jnp.int32, (8, 2 * BOX), 1) < BOX
    top = lax.broadcasted_iota(jnp.int32, (8, 2 * BOX), 0) < 4
    half = []
    for h in range(2):
        a, b = block[2 * h], block[2 * h + 1]
        half.append(
            (
                jnp.where(front, a, pltpu.roll(b, BOX, 1)),
                jnp.where(front, pltpu.roll(a, BOX, 1), b),
            )
        )
    out = [None] * 4
    for i in range(2):
        a, b = half[0][i], half[1][i]
        out[i] = jnp.where(top, a, pltpu.roll(b, 4, 0))
        out[2 + i] = jnp.where(top, pltpu.roll(a, 4, 0), b)
    return out


def turn_in(src, dst):
    for s in range(16):
        tiles = [src[4 * s + c].astype(F32) for c in range(4)]
        re = corner_turn([t[0:8] for t in tiles])
        im = corner_turn([t[8:16] for t in tiles])
        for c in range(4):
            dst[4 * s + c, 0:8] = re[c]
            dst[4 * s + c, 8:16] = im[c]


def pair(ref):
    return lambda n: (ref[n, 0:8], ref[n, 8:16])


def put_pair(ref, rows, dtype):
    def store(n, value):
        ref[n, rows] = jnp.concatenate([value[0], value[1]], axis=0).astype(dtype)

    return store


def split_dot(x, high, low):
    hi = x.astype(BF16)
    lo = (x - hi.astype(F32)).astype(BF16)
    dot = functools.partial(jnp.dot, preferred_element_type=F32)
    return dot(hi, high) + dot(lo, high) + dot(hi, low)


def lanes_forward(src, first_row, high, low, dst):
    a = src[:, pl.ds(first_row, 8), :].reshape(KEPT * 8, 2 * BOX)
    b = src[:, pl.ds(first_row + 8, 8), :].reshape(KEPT * 8, 2 * BOX)
    out = split_dot(jnp.concatenate([a, b], axis=1), high, low)
    dst[0:KEPT, 0:8, :] = out[:, : 2 * BOX].reshape(KEPT, 8, 2 * BOX)
    dst[0:KEPT, 8:16, :] = out[:, 2 * BOX :].reshape(KEPT, 8, 2 * BOX)


def lanes_back(src, high, low):
    x = jnp.concatenate(
        [
            src[0:KEPT, 0:8, :].reshape(KEPT * 8, 2 * BOX),
            src[0:KEPT, 8:16, :].reshape(KEPT * 8, 2 * BOX),
        ],
        axis=1,
    )
    out = split_dot(x, high, low)
    return (
        out[:, : 2 * BOX].reshape(KEPT, 8, 2 * BOX),
        out[:, 2 * BOX :].reshape(KEPT, 8, 2 * BOX),
    )


def lane_tables():
    index = np.arange(BOX)
    angle = (index[:, None] * index[None, :] % BOX) * (2.0 * np.pi / BOX)
    c, s, z = np.cos(angle), np.sin(angle), np.zeros((BOX, BOX))
    forward = np.block([[c, z, s, z], [-s, z, c, z], [z, c, z, s], [z, -s, z, c]])
    s = -s
    back = np.block([[c, s, z, z], [z, z, c, s], [-s, c, z, z], [z, z, -s, c]])
    out = []
    for w in (forward, back):
        w = jnp.asarray(w, F32)
        high = w.astype(BF16)
        out += [high, (w - high.astype(F32)).astype(BF16)]
    return out


kept_place = lambda n: n if n <= GCUT else (n - (BOX - KEPT) if n >= BOX - GCUT else None)
KEPT_SET = frozenset(f % BOX for f in kept_freqs)
ALL_SET = frozenset(range(BOX))


def load_kept(ref):
    def load(n):
        place = kept_place(n)
        return None if place is None else (ref[place, 0:8], ref[place, 8:16])

    return load


def forward_tile(src, first_row, high, low, near, tmp, store):
    lanes_forward(src, first_row, high, low, near)
    dft64(load_kept(near), ALL_SET, tmp, store, 1)


def back_tile(src, high, low, near, tmp):
    turn_in(src, near)

    def store(n, value):
        tmp2 = near
        tmp2[kept_place(n), 0:8] = value[0]
        tmp2[kept_place(n), 8:16] = value[1]

    dft64(pair(near), KEPT_SET, tmp, store, -1)
    return lanes_back(near, high, low)


def front_lanes(shape):
    return lax.broadcasted_iota(jnp.int32, shape, len(shape) - 1) % BOX < BOX // 2


def widest(f):
    return int(math.sqrt(GCUT**2 - max(abs(f) - 0.5, 0.0) ** 2) + 0.5)


def lay_rows():
    order = sorted(kept_freqs, key=lambda f: (abs(f), -f))
    hosts, others = order[:ROWS], order[ROWS:]
    room = [[widest(f) + 1, BOX - 1 - widest(f)] for f in hosts]
    pieces = sorted(
        [(widest(f) + 1, f, True) for f in others] + [(widest(f), f, False) for f in others],
        key=lambda piece: -piece[0],
    )
    guests, where = [[] for _ in hosts], {}
    for size, f, ahead in pieces:
        fits = [r for r in range(ROWS) if room[r][1] - room[r][0] + 1 >= size]
        r = min(fits, key=lambda n: (room[n][1] - room[n][0] + 1 - size, n))
        start = room[r][0]
        shift = start if ahead else start - (BOX - size)
        room[r][0] = start + size
        guests[r].append((f, ahead, shift % (2 * BOX)))
        where[f, ahead] = (r, shift % (2 * BOX))
    return hosts, guests, where


hosts, guests, where_laid = lay_rows()


def pack_row(get, r):
    value = get(hosts[r])
    front = front_lanes(value.shape)
    for f, ahead, shift in guests[r]:
        row = get(f)
        piece = jnp.where(front, row, 0.0) if ahead else jnp.where(front, 0.0, row)
        value = value + pltpu.roll(piece, shift, value.ndim - 1)
    return value


def unpack_row(get, f):
    if f in hosts:
        return get(hosts.index(f))
    (r, up), (n, down) = where_laid[f, True], where_laid[f, False]
    first, second = get(r), get(n)
    axis = first.ndim - 1
    return jnp.where(
        front_lanes(first.shape),
        pltpu.roll(first, (2 * BOX - up) % (2 * BOX), axis),
        pltpu.roll(second, (2 * BOX - down) % (2 * BOX), axis),
    )


def lane_sign(shape):
    return jnp.where(lax.broadcasted_iota(jnp.int32, shape, len(shape) - 1) < BOX, 1.0, -1.0)


def panel_rows(panel, slots, r, p):
    rows = [jnp.concatenate([panel[d, p, n] for d in slots], axis=0) for n in (r, r + 1)]
    return jnp.concatenate(rows, axis=1)


def pack_values(values, packed):
    sign = lane_sign((48, 2 * BOX))
    for r in range(ROWS):
        straight = pack_row(lambda f: values[place_of[f]], r)
        turned = pack_row(lambda f: pltpu.roll(values[place_of[f]], BOX, 1) * sign, r)
        packed[r] = jnp.concatenate([straight, turned], axis=0).astype(BF16)


def correlate(packed, panel, fold, slots, planes=(0, 1, 2, 3)):
    count = 64 * len(slots)
    nt = (((1,), (1,)), ((), ()))
    total = {p: None for p in planes}
    for r in range(0, ROWS, 2):
        y = jnp.concatenate([packed[r], packed[r + 1]], axis=1)
        for p in planes:
            part = lax.dot_general(
                panel_rows(panel, slots, r, p), y, nt, preferred_element_type=F32
            )
            total[p] = part if total[p] is None else total[p] + part
    column = lax.broadcasted_iota(jnp.int32, (count, 96), 1) % 16 // 4
    chosen = jnp.zeros((count, 96), F32)
    for p in planes:
        chosen = jnp.where(column == 2 * (p % 2) + p // 2, total[p], chosen)
    hi = chosen.astype(BF16)
    lo = (chosen - hi.astype(F32)).astype(BF16)
    return lax.dot_general(fold, hi, nt, preferred_element_type=F32) + lax.dot_general(
        fold, lo, nt, preferred_element_type=F32
    )


def fold_table():
    f = np.zeros((2, 3, 4, 2, 3, 4, 4), np.float32)
    for a in range(2):
        for t in range(3):
            for q in range(4):
                f[a, t, q, a, t, :, q] = 1.0
    return f.reshape(24, 96)


def spread_table():
    f = np.zeros((4, 2, 3, 2, 2, 4, 2, 3, 4), np.float32)
    for p in range(4):
        for a in range(2):
            for t in range(3):
                for q in range(4):
                    f[p, a, t, p % 2, p // 2, q, a, t, q] = 1.0
    return f.reshape(384, 24)


def multiply(corr, panel, spread, product, slots, more=False):
    rows = jnp.dot(spread[...], corr, preferred_element_type=F32).astype(BF16)
    sign = -lane_sign((48, 2 * BOX))
    for r in range(0, ROWS, 2):
        total = None
        for p in range(4):
            part = jnp.dot(
                rows[96 * p : 96 * p + 96], panel_rows(panel, slots, r, p), preferred_element_type=F32
            )
            total = part if total is None else total + part
        for c in range(2):
            lanes = slice(2 * BOX * c, 2 * BOX * (c + 1))
            value = total[:48, lanes] + pltpu.roll(total[48:, lanes], BOX, 1) * sign
            product[r + c] = product[r + c] + value if more else value


def lay_out(product, finish):
    for f in kept_freqs:
        finish(place_of[f], unpack_row(lambda r: product[r], f))


VMEM_LIMIT = 62 * 1024 * 1024
MESH = pl.DeviceIdType.MESH
vmem = pl.BlockSpec(memory_space=pltpu.VMEM)
smem = pl.BlockSpec(memory_space=pltpu.SMEM)
STEP = 72
SLOTS = (0, 1, 3, 2)


def shape(dims, dtype=F32):
    return jax.ShapeDtypeStruct(dims, dtype)


def remote(src, dst, send, recv, where):
    return pltpu.make_async_remote_copy(
        src_ref=src, dst_ref=dst, send_sem=send, recv_sem=recv, device_id=where, device_id_type=MESH
    )


def away(step):
    return min(step[0], 4 - step[0]) + min(step[1], 4 - step[1])


STEPS = sorted([(y, x) for y in range(4) for x in range(4) if (y, x) != (0, 0)], key=lambda s: -away(s))


def peers(me):
    for dy, dx in STEPS:
        yield 4 * lax.rem(me // 4 + dy, 4) + lax.rem(lax.rem(me, 4) + dx, 4)


def to_peers(me, src_of, dst, send, recv):
    for g in peers(me):
        remote(src_of(g), dst, send, recv, {"ga": g}).start()


def kernel(
    psi, g_mask, v_local, dv, energies, k_point, fwd_hi, fwd_lo, back_hi, back_lo, fold, spread,
    response, residual,
    raw, mask_rows, mask, level, solved, changes, potential, solved_rows, weights, wide_rows, panel, near, tmp, space, send_a, came_a, send_b, came_b, send_1, send_2,
    came_1, came_2, packed, product, share, shares, far_share, far_shares, source, vec, image, sums, sums_here, all_sums,
    raw_sem, ring_send, ring_recv, a_sem, b_send, b_recv, s1, r1, s2, r2, c_send, c_recv, m_sem,
):
    me = lax.axis_index("ga")
    z = lax.axis_index("band")
    up, down = lax.rem(z + 1, 4), lax.rem(z + 3, 4)

    barrier = pltpu.get_barrier_semaphore()

    for g in peers(me):
        pl.semaphore_signal(barrier, inc=1, device_id={"ga": g}, device_id_type=MESH)
    for other in (up, down):
        pl.semaphore_signal(barrier, inc=1, device_id={"band": other}, device_id_type=MESH)

    def raw_copy(p):
        return pltpu.make_async_copy(psi.at[:, p], raw.at[p], raw_sem.at[p])

    for p in range(4):
        raw_copy(p).start()

    front = lax.broadcasted_iota(jnp.int32, (4, 2 * BOX), 1) < BOX
    top = lax.broadcasted_iota(jnp.int32, (8, 2 * BOX), 0) < 4
    for c in range(BOX // 2):
        both = g_mask[:, 2 * BOX * c : 2 * BOX * (c + 1)].astype(F32)
        turned = pltpu.roll(both, BOX, 1)
        for n, rows in ((2 * c, jnp.where(front, both, turned)), (2 * c + 1, jnp.where(front, turned, both))):
            for p in range(4):
                mask_rows[p, n : n + 1] = rows[p : p + 1]

    def spread_rows(first, second):
        return jnp.where(top, jnp.broadcast_to(first, (8, 2 * BOX)), jnp.broadcast_to(second, (8, 2 * BOX)))

    def pack_plane(u, carry):
        p = 2 * lax.rem(u, 2) + u // 2
        raw_copy(p).wait()

        def widen(m, c):
            wide_rows[pl.ds(pl.multiple_of(STEP * m, 8), BOX), :] = raw[p, m].astype(F32)
            return c

        lax.fori_loop(0, 64, widen, 0)

        def get(f):
            n = f % BOX
            return wide_rows[pl.ds(n, 64, stride=STEP), :] * mask_rows[p, n : n + 1]

        for r in range(ROWS):
            panel[0, p, r] = pack_row(get, r).astype(BF16)
        return carry

    lax.fori_loop(0, 2, pack_plane, 0)
    pl.semaphore_wait(barrier, 17)

    def ring(src_slot, dst_slot, p, where, n):
        return remote(
            panel.at[src_slot, p], panel.at[dst_slot, p], ring_send.at[n], ring_recv.at[dst_slot, p],
            {"band": where},
        )

    def ring_up(p):
        return ring(0, 3, p, up, p)

    def ring_down(p):
        return ring(0, 1, p, down, 4 + p)

    ring_up(0).start()
    ring_down(2).start()
    lax.fori_loop(2, 4, pack_plane, 0)
    ring_up(1).start()
    ring_down(3).start()
    ring_up(2).start()
    ring_down(0).start()
    ring_up(3).start()
    ring_down(1).start()

    for i in range(2):
        for k in range(2):
            for q in range(4):
                solved_rows[pl.ds(STEP * (8 * i + 4 * k + q), BOX), :] = raw[2 * k + i, STRIDE * q].astype(F32)
    for f in kept_freqs:
        n = f % BOX
        for i in range(2):
            rows = mask_rows[i, n : n + 1], mask_rows[2 + i, n : n + 1]
            mask[place_of[f], 8 * i : 8 * i + 8] = spread_rows(*rows)
        solved[place_of[f]] = solved_rows[pl.ds(n, 16, stride=STEP), :] * mask[place_of[f]]
    forward_tile(solved, 0, fwd_hi[...], fwd_lo[...], near, tmp, put_pair(send_a, slice(0, 16), F32))

    mine = pl.ds(4 * me, 4)
    to_peers(me, lambda g: send_a.at[pl.ds(4 * g, 4)], came_a.at[mine], a_sem.at[0], a_sem.at[1])
    came_a[mine] = send_a[mine]

    def spread_field(n, carry):
        line = v_local[pl.ds(n, 1), :]
        potential[n] = spread_rows(line[:, : 2 * BOX], line[:, 2 * BOX :])
        for p in range(NPERT):
            line = dv[p, pl.ds(n, 1), :]
            changes[p, n] = spread_rows(line[:, : 2 * BOX], line[:, 2 * BOX :])
        return carry

    lax.fori_loop(0, BOX, spread_field, 0)

    factor = 0.5 * (2.0 * math.pi / cell_length) ** 2
    row = lax.broadcasted_iota(jnp.int32, (8, 2 * BOX), 0)
    third = lax.broadcasted_iota(jnp.int32, (8, 2 * BOX), 1) % BOX
    third = jnp.where(third < BOX // 2, third, third - BOX).astype(F32)
    for i in range(2):
        first = 4 * me + 2 * (row // 4) + i
        first = jnp.where(first < BOX // 2, first, first - BOX).astype(F32)
        still = factor * ((first + k_point[0]) ** 2 + (third + k_point[2]) ** 2)
        for q in range(4):
            still = jnp.where(row % 4 == q, still - energies[q], still)
        for f in kept_freqs:
            here = mask[place_of[f], 8 * i : 8 * i + 8]
            rise = factor * (float(f) + k_point[1]) * (float(f) + k_point[1])
            level[place_of[f], 8 * i : 8 * i + 8] = (still + rise) * here
            mask[place_of[f], 8 * i : 8 * i + 8] = here * (1.0 / BOX**3)

    def wait_all(src, dst, send, recv):
        return remote(src, dst, send, recv, {"ga": lax.rem(me + 1, 16)})

    every = pl.ds(0, 60)
    wait_all(send_a.at[every], came_a.at[every], a_sem.at[0], a_sem.at[1]).wait()

    turn_in(came_a, near)

    def keep(n, value):
        space[n, 0:8] = value[0]
        space[n, 8:16] = value[1]

    dft64(pair(near), ALL_SET, tmp, keep, 1)

    def each_change(p, carry):
        def load(n):
            d = changes[p, n]
            return (space[n, 0:8] * d, space[n, 8:16] * d)

        dft64(load, ALL_SET, tmp, put_pair(send_b.at[p], slice(0, 16), F32), -1)
        to_peers(
            me, lambda g: send_b.at[p, pl.ds(4 * g, 4)], came_b.at[p, mine], b_send.at[p], b_recv.at[p]
        )
        came_b[p, mine] = send_b[p, mine]
        return carry

    lax.fori_loop(0, NPERT, each_change, 0)

    def pass_on(p_up, p_down):
        ring(0, 3, p_up, up, p_up).wait_recv()
        first = ring(3, 2, p_up, up, 8 + p_up)
        first.start()
        ring(0, 1, p_down, down, 4 + p_down).wait_recv()
        second = ring(1, 2, p_down, down, 8 + p_down)
        second.start()

    pass_on(0, 2)
    pass_on(1, 3)

    def back(came, dst_add):
        def each(t, carry):
            dst_add(t)
            return carry

        lax.fori_loop(0, 3, each, 0)

    def source_tile(t):
        wait_all(send_b.at[t, every], came_b.at[t, every], b_send.at[t], b_recv.at[t]).wait()
        start = pl.multiple_of(16 * t, 16)
        a, b = back_tile(came_b.at[t], back_hi[...], back_lo[...], near, tmp)
        source[:, pl.ds(start, 8), :] = a * mask[:, 0:8, :]
        source[:, pl.ds(start + 8, 8), :] = b * mask[:, 8:16, :]

    back(came_b, source_tile)

    def send_share(n, src):
        to_peers(me, lambda g: src, shares.at[n, me], c_send.at[n], c_recv.at[n])

    def total_share(n):
        first = pl.ds(0, 15)
        wait_all(shares.at[n, first], shares.at[n, first], c_send.at[n], c_recv.at[n]).wait()
        total = shares[n, 0].astype(F32)
        for g in range(1, 16):
            total = total + shares[n, g].astype(F32)
        return total.astype(BF16)

    pack_values(source, packed)
    for p in range(2, 4):
        ring(0, 3, p, up, p).wait_recv()
    for p in range(2):
        ring(0, 1, p, down, 4 + p).wait_recv()
    early = correlate(packed, panel, fold[...], SLOTS[:3]).astype(BF16)
    share[0] = jnp.concatenate([early, jnp.zeros((24, 64), BF16)], axis=1)
    shares[0, me] = share[0]
    send_share(0, share.at[0])
    ring(3, 2, 0, up, 8).wait_recv()
    ring(1, 2, 2, down, 10).wait_recv()
    late = correlate(packed, panel, fold[...], SLOTS[3:], (0, 2))
    multiply(total_share(0)[:, :192], panel, spread, product, SLOTS[:3])
    ring(3, 2, 1, up, 9).wait_recv()
    ring(1, 2, 3, down, 11).wait_recv()
    late = late + correlate(packed, panel, fold[...], SLOTS[3:], (1, 3))
    far_share[...] = jnp.concatenate([late.astype(BF16), jnp.zeros((24, 64), BF16)], axis=1)
    far_shares[me] = far_share[...]
    to_peers(me, lambda g: far_share, far_shares.at[me], c_send.at[3], c_recv.at[3])

    def first_row(place, row):
        for t in range(3):
            rows = slice(16 * t, 16 * t + 16)
            vec[0, place, rows] = row[rows] * mask[place] - source[place, rows]

    first = pl.ds(0, 15)
    wait_all(far_shares.at[first], far_shares.at[first], c_send.at[3], c_recv.at[3]).wait()
    total = far_shares[0].astype(F32)
    for g in range(1, 16):
        total = total + far_shares[g].astype(F32)
    multiply(total.astype(BF16)[:, :64], panel, spread, product, SLOTS[3:], True)
    lay_out(product, first_row)

    lane = lax.broadcasted_iota(jnp.int32, (8, 2 * BOX), 1)

    def apply(it, carry):
        def near_tile(t, c):
            start = pl.multiple_of(16 * t, 16)
            forward_tile(
                vec.at[it], start, fwd_hi[...], fwd_lo[...], near, tmp,
                put_pair(send_1.at[it, t], slice(0, 16), BF16),
            )
            to_peers(
                me, lambda g: send_1.at[it, t, pl.ds(4 * g, 4)], came_1.at[it, t, mine],
                s1.at[it, t], r1.at[it, t],
            )
            came_1[it, t, mine] = send_1[it, t, mine]
            return c

        lax.fori_loop(0, 3, near_tile, 0)

        pack_values(vec.at[it], packed)
        n = it + 1
        share[n] = correlate(packed, panel, fold[...], SLOTS).astype(BF16)
        shares[n, me] = share[n]
        send_share(n, share.at[n])

        def space_tile(t, c):
            wait_all(send_1.at[it, t, every], came_1.at[it, t, every], s1.at[it, t], r1.at[it, t]).wait()
            turn_in(came_1.at[it, t], near)

            weight = [jnp.zeros((8, 2 * BOX), F32)]

            def with_potential(k, value):
                v = potential[k]
                re, im = value[0] * v, value[1] * v
                near[k, 0:8] = re
                near[k, 8:16] = im
                weight[0] = weight[0] + (value[0] * re + value[1] * im)

            dft64(pair(near), ALL_SET, tmp, with_potential, 1)
            weights[t] = weight[0]
            dft64(pair(near), ALL_SET, tmp, put_pair(send_2.at[it, t], slice(0, 16), BF16), -1)
            to_peers(
                me, lambda g: send_2.at[it, t, pl.ds(4 * g, 4)], came_2.at[it, t, mine],
                s2.at[it, t], r2.at[it, t],
            )
            came_2[it, t, mine] = send_2[it, t, mine]
            return c

        lax.fori_loop(0, 3, space_tile, 0)

        def with_level(place, row):
            for t in range(3):
                rows = slice(16 * t, 16 * t + 16)
                image[it, place, rows] = (
                    row[rows] * (shift_weight * mask[place])
                    + level[place] * vec[it, place, rows]
                )

        corr = total_share(n)

        @pl.when(it == 1)
        def _():
            def moments(place, totals):
                b, ab, w = vec[0, place], image[0, place], vec[1, place]
                lift = jnp.concatenate([level[place]] * 3, axis=0)
                return tuple(x + y for x, y in zip(totals, (b * b, b * ab, ab * ab, lift * w * w)))

            zero = jnp.zeros((48, 2 * BOX), F32)
            totals = lax.fori_loop(0, KEPT, moments, (zero,) * 4)
            own = jnp.zeros((8, 2 * BOX), F32)
            for m, total in enumerate(totals):
                line = jnp.sum(total, axis=1, keepdims=True) * (1.0 / BOX**3)
                for t in range(3):
                    both = line[16 * t : 16 * t + 8] + line[16 * t + 8 : 16 * t + 16]
                    if m == 3:
                        both = both + jnp.sum(weights[t], axis=1, keepdims=True) * (1.0 / BOX**6)
                    own = jnp.where(lane == 4 * t + m, jnp.broadcast_to(both, own.shape), own)
            own = own + pltpu.roll(own, 4, 0)
            sums[...] = own
            all_sums[me] = own
            to_peers(me, lambda g: sums, all_sums.at[me], m_sem.at[0], m_sem.at[1])
            square = corr.astype(F32)
            square = jnp.sum(square * square, axis=1, keepdims=True) * (shift_weight / BOX**6)
            rest = jnp.zeros((8, 2 * BOX), F32)
            for t in range(3):
                four = square[4 * t : 4 * t + 4] + square[12 + 4 * t : 16 + 4 * t]
                eight = jnp.concatenate([four, four], axis=0)
                rest = jnp.where(lane == 4 * t + 3, jnp.broadcast_to(eight, rest.shape), rest)
            sums_here[...] = rest

        multiply(corr, panel, spread, product, SLOTS)
        lay_out(product, with_level)

        def far_tile(t, c):
            wait_all(send_2.at[it, t, every], came_2.at[it, t, every], s2.at[it, t], r2.at[it, t]).wait()
            start = pl.multiple_of(16 * t, 16)
            a, b = back_tile(came_2.at[it, t], back_hi[...], back_lo[...], near, tmp)
            for half, value in ((0, a), (8, b)):
                rows = pl.ds(start + half, 8)
                total = image[it, :, rows, :] + value * mask[:, half : half + 8, :]
                image[it, :, rows, :] = total
                vec[it + 1, :, rows, :] = total - SHIFT * vec[it, :, rows, :]
            return c

        lax.fori_loop(0, 3, far_tile, 0)
        return carry

    lax.fori_loop(0, 2, apply, 0)

    first = pl.ds(0, 15)
    wait_all(all_sums.at[first], all_sums.at[first], m_sem.at[0], m_sem.at[1]).wait()
    m0 = sums_here[...] + all_sums[0]
    for g in range(1, 16):
        m0 = m0 + all_sums[g]
    m1, m2, m3 = (pltpu.roll(m0, 2 * BOX - n, 1) for n in (1, 2, 3))
    step0 = m0 / m1
    fresh = m0 - 2.0 * step0 * m1 + step0 * step0 * m2
    u = 1.0 + fresh / m0 - step0 * SHIFT
    curve = u * u * m1 - 2.0 * u * step0 * (m2 - SHIFT * m1) + step0 * step0 * m3
    step1 = fresh / curve
    low_part, high_part = step0 + step1 * u, step1 * step0
    for t in range(3):
        a = jnp.broadcast_to(low_part[:, 4 * t : 4 * t + 1], (8, 2 * BOX))
        e = jnp.broadcast_to(high_part[:, 4 * t : 4 * t + 1], (8, 2 * BOX))
        for half in (0, 8):
            rows = slice(16 * t + half, 16 * t + half + 8)
            b, ab = vec[0, :, rows, :], image[0, :, rows, :]
            response[:, rows, :] = a * b - e * vec[1, :, rows, :]
            residual[:, rows, :] = b - a * ab + e * image[1, :, rows, :]

    for p in range(4):
        ring_up(p).wait_send()
        ring_down(p).wait_send()
    for p in range(2):
        ring(3, 2, p, up, 8 + p).wait_send()
    for p in range(2, 4):
        ring(1, 2, p, down, 8 + p).wait_send()


def run(*args):
    grid_f = pltpu.VMEM((BOX, 16, 2 * BOX), F32)
    three_f = pltpu.VMEM((3, BOX, 16, 2 * BOX), F32)
    six_b = pltpu.VMEM((2, 3, BOX, 16, 2 * BOX), BF16)
    natural = (KEPT, 48, 2 * BOX)
    dma = pltpu.SemaphoreType.DMA
    return pl.pallas_call(
        kernel,
        out_shape=(shape(natural), shape(natural)),
        in_specs=[pl.BlockSpec(memory_space=pl.ANY)] + [vmem] * 3 + [smem] * 2 + [vmem] * 6,
        out_specs=(vmem, vmem),
        scratch_shapes=[
            pltpu.VMEM((4, 64, BOX, 2 * BOX), BF16),
            pltpu.VMEM((4, BOX, 2 * BOX), F32),
            pltpu.VMEM((KEPT, 16, 2 * BOX), F32),
            pltpu.VMEM((KEPT, 16, 2 * BOX), F32),
            pltpu.VMEM((KEPT, 16, 2 * BOX), F32),
            pltpu.VMEM((NPERT, BOX, 8, 2 * BOX), F32),
            pltpu.VMEM((BOX, 8, 2 * BOX), F32),
            pltpu.VMEM((16 * STEP, 2 * BOX), F32),
            pltpu.VMEM((3, 8, 2 * BOX), F32),
            pltpu.VMEM((64 * STEP, 2 * BOX), F32),
            pltpu.VMEM((4, 4, ROWS, 64, 2 * BOX), BF16),
            grid_f, grid_f, grid_f,
            grid_f, grid_f, three_f, three_f, six_b, six_b, six_b, six_b,
            pltpu.VMEM((ROWS, 96, 2 * BOX), BF16),
            pltpu.VMEM((ROWS, 48, 2 * BOX), F32),
            pltpu.VMEM((3, 24, 256), BF16),
            pltpu.VMEM((3, 16, 24, 256), BF16),
            pltpu.VMEM((24, 128), BF16),
            pltpu.VMEM((16, 24, 128), BF16),
            pltpu.VMEM(natural, F32),
            pltpu.VMEM((3, *natural), F32),
            pltpu.VMEM((2, *natural), F32),
            pltpu.VMEM((8, 2 * BOX), F32),
            pltpu.VMEM((8, 2 * BOX), F32),
            pltpu.VMEM((16, 8, 2 * BOX), F32),
            dma((4,)), dma((12,)), dma((4, 4)), dma((2,)), dma((3,)), dma((3,)),
            dma((2, 3)), dma((2, 3)), dma((2, 3)), dma((2, 3)), dma((4,)), dma((4,)), dma((2,)),
        ],
        compiler_params=pltpu.CompilerParams(
            vmem_limit_bytes=VMEM_LIMIT, collective_id=0, has_side_effects=True
        ),
    )(*args)


def place_body(response, residual, *outs):
    for src, out in zip((response, residual), outs):
        flat = src.reshape(KEPT * 16, 2 * BOX)
        for i in range(2):
            for k in range(2):
                for q in range(4):
                    line = flat[pl.ds(8 * i + 4 * k + q, KEPT, stride=16), :]
                    out[q, 0, 2 * k + i, 0 : GCUT + 1] = line[: GCUT + 1]
                    out[q, 0, 2 * k + i, GCUT + 1 : BOX - GCUT] = jnp.zeros((BOX - KEPT, 2 * BOX), F32)
                    out[q, 0, 2 * k + i, BOX - GCUT :] = line[GCUT + 1 :]


def place(*values):
    out = shape((4, NPERT, 4, BOX, 2 * BOX))
    return pl.pallas_call(
        place_body,
        grid=(NPERT,),
        out_shape=(out, out),
        in_specs=[pl.BlockSpec((KEPT, 16, 2 * BOX), lambda t: (0, t, 0))] * 2,
        out_specs=(pl.BlockSpec((4, 1, 4, BOX, 2 * BOX), lambda t: (0, t, 0, 0, 0)),) * 2,
    )(*values)


def on_device(psi_occ, energies, k_point, g_mask, v_local, dv):
    response, residual = run(
        psi_occ, g_mask, v_local, dv, energies, k_point, *lane_tables(),
        jnp.asarray(fold_table(), BF16), jnp.asarray(spread_table(), BF16),
    )

    return place(response, residual)


def solution(mesh):
    placed = (
        P(("pool", "band"), "ga", None, None),
        P(("pool", "band")),
        P("pool"),
        P(("pool", "ga"), None),
        P(None, "ga"),
        P(None, None, "ga"),
    )
    return jax.shard_map(
        on_device,
        mesh=mesh,
        in_specs=placed,
        out_specs=(
            P(("pool", "band"), None, "ga", None, None),
            P(("pool", "band"), None, "ga", None, None),
        ),
        check_vma=False,
    )
```

```python
import functools
import math

import jax
import jax.numpy as jnp
import numpy as np
from jax import lax
from jax.experimental import pallas as pl
from jax.experimental.pallas import tpu as pltpu
from jax.sharding import PartitionSpec as P

BOX = 64
GCUT = 21
KEPT = 2 * GCUT + 1
NPERT = 3
STRIDE = 16
SHIFT = 16.0
ROWS = 24

cell_length = 16.5
shift_weight = 8.0

kept_freqs = list(range(GCUT + 1)) + list(range(-GCUT, 0))
place_of = {f: i for i, f in enumerate(kept_freqs)}
F32 = jnp.float32
BF16 = jnp.bfloat16


def add(a, b):
    if a is None:
        return b
    if b is None:
        return a
    return (a[0] + b[0], a[1] + b[1])


def sub(a, b):
    if b is None:
        return a
    if a is None:
        return (-b[0], -b[1])
    return (a[0] - b[0], a[1] - b[1])


def times_phase(a, turns, sign):
    if a is None:
        return None
    turns = turns % 1.0
    re, im = a
    if turns == 0.0:
        return a
    if turns == 0.5:
        return (-re, -im)
    if turns in (0.25, 0.75):
        if (turns == 0.25) == (sign > 0):
            return (-im, re)
        return (im, -re)
    c, s = math.cos(2 * math.pi * turns), sign * math.sin(2 * math.pi * turns)
    if turns in (0.125, 0.375, 0.625, 0.875):
        h = abs(c)
        if (c > 0) == (s > 0):
            pair = ((re - im) * h, (re + im) * h)
        else:
            pair = ((re + im) * h, (im - re) * h)
        return pair if c > 0 else (-pair[0], -pair[1])
    return (re * c - im * s, im * c + re * s)


def small_dft(xs, sign):
    n = len(xs)
    if n == 1:
        return xs
    even, odd = small_dft(xs[0::2], sign), small_dft(xs[1::2], sign)
    turned = [times_phase(o, k / n, sign) for k, o in enumerate(odd)]
    return [add(e, o) for e, o in zip(even, turned)] + [sub(e, o) for e, o in zip(even, turned)]


def dft64(load, keep, tmp, store, sign):
    for n2 in range(8):
        out = small_dft([load(8 * n1 + n2) for n1 in range(8)], sign)
        for k1 in range(8):
            re, im = times_phase(out[k1], n2 * k1 / 64.0, sign)
            tmp[8 * n2 + k1, 0:8] = re
            tmp[8 * n2 + k1, 8:16] = im
    for k1 in range(8):
        if not any((k1 + 8 * k2) in keep for k2 in range(8)):
            continue
        out = small_dft([(tmp[8 * n2 + k1, 0:8], tmp[8 * n2 + k1, 8:16]) for n2 in range(8)], sign)
        for k2 in range(8):
            if (k1 + 8 * k2) in keep:
                store(k1 + 8 * k2, out[k2])


def corner_turn(block):
    front = lax.broadcasted_iota(jnp.int32, (8, 2 * BOX), 1) < BOX
    top = lax.broadcasted_iota(jnp.int32, (8, 2 * BOX), 0) < 4
    half = []
    for h in range(2):
        a, b = block[2 * h], block[2 * h + 1]
        half.append(
            (
                jnp.where(front, a, pltpu.roll(b, BOX, 1)),
                jnp.where(front, pltpu.roll(a, BOX, 1), b),
            )
        )
    out = [None] * 4
    for i in range(2):
        a, b = half[0][i], half[1][i]
        out[i] = jnp.where(top, a, pltpu.roll(b, 4, 0))
        out[2 + i] = jnp.where(top, pltpu.roll(a, 4, 0), b)
    return out


def turn_in(src, dst):
    for s in range(16):
        tiles = [src[4 * s + c].astype(F32) for c in range(4)]
        re = corner_turn([t[0:8] for t in tiles])
        im = corner_turn([t[8:16] for t in tiles])
        for c in range(4):
            dst[4 * s + c, 0:8] = re[c]
            dst[4 * s + c, 8:16] = im[c]


def pair(ref):
    return lambda n: (ref[n, 0:8], ref[n, 8:16])


def put_pair(ref, rows, dtype):
    def store(n, value):
        ref[n, rows] = jnp.concatenate([value[0], value[1]], axis=0).astype(dtype)

    return store


def split_dot(x, high, low):
    hi = x.astype(BF16)
    lo = (x - hi.astype(F32)).astype(BF16)
    dot = functools.partial(jnp.dot, preferred_element_type=F32)
    return dot(hi, high) + dot(lo, high) + dot(hi, low)


def lanes_forward(src, first_row, high, low, dst):
    a = src[:, pl.ds(first_row, 8), :].reshape(KEPT * 8, 2 * BOX)
    b = src[:, pl.ds(first_row + 8, 8), :].reshape(KEPT * 8, 2 * BOX)
    out = split_dot(jnp.concatenate([a, b], axis=1), high, low)
    dst[0:KEPT, 0:8, :] = out[:, : 2 * BOX].reshape(KEPT, 8, 2 * BOX)
    dst[0:KEPT, 8:16, :] = out[:, 2 * BOX :].reshape(KEPT, 8, 2 * BOX)


def lanes_back(src, high, low):
    x = jnp.concatenate(
        [
            src[0:KEPT, 0:8, :].reshape(KEPT * 8, 2 * BOX),
            src[0:KEPT, 8:16, :].reshape(KEPT * 8, 2 * BOX),
        ],
        axis=1,
    )
    out = split_dot(x, high, low)
    return (
        out[:, : 2 * BOX].reshape(KEPT, 8, 2 * BOX),
        out[:, 2 * BOX :].reshape(KEPT, 8, 2 * BOX),
    )


def lane_tables():
    index = np.arange(BOX)
    angle = (index[:, None] * index[None, :] % BOX) * (2.0 * np.pi / BOX)
    c, s, z = np.cos(angle), np.sin(angle), np.zeros((BOX, BOX))
    forward = np.block([[c, z, s, z], [-s, z, c, z], [z, c, z, s], [z, -s, z, c]])
    s = -s
    back = np.block([[c, s, z, z], [z, z, c, s], [-s, c, z, z], [z, z, -s, c]])
    grid = np.block([[c, z, -s, z], [z, c, z, -s], [s, z, c, z], [z, s, z, c]])
    out = []
    for w in (forward, back, grid, grid.T):
        w = jnp.asarray(w, F32)
        high = w.astype(BF16)
        out += [high, (w - high.astype(F32)).astype(BF16)]
    return out


kept_place = lambda n: n if n <= GCUT else (n - (BOX - KEPT) if n >= BOX - GCUT else None)
KEPT_SET = frozenset(f % BOX for f in kept_freqs)
ALL_SET = frozenset(range(BOX))


def load_kept(ref):
    def load(n):
        place = kept_place(n)
        return None if place is None else (ref[place, 0:8], ref[place, 8:16])

    return load


def forward_tile(src, first_row, high, low, near, tmp, store):
    lanes_forward(src, first_row, high, low, near)
    dft64(load_kept(near), ALL_SET, tmp, store, 1)


def back_tile(src, high, low, near, tmp):
    turn_in(src, near)

    def store(n, value):
        tmp2 = near
        tmp2[kept_place(n), 0:8] = value[0]
        tmp2[kept_place(n), 8:16] = value[1]

    dft64(pair(near), KEPT_SET, tmp, store, -1)
    return lanes_back(near, high, low)


def squeeze(src, dst):
    front = front_lanes((16, 2 * BOX))
    for g in range(16):
        first, second, third, guest = (src[4 * g + c] for c in range(4))
        ahead = pltpu.roll(jnp.where(front, guest, 0.0), GCUT + 1, 1)
        behind = pltpu.roll(jnp.where(front, 0.0, guest), 2 * BOX - GCUT, 1)
        dst[3 * g] = (first + ahead).astype(BF16)
        dst[3 * g + 1] = (second + behind).astype(BF16)
        dst[3 * g + 2] = third.astype(BF16)


def turn_squeezed(src, dst, valid=None):
    front = front_lanes((16, 2 * BOX))
    for g in range(16):
        tiles = [src[3 * g + c].astype(F32) for c in range(3)]
        ahead = pltpu.roll(tiles[0], 2 * BOX - GCUT - 1, 1)
        tiles.append(jnp.where(front, ahead, pltpu.roll(tiles[1], GCUT, 1)))
        if valid is not None:
            tiles = [t * valid for t in tiles]
        re = corner_turn([t[0:8] for t in tiles])
        im = corner_turn([t[8:16] for t in tiles])
        for c in range(4):
            dst[4 * g + c, 0:8] = re[c]
            dst[4 * g + c, 8:16] = im[c]


def natural_to_pair(src, first_row, dst):
    front = lax.broadcasted_iota(jnp.int32, (8, 2 * BOX), 1) < BOX
    for n in range(KEPT):
        a, b = src[n, pl.ds(first_row, 8), :], src[n, pl.ds(first_row + 8, 8), :]
        dst[n, 0:8] = jnp.where(front, a, pltpu.roll(b, BOX, 1))
        dst[n, 8:16] = jnp.where(front, pltpu.roll(a, BOX, 1), b)


def pair_to_natural(src, n):
    front = lax.broadcasted_iota(jnp.int32, (8, 2 * BOX), 1) < BOX
    re, im = src[n, 0:8], src[n, 8:16]
    return jnp.where(front, re, pltpu.roll(im, BOX, 1)), jnp.where(front, pltpu.roll(re, BOX, 1), im)


def grid_lanes(ref, high, low, valid=None):
    x = [ref[:, h : h + 8, :].reshape(BOX * 8, 2 * BOX) for h in (0, 8)]
    x = jnp.concatenate(x, axis=1).astype(BF16)
    out = jnp.dot(x, high, preferred_element_type=F32) + jnp.dot(x, low, preferred_element_type=F32)
    for h, lanes in ((0, slice(0, 2 * BOX)), (8, slice(2 * BOX, 4 * BOX))):
        part = out[:, lanes].reshape(BOX, 8, 2 * BOX)
        ref[:, h : h + 8, :] = part if valid is None else part * valid[0:8]


def front_lanes(shape):
    return lax.broadcasted_iota(jnp.int32, shape, len(shape) - 1) % BOX < BOX // 2


def widest(f):
    return int(math.sqrt(GCUT**2 - max(abs(f) - 0.5, 0.0) ** 2) + 0.5)


def lay_rows():
    order = sorted(kept_freqs, key=lambda f: (abs(f), -f))
    hosts, others = order[:ROWS], order[ROWS:]
    room = [[widest(f) + 1, BOX - 1 - widest(f)] for f in hosts]
    pieces = sorted(
        [(widest(f) + 1, f, True) for f in others] + [(widest(f), f, False) for f in others],
        key=lambda piece: -piece[0],
    )
    guests, where = [[] for _ in hosts], {}
    for size, f, ahead in pieces:
        fits = [r for r in range(ROWS) if room[r][1] - room[r][0] + 1 >= size]
        r = min(fits, key=lambda n: (room[n][1] - room[n][0] + 1 - size, n))
        start = room[r][0]
        shift = start if ahead else start - (BOX - size)
        room[r][0] = start + size
        guests[r].append((f, ahead, shift % (2 * BOX)))
        where[f, ahead] = (r, shift % (2 * BOX))
    return hosts, guests, where


hosts, guests, where_laid = lay_rows()


def pack_row(get, r):
    value = get(hosts[r])
    front = front_lanes(value.shape)
    for f, ahead, shift in guests[r]:
        row = get(f)
        piece = jnp.where(front, row, 0.0) if ahead else jnp.where(front, 0.0, row)
        value = value + pltpu.roll(piece, shift, value.ndim - 1)
    return value


def unpack_row(get, f):
    if f in hosts:
        return get(hosts.index(f))
    (r, up), (n, down) = where_laid[f, True], where_laid[f, False]
    first, second = get(r), get(n)
    axis = first.ndim - 1
    return jnp.where(
        front_lanes(first.shape),
        pltpu.roll(first, (2 * BOX - up) % (2 * BOX), axis),
        pltpu.roll(second, (2 * BOX - down) % (2 * BOX), axis),
    )


def lane_sign(shape):
    return jnp.where(lax.broadcasted_iota(jnp.int32, shape, len(shape) - 1) < BOX, 1.0, -1.0)


def panel_rows(panel, slots, r, p):
    rows = [jnp.concatenate([panel[d, p, n] for d in slots], axis=0) for n in (r, r + 1)]
    return jnp.concatenate(rows, axis=1)


def pack_values(values, packed):
    sign = lane_sign((48, 2 * BOX))
    for r in range(ROWS):
        straight = pack_row(lambda f: values[place_of[f]], r)
        turned = pack_row(lambda f: pltpu.roll(values[place_of[f]], BOX, 1) * sign, r)
        packed[r] = jnp.concatenate([straight, turned], axis=0).astype(BF16)


def correlate(packed, panel, fold, slots, planes=(0, 1, 2, 3)):
    count = 64 * len(slots)
    nt = (((1,), (1,)), ((), ()))
    total = {p: None for p in planes}
    for r in range(0, ROWS, 2):
        y = jnp.concatenate([packed[r], packed[r + 1]], axis=1)
        for p in planes:
            part = lax.dot_general(
                panel_rows(panel, slots, r, p), y, nt, preferred_element_type=F32
            )
            total[p] = part if total[p] is None else total[p] + part
    column = lax.broadcasted_iota(jnp.int32, (count, 96), 1) % 16 // 4
    chosen = jnp.zeros((count, 96), F32)
    for p in planes:
        chosen = jnp.where(column == 2 * (p % 2) + p // 2, total[p], chosen)
    hi = chosen.astype(BF16)
    lo = (chosen - hi.astype(F32)).astype(BF16)
    return lax.dot_general(fold, hi, nt, preferred_element_type=F32) + lax.dot_general(
        fold, lo, nt, preferred_element_type=F32
    )


def fold_table():
    f = np.zeros((2, 3, 4, 2, 3, 4, 4), np.float32)
    for a in range(2):
        for t in range(3):
            for q in range(4):
                f[a, t, q, a, t, :, q] = 1.0
    return f.reshape(24, 96)


def spread_table():
    f = np.zeros((4, 2, 3, 2, 2, 4, 2, 3, 4), np.float32)
    for p in range(4):
        for a in range(2):
            for t in range(3):
                for q in range(4):
                    f[p, a, t, p % 2, p // 2, q, a, t, q] = 1.0
    return f.reshape(384, 24)


def multiply(corr, panel, spread, product, slots, more=False):
    rows = jnp.dot(spread[...], corr, preferred_element_type=F32).astype(BF16)
    sign = -lane_sign((48, 2 * BOX))
    for r in range(0, ROWS, 2):
        total = None
        for p in range(4):
            part = jnp.dot(
                rows[96 * p : 96 * p + 96], panel_rows(panel, slots, r, p), preferred_element_type=F32
            )
            total = part if total is None else total + part
        for c in range(2):
            lanes = slice(2 * BOX * c, 2 * BOX * (c + 1))
            value = total[:48, lanes] + pltpu.roll(total[48:, lanes], BOX, 1) * sign
            product[r + c] = product[r + c] + value if more else value


def lay_out(product, finish):
    for f in kept_freqs:
        finish(place_of[f], unpack_row(lambda r: product[r], f))


VMEM_LIMIT = 62 * 1024 * 1024
MESH = pl.DeviceIdType.MESH
vmem = pl.BlockSpec(memory_space=pltpu.VMEM)
smem = pl.BlockSpec(memory_space=pltpu.SMEM)
STEP = 72
SLOTS = (0, 1, 3, 2)


def shape(dims, dtype=F32):
    return jax.ShapeDtypeStruct(dims, dtype)


def remote(src, dst, send, recv, where):
    return pltpu.make_async_remote_copy(
        src_ref=src, dst_ref=dst, send_sem=send, recv_sem=recv, device_id=where, device_id_type=MESH
    )


def away(step):
    return min(step[0], 4 - step[0]) + min(step[1], 4 - step[1])


STEPS = sorted([(y, x) for y in range(4) for x in range(4) if (y, x) != (0, 0)], key=lambda s: -away(s))


def peers(me):
    for dy, dx in STEPS:
        yield 4 * lax.rem(me // 4 + dy, 4) + lax.rem(lax.rem(me, 4) + dx, 4)


def to_peers(me, src_of, dst, send, recv):
    for g in peers(me):
        remote(src_of(g), dst, send, recv, {"ga": g}).start()


def kernel(
    psi, g_mask, v_local, dv, energies, k_point, fwd_hi, fwd_lo, back_hi, back_lo, up_hi, up_lo, down_hi, down_lo,
    fold, spread,
    response, residual,
    raw, mask_rows, mask, level, solved, changes, potential, solved_rows, weights, wide_rows, panel, near, tmp, space, send_a, came_a, send_b, came_b, send_1, send_2,
    came_1, came_2, packed, product, share, shares, far_share, far_shares, source, vec, image, sums, sums_here, all_sums,
    raw_sem, ring_send, ring_recv, a_sem, b_send, b_recv, s1, r1, s2, r2, c_send, c_recv, m_sem,
):
    me = lax.axis_index("ga")
    z = lax.axis_index("band")
    up, down = lax.rem(z + 1, 4), lax.rem(z + 3, 4)

    barrier = pltpu.get_barrier_semaphore()

    for g in peers(me):
        pl.semaphore_signal(barrier, inc=1, device_id={"ga": g}, device_id_type=MESH)
    for other in (up, down):
        pl.semaphore_signal(barrier, inc=1, device_id={"band": other}, device_id_type=MESH)

    def raw_copy(p):
        return pltpu.make_async_copy(psi.at[:, p], raw.at[p], raw_sem.at[p])

    for p in range(4):
        raw_copy(p).start()

    front = lax.broadcasted_iota(jnp.int32, (4, 2 * BOX), 1) < BOX
    top = lax.broadcasted_iota(jnp.int32, (8, 2 * BOX), 0) < 4
    for c in range(BOX // 2):
        both = g_mask[:, 2 * BOX * c : 2 * BOX * (c + 1)].astype(F32)
        turned = pltpu.roll(both, BOX, 1)
        for n, rows in ((2 * c, jnp.where(front, both, turned)), (2 * c + 1, jnp.where(front, turned, both))):
            for p in range(4):
                mask_rows[p, n : n + 1] = rows[p : p + 1]

    def spread_rows(first, second):
        return jnp.where(top, jnp.broadcast_to(first, (8, 2 * BOX)), jnp.broadcast_to(second, (8, 2 * BOX)))

    def pack_plane(u, carry):
        p = 2 * lax.rem(u, 2) + u // 2
        raw_copy(p).wait()

        def widen(m, c):
            wide_rows[pl.ds(pl.multiple_of(STEP * m, 8), BOX), :] = raw[p, m].astype(F32)
            return c

        lax.fori_loop(0, 64, widen, 0)

        def get(f):
            n = f % BOX
            return wide_rows[pl.ds(n, 64, stride=STEP), :] * mask_rows[p, n : n + 1]

        for r in range(ROWS):
            panel[0, p, r] = pack_row(get, r).astype(BF16)
        return carry

    lax.fori_loop(0, 2, pack_plane, 0)
    pl.semaphore_wait(barrier, 17)

    def ring(src_slot, dst_slot, p, where, n):
        return remote(
            panel.at[src_slot, p], panel.at[dst_slot, p], ring_send.at[n], ring_recv.at[dst_slot, p],
            {"band": where},
        )

    def ring_up(p):
        return ring(0, 3, p, up, p)

    def ring_down(p):
        return ring(0, 1, p, down, 4 + p)

    ring_up(0).start()
    ring_down(2).start()
    lax.fori_loop(2, 4, pack_plane, 0)
    ring_up(1).start()
    ring_down(3).start()
    ring_up(2).start()
    ring_down(0).start()
    ring_up(3).start()
    ring_down(1).start()

    for i in range(2):
        for k in range(2):
            for q in range(4):
                solved_rows[pl.ds(STEP * (8 * i + 4 * k + q), BOX), :] = raw[2 * k + i, STRIDE * q].astype(F32)
    for f in kept_freqs:
        n = f % BOX
        for i in range(2):
            rows = mask_rows[i, n : n + 1], mask_rows[2 + i, n : n + 1]
            mask[place_of[f], 8 * i : 8 * i + 8] = spread_rows(*rows)
        solved[place_of[f]] = solved_rows[pl.ds(n, 16, stride=STEP), :] * mask[place_of[f]]
    forward_tile(solved, 0, fwd_hi[...], fwd_lo[...], near, tmp, put_pair(send_a, slice(0, 16), F32))

    mine = pl.ds(4 * me, 4)
    to_peers(me, lambda g: send_a.at[pl.ds(4 * g, 4)], came_a.at[mine], a_sem.at[0], a_sem.at[1])
    came_a[mine] = send_a[mine]

    def spread_field(n, carry):
        line = v_local[pl.ds(n, 1), :]
        potential[n] = spread_rows(line[:, : 2 * BOX], line[:, 2 * BOX :])
        for p in range(NPERT):
            line = dv[p, pl.ds(n, 1), :]
            changes[p, n] = spread_rows(line[:, : 2 * BOX], line[:, 2 * BOX :])
        return carry

    lax.fori_loop(0, BOX, spread_field, 0)

    factor = 0.5 * (2.0 * math.pi / cell_length) ** 2
    row = lax.broadcasted_iota(jnp.int32, (8, 2 * BOX), 0)
    third = lax.broadcasted_iota(jnp.int32, (8, 2 * BOX), 1) % BOX
    third = jnp.where(third < BOX // 2, third, third - BOX).astype(F32)
    for i in range(2):
        first = 4 * me + 2 * (row // 4) + i
        first = jnp.where(first < BOX // 2, first, first - BOX).astype(F32)
        still = factor * ((first + k_point[0]) ** 2 + (third + k_point[2]) ** 2)
        for q in range(4):
            still = jnp.where(row % 4 == q, still - energies[q], still)
        for f in kept_freqs:
            here = mask[place_of[f], 8 * i : 8 * i + 8]
            rise = factor * (float(f) + k_point[1]) * (float(f) + k_point[1])
            level[place_of[f], 8 * i : 8 * i + 8] = (still + rise) * here
            mask[place_of[f], 8 * i : 8 * i + 8] = here * (1.0 / BOX**3)

    def wait_all(src, dst, send, recv):
        return remote(src, dst, send, recv, {"ga": lax.rem(me + 1, 16)})

    every = pl.ds(0, 60)
    wait_all(send_a.at[every], came_a.at[every], a_sem.at[0], a_sem.at[1]).wait()

    turn_in(came_a, near)

    def keep(n, value):
        space[n, 0:8] = value[0]
        space[n, 8:16] = value[1]

    dft64(pair(near), ALL_SET, tmp, keep, 1)

    def each_change(p, carry):
        def load(n):
            d = changes[p, n]
            return (space[n, 0:8] * d, space[n, 8:16] * d)

        dft64(load, ALL_SET, tmp, put_pair(send_b.at[p], slice(0, 16), F32), -1)
        to_peers(
            me, lambda g: send_b.at[p, pl.ds(4 * g, 4)], came_b.at[p, mine], b_send.at[p], b_recv.at[p]
        )
        came_b[p, mine] = send_b[p, mine]
        return carry

    lax.fori_loop(0, NPERT, each_change, 0)

    def pass_on(p_up, p_down):
        ring(0, 3, p_up, up, p_up).wait_recv()
        first = ring(3, 2, p_up, up, 8 + p_up)
        first.start()
        ring(0, 1, p_down, down, 4 + p_down).wait_recv()
        second = ring(1, 2, p_down, down, 8 + p_down)
        second.start()

    pass_on(0, 2)
    pass_on(1, 3)

    def back(came, dst_add):
        def each(t, carry):
            dst_add(t)
            return carry

        lax.fori_loop(0, 3, each, 0)

    def source_tile(t):
        wait_all(send_b.at[t, every], came_b.at[t, every], b_send.at[t], b_recv.at[t]).wait()
        start = pl.multiple_of(16 * t, 16)
        a, b = back_tile(came_b.at[t], back_hi[...], back_lo[...], near, tmp)
        source[:, pl.ds(start, 8), :] = a * mask[:, 0:8, :]
        source[:, pl.ds(start + 8, 8), :] = b * mask[:, 8:16, :]

    back(came_b, source_tile)

    def send_share(n, src):
        to_peers(me, lambda g: src, shares.at[n, me], c_send.at[n], c_recv.at[n])

    def total_share(n):
        first = pl.ds(0, 15)
        wait_all(shares.at[n, first], shares.at[n, first], c_send.at[n], c_recv.at[n]).wait()
        total = shares[n, 0].astype(F32)
        for g in range(1, 16):
            total = total + shares[n, g].astype(F32)
        return total.astype(BF16)

    pack_values(source, packed)
    for p in range(2, 4):
        ring(0, 3, p, up, p).wait_recv()
    for p in range(2):
        ring(0, 1, p, down, 4 + p).wait_recv()
    early = correlate(packed, panel, fold[...], SLOTS[:3]).astype(BF16)
    share[0] = jnp.concatenate([early, jnp.zeros((24, 64), BF16)], axis=1)
    shares[0, me] = share[0]
    send_share(0, share.at[0])
    ring(3, 2, 0, up, 8).wait_recv()
    ring(1, 2, 2, down, 10).wait_recv()
    late = correlate(packed, panel, fold[...], SLOTS[3:], (0, 2))
    multiply(total_share(0)[:, :192], panel, spread, product, SLOTS[:3])
    ring(3, 2, 1, up, 9).wait_recv()
    ring(1, 2, 3, down, 11).wait_recv()
    late = late + correlate(packed, panel, fold[...], SLOTS[3:], (1, 3))
    far_share[...] = jnp.concatenate([late.astype(BF16), jnp.zeros((24, 64), BF16)], axis=1)
    far_shares[me] = far_share[...]
    to_peers(me, lambda g: far_share, far_shares.at[me], c_send.at[3], c_recv.at[3])

    def first_row(place, row):
        for t in range(3):
            rows = slice(16 * t, 16 * t + 16)
            vec[0, place, rows] = row[rows] * mask[place] - source[place, rows]

    first = pl.ds(0, 15)
    wait_all(far_shares.at[first], far_shares.at[first], c_send.at[3], c_recv.at[3]).wait()
    total = far_shares[0].astype(F32)
    for g in range(1, 16):
        total = total + far_shares[g].astype(F32)
    multiply(total.astype(BF16)[:, :64], panel, spread, product, SLOTS[3:], True)
    lay_out(product, first_row)

    lane = lax.broadcasted_iota(jnp.int32, (8, 2 * BOX), 1)
    mine3, most = pl.ds(3 * me, 3), pl.ds(0, 45)
    third = lax.broadcasted_iota(jnp.int32, (16, 2 * BOX), 1) % BOX
    third = jnp.where(third < BOX // 2, third, third - BOX)
    side = jnp.minimum(jnp.maximum(4.0 * k_point[2], -1.0), 1.0)
    edge = jnp.where(third == GCUT, 0.5 - 0.5 * side, jnp.where(third == -GCUT, 0.5 + 0.5 * side, 0.0))
    valid = jnp.where(jnp.abs(third) < GCUT, 1.0, edge)

    def apply(it, carry):
        def near_tile(t, c):
            natural_to_pair(vec.at[it], pl.multiple_of(16 * t, 16), near)
            dft64(load_kept(near), ALL_SET, tmp, put_pair(space, slice(0, 16), F32), 1)
            squeeze(space, send_1.at[it, t])
            to_peers(
                me, lambda g: send_1.at[it, t, pl.ds(3 * g, 3)], came_1.at[it, t, mine3],
                s1.at[it, t], r1.at[it, t],
            )
            came_1[it, t, mine3] = send_1[it, t, mine3]
            return c

        lax.fori_loop(0, 3, near_tile, 0)

        pack_values(vec.at[it], packed)
        n = it + 1
        share[n] = correlate(packed, panel, fold[...], SLOTS).astype(BF16)
        shares[n, me] = share[n]
        send_share(n, share.at[n])

        def space_tile(t, c):
            wait_all(send_1.at[it, t, most], came_1.at[it, t, most], s1.at[it, t], r1.at[it, t]).wait()
            turn_squeezed(came_1.at[it, t], near, valid)
            grid_lanes(near, up_hi[...], up_lo[...])

            weight = [jnp.zeros((8, 2 * BOX), F32)]

            def with_potential(k, value):
                v = potential[k]
                re, im = value[0] * v, value[1] * v
                near[k, 0:8] = re
                near[k, 8:16] = im
                weight[0] = weight[0] + (value[0] * re + value[1] * im)

            dft64(pair(near), ALL_SET, tmp, with_potential, 1)
            weights[t] = weight[0]
            dft64(pair(near), ALL_SET, tmp, put_pair(near, slice(0, 16), F32), -1)
            grid_lanes(near, down_hi[...], down_lo[...], valid)
            squeeze(near, send_2.at[it, t])
            to_peers(
                me, lambda g: send_2.at[it, t, pl.ds(3 * g, 3)], came_2.at[it, t, mine3],
                s2.at[it, t], r2.at[it, t],
            )
            came_2[it, t, mine3] = send_2[it, t, mine3]
            return c

        lax.fori_loop(0, 3, space_tile, 0)

        def with_level(place, row):
            for t in range(3):
                rows = slice(16 * t, 16 * t + 16)
                image[it, place, rows] = (
                    row[rows] * (shift_weight * mask[place])
                    + level[place] * vec[it, place, rows]
                )

        corr = total_share(n)

        @pl.when(it == 1)
        def _():
            def moments(place, totals):
                b, ab, w = vec[0, place], image[0, place], vec[1, place]
                lift = jnp.concatenate([level[place]] * 3, axis=0)
                return tuple(x + y for x, y in zip(totals, (b * b, b * ab, ab * ab, lift * w * w)))

            zero = jnp.zeros((48, 2 * BOX), F32)
            totals = lax.fori_loop(0, KEPT, moments, (zero,) * 4)
            own = jnp.zeros((8, 2 * BOX), F32)
            for m, total in enumerate(totals):
                line = jnp.sum(total, axis=1, keepdims=True) * (1.0 / BOX**3)
                for t in range(3):
                    both = line[16 * t : 16 * t + 8] + line[16 * t + 8 : 16 * t + 16]
                    if m == 3:
                        both = both + jnp.sum(weights[t], axis=1, keepdims=True) * (1.0 / BOX**6)
                    own = jnp.where(lane == 4 * t + m, jnp.broadcast_to(both, own.shape), own)
            own = own + pltpu.roll(own, 4, 0)
            sums[...] = own
            all_sums[me] = own
            to_peers(me, lambda g: sums, all_sums.at[me], m_sem.at[0], m_sem.at[1])
            square = corr.astype(F32)
            square = jnp.sum(square * square, axis=1, keepdims=True) * (shift_weight / BOX**6)
            rest = jnp.zeros((8, 2 * BOX), F32)
            for t in range(3):
                four = square[4 * t : 4 * t + 4] + square[12 + 4 * t : 16 + 4 * t]
                eight = jnp.concatenate([four, four], axis=0)
                rest = jnp.where(lane == 4 * t + 3, jnp.broadcast_to(eight, rest.shape), rest)
            sums_here[...] = rest

        multiply(corr, panel, spread, product, SLOTS)
        lay_out(product, with_level)

        def far_tile(t, c):
            wait_all(send_2.at[it, t, most], came_2.at[it, t, most], s2.at[it, t], r2.at[it, t]).wait()
            start = pl.multiple_of(16 * t, 16)
            turn_squeezed(came_2.at[it, t], near)

            def to_near(n, value):
                near[kept_place(n), 0:8] = value[0]
                near[kept_place(n), 8:16] = value[1]

            dft64(pair(near), KEPT_SET, tmp, to_near, -1)
            for n in range(KEPT):
                for half, value in zip((0, 8), pair_to_natural(near, n)):
                    rows = pl.ds(start + half, 8)
                    total = image[it, n, rows, :] + value * mask[n, half : half + 8]
                    image[it, n, rows, :] = total
                    vec[it + 1, n, rows, :] = total - SHIFT * vec[it, n, rows, :]
            return c

        lax.fori_loop(0, 3, far_tile, 0)
        return carry

    lax.fori_loop(0, 2, apply, 0)

    first = pl.ds(0, 15)
    wait_all(all_sums.at[first], all_sums.at[first], m_sem.at[0], m_sem.at[1]).wait()
    m0 = sums_here[...] + all_sums[0]
    for g in range(1, 16):
        m0 = m0 + all_sums[g]
    m1, m2, m3 = (pltpu.roll(m0, 2 * BOX - n, 1) for n in (1, 2, 3))
    step0 = m0 / m1
    fresh = m0 - 2.0 * step0 * m1 + step0 * step0 * m2
    u = 1.0 + fresh / m0 - step0 * SHIFT
    curve = u * u * m1 - 2.0 * u * step0 * (m2 - SHIFT * m1) + step0 * step0 * m3
    step1 = fresh / curve
    low_part, high_part = step0 + step1 * u, step1 * step0
    for t in range(3):
        a = jnp.broadcast_to(low_part[:, 4 * t : 4 * t + 1], (8, 2 * BOX))
        e = jnp.broadcast_to(high_part[:, 4 * t : 4 * t + 1], (8, 2 * BOX))
        for half in (0, 8):
            rows = slice(16 * t + half, 16 * t + half + 8)
            b, ab = vec[0, :, rows, :], image[0, :, rows, :]
            response[:, rows, :] = a * b - e * vec[1, :, rows, :]
            residual[:, rows, :] = b - a * ab + e * image[1, :, rows, :]

    for p in range(4):
        ring_up(p).wait_send()
        ring_down(p).wait_send()
    for p in range(2):
        ring(3, 2, p, up, 8 + p).wait_send()
    for p in range(2, 4):
        ring(1, 2, p, down, 8 + p).wait_send()


def run(*args):
    grid_f = pltpu.VMEM((BOX, 16, 2 * BOX), F32)
    three_f = pltpu.VMEM((3, BOX, 16, 2 * BOX), F32)
    six_b = pltpu.VMEM((2, 3, 48, 16, 2 * BOX), BF16)
    natural = (KEPT, 48, 2 * BOX)
    dma = pltpu.SemaphoreType.DMA
    return pl.pallas_call(
        kernel,
        out_shape=(shape(natural), shape(natural)),
        in_specs=[pl.BlockSpec(memory_space=pl.ANY)] + [vmem] * 3 + [smem] * 2 + [vmem] * 10,
        out_specs=(vmem, vmem),
        scratch_shapes=[
            pltpu.VMEM((4, 64, BOX, 2 * BOX), BF16),
            pltpu.VMEM((4, BOX, 2 * BOX), F32),
            pltpu.VMEM((KEPT, 16, 2 * BOX), F32),
            pltpu.VMEM((KEPT, 16, 2 * BOX), F32),
            pltpu.VMEM((KEPT, 16, 2 * BOX), F32),
            pltpu.VMEM((NPERT, BOX, 8, 2 * BOX), F32),
            pltpu.VMEM((BOX, 8, 2 * BOX), F32),
            pltpu.VMEM((16 * STEP, 2 * BOX), F32),
            pltpu.VMEM((3, 8, 2 * BOX), F32),
            pltpu.VMEM((64 * STEP, 2 * BOX), F32),
            pltpu.VMEM((4, 4, ROWS, 64, 2 * BOX), BF16),
            grid_f, grid_f, grid_f,
            grid_f, grid_f, three_f, three_f, six_b, six_b, six_b, six_b,
            pltpu.VMEM((ROWS, 96, 2 * BOX), BF16),
            pltpu.VMEM((ROWS, 48, 2 * BOX), F32),
            pltpu.VMEM((3, 24, 256), BF16),
            pltpu.VMEM((3, 16, 24, 256), BF16),
            pltpu.VMEM((24, 128), BF16),
            pltpu.VMEM((16, 24, 128), BF16),
            pltpu.VMEM(natural, F32),
            pltpu.VMEM((3, *natural), F32),
            pltpu.VMEM((2, *natural), F32),
            pltpu.VMEM((8, 2 * BOX), F32),
            pltpu.VMEM((8, 2 * BOX), F32),
            pltpu.VMEM((16, 8, 2 * BOX), F32),
            dma((4,)), dma((12,)), dma((4, 4)), dma((2,)), dma((3,)), dma((3,)),
            dma((2, 3)), dma((2, 3)), dma((2, 3)), dma((2, 3)), dma((4,)), dma((4,)), dma((2,)),
        ],
        compiler_params=pltpu.CompilerParams(
            vmem_limit_bytes=VMEM_LIMIT, collective_id=0, has_side_effects=True
        ),
    )(*args)


def place_body(response, residual, *outs):
    for src, out in zip((response, residual), outs):
        flat = src.reshape(KEPT * 16, 2 * BOX)
        for i in range(2):
            for k in range(2):
                for q in range(4):
                    line = flat[pl.ds(8 * i + 4 * k + q, KEPT, stride=16), :]
                    out[q, 0, 2 * k + i, 0 : GCUT + 1] = line[: GCUT + 1]
                    out[q, 0, 2 * k + i, GCUT + 1 : BOX - GCUT] = jnp.zeros((BOX - KEPT, 2 * BOX), F32)
                    out[q, 0, 2 * k + i, BOX - GCUT :] = line[GCUT + 1 :]


def place(*values):
    out = shape((4, NPERT, 4, BOX, 2 * BOX))
    return pl.pallas_call(
        place_body,
        grid=(NPERT,),
        out_shape=(out, out),
        in_specs=[pl.BlockSpec((KEPT, 16, 2 * BOX), lambda t: (0, t, 0))] * 2,
        out_specs=(pl.BlockSpec((4, 1, 4, BOX, 2 * BOX), lambda t: (0, t, 0, 0, 0)),) * 2,
    )(*values)


def on_device(psi_occ, energies, k_point, g_mask, v_local, dv):
    response, residual = run(
        psi_occ, g_mask, v_local, dv, energies, k_point, *lane_tables(),
        jnp.asarray(fold_table(), BF16), jnp.asarray(spread_table(), BF16),
    )

    return place(response, residual)


def solution(mesh):
    placed = (
        P(("pool", "band"), "ga", None, None),
        P(("pool", "band")),
        P("pool"),
        P(("pool", "ga"), None),
        P(None, "ga"),
        P(None, None, "ga"),
    )
    return jax.shard_map(
        on_device,
        mesh=mesh,
        in_specs=placed,
        out_specs=(
            P(("pool", "band"), None, "ga", None, None),
            P(("pool", "band"), None, "ga", None, None),
        ),
        check_vma=False,
    )
```

```python
import functools
import math

import jax
import jax.numpy as jnp
import numpy as np
from jax import lax
from jax.experimental import pallas as pl
from jax.experimental.pallas import tpu as pltpu
from jax.sharding import PartitionSpec as P

BOX = 64
GCUT = 21
KEPT = 2 * GCUT + 1
NPERT = 3
STRIDE = 16
SHIFT = 16.0
ROWS = 24

cell_length = 16.5
shift_weight = 8.0

kept_freqs = list(range(GCUT + 1)) + list(range(-GCUT, 0))
place_of = {f: i for i, f in enumerate(kept_freqs)}
F32 = jnp.float32
BF16 = jnp.bfloat16


def add(a, b):
    if a is None:
        return b
    if b is None:
        return a
    return (a[0] + b[0], a[1] + b[1])


def sub(a, b):
    if b is None:
        return a
    if a is None:
        return (-b[0], -b[1])
    return (a[0] - b[0], a[1] - b[1])


def times_phase(a, turns, sign):
    if a is None:
        return None
    turns = turns % 1.0
    re, im = a
    if turns == 0.0:
        return a
    if turns == 0.5:
        return (-re, -im)
    if turns in (0.25, 0.75):
        if (turns == 0.25) == (sign > 0):
            return (-im, re)
        return (im, -re)
    c, s = math.cos(2 * math.pi * turns), sign * math.sin(2 * math.pi * turns)
    if turns in (0.125, 0.375, 0.625, 0.875):
        h = abs(c)
        if (c > 0) == (s > 0):
            pair = ((re - im) * h, (re + im) * h)
        else:
            pair = ((re + im) * h, (im - re) * h)
        return pair if c > 0 else (-pair[0], -pair[1])
    return (re * c - im * s, im * c + re * s)


def small_dft(xs, sign):
    n = len(xs)
    if n == 1:
        return xs
    even, odd = small_dft(xs[0::2], sign), small_dft(xs[1::2], sign)
    turned = [times_phase(o, k / n, sign) for k, o in enumerate(odd)]
    return [add(e, o) for e, o in zip(even, turned)] + [sub(e, o) for e, o in zip(even, turned)]


def dft64(load, keep, tmp, store, sign):
    for n2 in range(8):
        out = small_dft([load(8 * n1 + n2) for n1 in range(8)], sign)
        for k1 in range(8):
            re, im = times_phase(out[k1], n2 * k1 / 64.0, sign)
            tmp[8 * n2 + k1, 0:8] = re
            tmp[8 * n2 + k1, 8:16] = im
    for k1 in range(8):
        if not any((k1 + 8 * k2) in keep for k2 in range(8)):
            continue
        out = small_dft([(tmp[8 * n2 + k1, 0:8], tmp[8 * n2 + k1, 8:16]) for n2 in range(8)], sign)
        for k2 in range(8):
            if (k1 + 8 * k2) in keep:
                store(k1 + 8 * k2, out[k2])


def corner_turn(block):
    front = lax.broadcasted_iota(jnp.int32, (8, 2 * BOX), 1) < BOX
    top = lax.broadcasted_iota(jnp.int32, (8, 2 * BOX), 0) < 4
    half = []
    for h in range(2):
        a, b = block[2 * h], block[2 * h + 1]
        half.append(
            (
                jnp.where(front, a, pltpu.roll(b, BOX, 1)),
                jnp.where(front, pltpu.roll(a, BOX, 1), b),
            )
        )
    out = [None] * 4
    for i in range(2):
        a, b = half[0][i], half[1][i]
        out[i] = jnp.where(top, a, pltpu.roll(b, 4, 0))
        out[2 + i] = jnp.where(top, pltpu.roll(a, 4, 0), b)
    return out


def turn_in(src, dst):
    for s in range(16):
        tiles = [src[4 * s + c].astype(F32) for c in range(4)]
        re = corner_turn([t[0:8] for t in tiles])
        im = corner_turn([t[8:16] for t in tiles])
        for c in range(4):
            dst[4 * s + c, 0:8] = re[c]
            dst[4 * s + c, 8:16] = im[c]


def pair(ref):
    return lambda n: (ref[n, 0:8], ref[n, 8:16])


def put_pair(ref, rows, dtype):
    def store(n, value):
        ref[n, rows] = jnp.concatenate([value[0], value[1]], axis=0).astype(dtype)

    return store


def split_dot(x, high, low):
    hi = x.astype(BF16)
    lo = (x - hi.astype(F32)).astype(BF16)
    dot = functools.partial(jnp.dot, preferred_element_type=F32)
    return dot(hi, high) + dot(lo, high) + dot(hi, low)


def lanes_forward(src, first_row, high, low, dst):
    a = src[:, pl.ds(first_row, 8), :].reshape(KEPT * 8, 2 * BOX)
    b = src[:, pl.ds(first_row + 8, 8), :].reshape(KEPT * 8, 2 * BOX)
    out = split_dot(jnp.concatenate([a, b], axis=1), high, low)
    dst[0:KEPT, 0:8, :] = out[:, : 2 * BOX].reshape(KEPT, 8, 2 * BOX)
    dst[0:KEPT, 8:16, :] = out[:, 2 * BOX :].reshape(KEPT, 8, 2 * BOX)


def lanes_back(src, high, low):
    x = jnp.concatenate(
        [
            src[0:KEPT, 0:8, :].reshape(KEPT * 8, 2 * BOX),
            src[0:KEPT, 8:16, :].reshape(KEPT * 8, 2 * BOX),
        ],
        axis=1,
    )
    out = split_dot(x, high, low)
    return (
        out[:, : 2 * BOX].reshape(KEPT, 8, 2 * BOX),
        out[:, 2 * BOX :].reshape(KEPT, 8, 2 * BOX),
    )


def lane_tables():
    index = np.arange(BOX)
    angle = (index[:, None] * index[None, :] % BOX) * (2.0 * np.pi / BOX)
    c, s, z = np.cos(angle), np.sin(angle), np.zeros((BOX, BOX))
    forward = np.block([[c, z, s, z], [-s, z, c, z], [z, c, z, s], [z, -s, z, c]])
    s = -s
    back = np.block([[c, s, z, z], [z, z, c, s], [-s, c, z, z], [z, z, -s, c]])
    grid = np.block([[c, z, -s, z], [z, c, z, -s], [s, z, c, z], [z, s, z, c]])
    out = []
    for w in (forward, back, grid, grid.T):
        w = jnp.asarray(w, F32)
        high = w.astype(BF16)
        out += [high, (w - high.astype(F32)).astype(BF16)]
    return out


kept_place = lambda n: n if n <= GCUT else (n - (BOX - KEPT) if n >= BOX - GCUT else None)
KEPT_SET = frozenset(f % BOX for f in kept_freqs)
ALL_SET = frozenset(range(BOX))


def load_kept(ref):
    def load(n):
        place = kept_place(n)
        return None if place is None else (ref[place, 0:8], ref[place, 8:16])

    return load


def forward_tile(src, first_row, high, low, near, tmp, store):
    lanes_forward(src, first_row, high, low, near)
    dft64(load_kept(near), ALL_SET, tmp, store, 1)


def back_tile(src, high, low, near, tmp):
    turn_in(src, near)

    def store(n, value):
        tmp2 = near
        tmp2[kept_place(n), 0:8] = value[0]
        tmp2[kept_place(n), 8:16] = value[1]

    dft64(pair(near), KEPT_SET, tmp, store, -1)
    return lanes_back(near, high, low)


def squeeze(src, dst):
    front = front_lanes((16, 2 * BOX))
    zero = jnp.zeros((16, 2 * BOX), BF16)
    for g in range(16):
        first, second, third, guest = (src[4 * g + c].astype(BF16) for c in range(4))
        dst[3 * g] = first + pltpu.roll(jnp.where(front, guest, zero), GCUT + 1, 1)
        dst[3 * g + 1] = second + pltpu.roll(jnp.where(front, zero, guest), 2 * BOX - GCUT, 1)
        dst[3 * g + 2] = third


def turn_squeezed(src, dst, valid=None):
    front = front_lanes((16, 2 * BOX))
    left = lax.broadcasted_iota(jnp.int32, (16, 2 * BOX), 1) < BOX
    top = lax.broadcasted_iota(jnp.int32, (8, 2 * BOX), 0) < 4
    for g in range(16):
        tiles = [src[3 * g + c] for c in range(3)]
        ahead = pltpu.roll(tiles[0], 2 * BOX - GCUT - 1, 1)
        tiles.append(jnp.where(front, ahead, pltpu.roll(tiles[1], GCUT, 1)))
        half = []
        for h in range(2):
            a, b = tiles[2 * h], tiles[2 * h + 1]
            half.append(
                (
                    jnp.where(left, a, pltpu.roll(b, BOX, 1)).astype(F32),
                    jnp.where(left, pltpu.roll(a, BOX, 1), b).astype(F32),
                )
            )
        for i in range(2):
            a, b = half[0][i], half[1][i]
            if valid is not None:
                a, b = a * valid, b * valid
            for rows in (slice(0, 8), slice(8, 16)):
                x, y = a[rows], b[rows]
                dst[4 * g + i, rows] = jnp.where(top, x, pltpu.roll(y, 4, 0))
                dst[4 * g + 2 + i, rows] = jnp.where(top, pltpu.roll(x, 4, 0), y)


def natural_to_pair(src, first_row, dst):
    front = lax.broadcasted_iota(jnp.int32, (8, 2 * BOX), 1) < BOX
    for n in range(KEPT):
        a, b = src[n, pl.ds(first_row, 8), :], src[n, pl.ds(first_row + 8, 8), :]
        dst[n, 0:8] = jnp.where(front, a, pltpu.roll(b, BOX, 1))
        dst[n, 8:16] = jnp.where(front, pltpu.roll(a, BOX, 1), b)


def pair_to_natural(src, n):
    front = lax.broadcasted_iota(jnp.int32, (8, 2 * BOX), 1) < BOX
    re, im = src[n, 0:8], src[n, 8:16]
    return jnp.where(front, re, pltpu.roll(im, BOX, 1)), jnp.where(front, pltpu.roll(re, BOX, 1), im)


def grid_lanes(ref, high, low, valid=None):
    x = [ref[:, h : h + 8, :].reshape(BOX * 8, 2 * BOX) for h in (0, 8)]
    x = jnp.concatenate(x, axis=1).astype(BF16)
    out = jnp.dot(x, high, preferred_element_type=F32) + jnp.dot(x, low, preferred_element_type=F32)
    for h, lanes in ((0, slice(0, 2 * BOX)), (8, slice(2 * BOX, 4 * BOX))):
        part = out[:, lanes].reshape(BOX, 8, 2 * BOX)
        ref[:, h : h + 8, :] = part if valid is None else part * valid[0:8]


def front_lanes(shape):
    return lax.broadcasted_iota(jnp.int32, shape, len(shape) - 1) % BOX < BOX // 2


def widest(f):
    return int(math.sqrt(GCUT**2 - max(abs(f) - 0.5, 0.0) ** 2) + 0.5)


def lay_rows():
    order = sorted(kept_freqs, key=lambda f: (abs(f), -f))
    hosts, others = order[:ROWS], order[ROWS:]
    room = [[widest(f) + 1, BOX - 1 - widest(f)] for f in hosts]
    pieces = sorted(
        [(widest(f) + 1, f, True) for f in others] + [(widest(f), f, False) for f in others],
        key=lambda piece: -piece[0],
    )
    guests, where = [[] for _ in hosts], {}
    for size, f, ahead in pieces:
        fits = [r for r in range(ROWS) if room[r][1] - room[r][0] + 1 >= size]
        r = min(fits, key=lambda n: (room[n][1] - room[n][0] + 1 - size, n))
        start = room[r][0]
        shift = start if ahead else start - (BOX - size)
        room[r][0] = start + size
        guests[r].append((f, ahead, shift % (2 * BOX)))
        where[f, ahead] = (r, shift % (2 * BOX))
    return hosts, guests, where


hosts, guests, where_laid = lay_rows()


def pack_row(get, r):
    value = get(hosts[r])
    front = front_lanes(value.shape)
    for f, ahead, shift in guests[r]:
        row = get(f)
        piece = jnp.where(front, row, 0.0) if ahead else jnp.where(front, 0.0, row)
        value = value + pltpu.roll(piece, shift, value.ndim - 1)
    return value


def unpack_row(get, f):
    if f in hosts:
        return get(hosts.index(f))
    (r, up), (n, down) = where_laid[f, True], where_laid[f, False]
    first, second = get(r), get(n)
    axis = first.ndim - 1
    return jnp.where(
        front_lanes(first.shape),
        pltpu.roll(first, (2 * BOX - up) % (2 * BOX), axis),
        pltpu.roll(second, (2 * BOX - down) % (2 * BOX), axis),
    )


def lane_sign(shape):
    return jnp.where(lax.broadcasted_iota(jnp.int32, shape, len(shape) - 1) < BOX, 1.0, -1.0)


def panel_rows(panel, slots, r, p):
    rows = [jnp.concatenate([panel[d, p, n] for d in slots], axis=0) for n in (r, r + 1)]
    return jnp.concatenate(rows, axis=1)


def pack_values(values, packed):
    sign = lane_sign((48, 2 * BOX))
    for r in range(ROWS):
        straight = pack_row(lambda f: values[place_of[f]], r)
        turned = pltpu.roll(straight, BOX, 1) * sign
        packed[r] = jnp.concatenate([straight, turned], axis=0).astype(BF16)


def correlate(packed, panel, fold, slots, planes=(0, 1, 2, 3)):
    count = 64 * len(slots)
    nt = (((1,), (1,)), ((), ()))
    total = {p: None for p in planes}
    for r in range(0, ROWS, 2):
        y = jnp.concatenate([packed[r], packed[r + 1]], axis=1)
        for p in planes:
            part = lax.dot_general(
                panel_rows(panel, slots, r, p), y, nt, preferred_element_type=F32
            )
            total[p] = part if total[p] is None else total[p] + part
    column = lax.broadcasted_iota(jnp.int32, (count, 96), 1) % 16 // 4
    chosen = jnp.zeros((count, 96), F32)
    for p in planes:
        chosen = jnp.where(column == 2 * (p % 2) + p // 2, total[p], chosen)
    hi = chosen.astype(BF16)
    lo = (chosen - hi.astype(F32)).astype(BF16)
    return lax.dot_general(fold, hi, nt, preferred_element_type=F32) + lax.dot_general(
        fold, lo, nt, preferred_element_type=F32
    )


def fold_table():
    f = np.zeros((2, 3, 4, 2, 3, 4, 4), np.float32)
    for a in range(2):
        for t in range(3):
            for q in range(4):
                f[a, t, q, a, t, :, q] = 1.0
    return f.reshape(24, 96)


def spread_table():
    f = np.zeros((4, 2, 3, 2, 2, 4, 2, 3, 4), np.float32)
    for p in range(4):
        for a in range(2):
            for t in range(3):
                for q in range(4):
                    f[p, a, t, p % 2, p // 2, q, a, t, q] = 1.0
    return f.reshape(384, 24)


def multiply(corr, panel, spread, product, slots, more=False):
    rows = jnp.dot(spread[...], corr, preferred_element_type=F32).astype(BF16)
    sign = -lane_sign((48, 2 * BOX))
    for r in range(0, ROWS, 2):
        total = None
        for p in range(4):
            part = jnp.dot(
                rows[96 * p : 96 * p + 96], panel_rows(panel, slots, r, p), preferred_element_type=F32
            )
            total = part if total is None else total + part
        for c in range(2):
            lanes = slice(2 * BOX * c, 2 * BOX * (c + 1))
            value = total[:48, lanes] + pltpu.roll(total[48:, lanes], BOX, 1) * sign
            product[r + c] = product[r + c] + value if more else value


def lay_out(product, finish):
    for f in kept_freqs:
        finish(place_of[f], unpack_row(lambda r: product[r], f))


VMEM_LIMIT = 62 * 1024 * 1024
MESH = pl.DeviceIdType.MESH
vmem = pl.BlockSpec(memory_space=pltpu.VMEM)
smem = pl.BlockSpec(memory_space=pltpu.SMEM)
far = pl.BlockSpec(memory_space=pltpu.HBM)
STEP = 72
SLOTS = (0, 1, 3, 2)


def shape(dims, dtype=F32):
    return jax.ShapeDtypeStruct(dims, dtype)


def remote(src, dst, send, recv, where):
    return pltpu.make_async_remote_copy(
        src_ref=src, dst_ref=dst, send_sem=send, recv_sem=recv, device_id=where, device_id_type=MESH
    )


def away(step):
    return min(step[0], 4 - step[0]) + min(step[1], 4 - step[1])


STEPS = sorted([(y, x) for y in range(4) for x in range(4) if (y, x) != (0, 0)], key=lambda s: -away(s))


def peers(me):
    for dy, dx in STEPS:
        yield 4 * lax.rem(me // 4 + dy, 4) + lax.rem(lax.rem(me, 4) + dx, 4)


def to_peers(me, src_of, dst, send, recv):
    for g in peers(me):
        remote(src_of(g), dst, send, recv, {"ga": g}).start()


def kernel(
    psi, g_mask, fold, spread, energies, k_point, far_v, far_dv, far_tables,
    response, residual,
    v_local, dv, tables, raw, mask_rows, mask, level, solved, changes, potential, solved_rows, weights, wide_rows, panel, near, tmp, space, send_a, came_a, send_b, came_b, send_1, send_2,
    came_1, came_2, packed, product, share, shares, far_share, far_shares, source, vec, image, sums, sums_here, all_sums,
    in_sem, raw_sem, ring_send, ring_recv, a_sem, b_send, b_recv, s1, r1, s2, r2, c_send, c_recv, m_sem,
):
    me = lax.axis_index("ga")
    z = lax.axis_index("band")
    up, down = lax.rem(z + 1, 4), lax.rem(z + 3, 4)

    barrier = pltpu.get_barrier_semaphore()

    for g in peers(me):
        pl.semaphore_signal(barrier, inc=1, device_id={"ga": g}, device_id_type=MESH)
    for other in (up, down):
        pl.semaphore_signal(barrier, inc=1, device_id={"band": other}, device_id_type=MESH)

    def raw_copy(p):
        return pltpu.make_async_copy(psi.at[:, p], raw.at[p], raw_sem.at[p])

    def late_copy(n):
        src, dst = ((far_tables, tables), (far_v, v_local), (far_dv, dv))[n]
        return pltpu.make_async_copy(src, dst, in_sem.at[n])

    for p in (0, 2, 1, 3):
        raw_copy(p).start()
    for n in range(3):
        late_copy(n).start()
    fwd_hi, fwd_lo, back_hi, back_lo, up_hi, up_lo, down_hi, down_lo = (tables.at[n] for n in range(8))

    front = lax.broadcasted_iota(jnp.int32, (4, 2 * BOX), 1) < BOX
    top = lax.broadcasted_iota(jnp.int32, (8, 2 * BOX), 0) < 4
    for c in range(BOX // 2):
        both = g_mask[:, 2 * BOX * c : 2 * BOX * (c + 1)].astype(F32)
        turned = pltpu.roll(both, BOX, 1)
        for n, rows in ((2 * c, jnp.where(front, both, turned)), (2 * c + 1, jnp.where(front, turned, both))):
            for p in range(4):
                mask_rows[p, n : n + 1] = rows[p : p + 1]

    def spread_rows(first, second):
        return jnp.where(top, jnp.broadcast_to(first, (8, 2 * BOX)), jnp.broadcast_to(second, (8, 2 * BOX)))

    def pack_plane(u, carry):
        p = 2 * lax.rem(u, 2) + u // 2
        raw_copy(p).wait()

        def widen(m, c):
            wide_rows[pl.ds(pl.multiple_of(STEP * m, 8), BOX), :] = raw[p, m].astype(F32)
            return c

        lax.fori_loop(0, 64, widen, 0)

        def get(f):
            n = f % BOX
            return wide_rows[pl.ds(n, 64, stride=STEP), :] * mask_rows[p, n : n + 1]

        for r in range(ROWS):
            panel[0, p, r] = pack_row(get, r).astype(BF16)
        return carry

    lax.fori_loop(0, 2, pack_plane, 0)
    pl.semaphore_wait(barrier, 17)

    def ring(src_slot, dst_slot, p, where, n):
        return remote(
            panel.at[src_slot, p], panel.at[dst_slot, p], ring_send.at[n], ring_recv.at[dst_slot, p],
            {"band": where},
        )

    def ring_up(p):
        return ring(0, 3, p, up, p)

    def ring_down(p):
        return ring(0, 1, p, down, 4 + p)

    ring_up(0).start()
    ring_down(2).start()
    lax.fori_loop(2, 4, pack_plane, 0)
    ring_up(1).start()
    ring_down(3).start()
    ring_up(2).start()
    ring_down(0).start()
    ring_up(3).start()
    ring_down(1).start()

    for i in range(2):
        for k in range(2):
            for q in range(4):
                solved_rows[pl.ds(STEP * (8 * i + 4 * k + q), BOX), :] = raw[2 * k + i, STRIDE * q].astype(F32)
    for f in kept_freqs:
        n = f % BOX
        for i in range(2):
            rows = mask_rows[i, n : n + 1], mask_rows[2 + i, n : n + 1]
            mask[place_of[f], 8 * i : 8 * i + 8] = spread_rows(*rows)
        solved[place_of[f]] = solved_rows[pl.ds(n, 16, stride=STEP), :] * mask[place_of[f]]
    for n in range(3):
        late_copy(n).wait()
    forward_tile(solved, 0, fwd_hi[...], fwd_lo[...], near, tmp, put_pair(send_a, slice(0, 16), F32))

    mine = pl.ds(4 * me, 4)
    to_peers(me, lambda g: send_a.at[pl.ds(4 * g, 4)], came_a.at[mine], a_sem.at[0], a_sem.at[1])
    came_a[mine] = send_a[mine]

    def spread_field(n, carry):
        line = v_local[pl.ds(n, 1), :]
        potential[n] = spread_rows(line[:, : 2 * BOX], line[:, 2 * BOX :])
        for p in range(NPERT):
            line = dv[p, pl.ds(n, 1), :]
            changes[p, n] = spread_rows(line[:, : 2 * BOX], line[:, 2 * BOX :])
        return carry

    lax.fori_loop(0, BOX, spread_field, 0)

    factor = 0.5 * (2.0 * math.pi / cell_length) ** 2
    row = lax.broadcasted_iota(jnp.int32, (8, 2 * BOX), 0)
    third = lax.broadcasted_iota(jnp.int32, (8, 2 * BOX), 1) % BOX
    third = jnp.where(third < BOX // 2, third, third - BOX).astype(F32)
    for i in range(2):
        first = 4 * me + 2 * (row // 4) + i
        first = jnp.where(first < BOX // 2, first, first - BOX).astype(F32)
        still = factor * ((first + k_point[0]) ** 2 + (third + k_point[2]) ** 2)
        for q in range(4):
            still = jnp.where(row % 4 == q, still - energies[q], still)
        for f in kept_freqs:
            here = mask[place_of[f], 8 * i : 8 * i + 8]
            rise = factor * (float(f) + k_point[1]) * (float(f) + k_point[1])
            level[place_of[f], 8 * i : 8 * i + 8] = (still + rise) * here
            mask[place_of[f], 8 * i : 8 * i + 8] = here * (1.0 / BOX**3)

    def wait_all(src, dst, send, recv):
        return remote(src, dst, send, recv, {"ga": lax.rem(me + 1, 16)})

    every = pl.ds(0, 60)
    wait_all(send_a.at[every], came_a.at[every], a_sem.at[0], a_sem.at[1]).wait()

    turn_in(came_a, near)

    def keep(n, value):
        space[n, 0:8] = value[0]
        space[n, 8:16] = value[1]

    dft64(pair(near), ALL_SET, tmp, keep, 1)

    def each_change(p, carry):
        def load(n):
            d = changes[p, n]
            return (space[n, 0:8] * d, space[n, 8:16] * d)

        dft64(load, ALL_SET, tmp, put_pair(send_b.at[p], slice(0, 16), F32), -1)
        to_peers(
            me, lambda g: send_b.at[p, pl.ds(4 * g, 4)], came_b.at[p, mine], b_send.at[p], b_recv.at[p]
        )
        came_b[p, mine] = send_b[p, mine]
        return carry

    lax.fori_loop(0, NPERT, each_change, 0)

    def pass_on(p_up, p_down):
        ring(0, 3, p_up, up, p_up).wait_recv()
        first = ring(3, 2, p_up, up, 8 + p_up)
        first.start()
        ring(0, 1, p_down, down, 4 + p_down).wait_recv()
        second = ring(1, 2, p_down, down, 8 + p_down)
        second.start()

    pass_on(0, 2)
    pass_on(1, 3)

    def back(came, dst_add):
        def each(t, carry):
            dst_add(t)
            return carry

        lax.fori_loop(0, 3, each, 0)

    def source_tile(t):
        wait_all(send_b.at[t, every], came_b.at[t, every], b_send.at[t], b_recv.at[t]).wait()
        start = pl.multiple_of(16 * t, 16)
        a, b = back_tile(came_b.at[t], back_hi[...], back_lo[...], near, tmp)
        source[:, pl.ds(start, 8), :] = a * mask[:, 0:8, :]
        source[:, pl.ds(start + 8, 8), :] = b * mask[:, 8:16, :]

    back(came_b, source_tile)

    def send_share(n, src):
        to_peers(me, lambda g: src, shares.at[n, me], c_send.at[n], c_recv.at[n])

    def total_share(n):
        first = pl.ds(0, 15)
        wait_all(shares.at[n, first], shares.at[n, first], c_send.at[n], c_recv.at[n]).wait()
        total = shares[n, 0].astype(F32)
        for g in range(1, 16):
            total = total + shares[n, g].astype(F32)
        return total.astype(BF16)

    pack_values(source, packed)
    for p in range(2, 4):
        ring(0, 3, p, up, p).wait_recv()
    for p in range(2):
        ring(0, 1, p, down, 4 + p).wait_recv()
    early = correlate(packed, panel, fold[...], SLOTS[:3]).astype(BF16)
    share[0] = jnp.concatenate([early, jnp.zeros((24, 64), BF16)], axis=1)
    shares[0, me] = share[0]
    send_share(0, share.at[0])
    ring(3, 2, 0, up, 8).wait_recv()
    ring(1, 2, 2, down, 10).wait_recv()
    late = correlate(packed, panel, fold[...], SLOTS[3:], (0, 2))
    multiply(total_share(0)[:, :192], panel, spread, product, SLOTS[:3])
    ring(3, 2, 1, up, 9).wait_recv()
    ring(1, 2, 3, down, 11).wait_recv()
    late = late + correlate(packed, panel, fold[...], SLOTS[3:], (1, 3))
    far_share[...] = jnp.concatenate([late.astype(BF16), jnp.zeros((24, 64), BF16)], axis=1)
    far_shares[me] = far_share[...]
    to_peers(me, lambda g: far_share, far_shares.at[me], c_send.at[3], c_recv.at[3])

    def first_row(place, row):
        for t in range(3):
            rows = slice(16 * t, 16 * t + 16)
            vec[0, place, rows] = row[rows] * mask[place] - source[place, rows]

    first = pl.ds(0, 15)
    wait_all(far_shares.at[first], far_shares.at[first], c_send.at[3], c_recv.at[3]).wait()
    total = far_shares[0].astype(F32)
    for g in range(1, 16):
        total = total + far_shares[g].astype(F32)
    multiply(total.astype(BF16)[:, :64], panel, spread, product, SLOTS[3:], True)
    lay_out(product, first_row)

    lane = lax.broadcasted_iota(jnp.int32, (8, 2 * BOX), 1)
    mine3, most = pl.ds(3 * me, 3), pl.ds(0, 45)
    third = lax.broadcasted_iota(jnp.int32, (16, 2 * BOX), 1) % BOX
    third = jnp.where(third < BOX // 2, third, third - BOX)
    side = jnp.minimum(jnp.maximum(4.0 * k_point[2], -1.0), 1.0)
    edge = jnp.where(third == GCUT, 0.5 - 0.5 * side, jnp.where(third == -GCUT, 0.5 + 0.5 * side, 0.0))
    valid = jnp.where(jnp.abs(third) < GCUT, 1.0, edge)

    def apply(it, carry):
        def near_tile(t, c):
            natural_to_pair(vec.at[it], pl.multiple_of(16 * t, 16), near)
            dft64(load_kept(near), ALL_SET, tmp, put_pair(space, slice(0, 16), F32), 1)
            squeeze(space, send_1.at[it, t])
            to_peers(
                me, lambda g: send_1.at[it, t, pl.ds(3 * g, 3)], came_1.at[it, t, mine3],
                s1.at[it, t], r1.at[it, t],
            )
            came_1[it, t, mine3] = send_1[it, t, mine3]
            return c

        lax.fori_loop(0, 3, near_tile, 0)

        pack_values(vec.at[it], packed)
        n = it + 1
        share[n] = correlate(packed, panel, fold[...], SLOTS).astype(BF16)
        shares[n, me] = share[n]
        send_share(n, share.at[n])

        def space_tile(t, c):
            wait_all(send_1.at[it, t, most], came_1.at[it, t, most], s1.at[it, t], r1.at[it, t]).wait()
            turn_squeezed(came_1.at[it, t], near, valid)
            grid_lanes(near, up_hi[...], up_lo[...])

            weight = [jnp.zeros((8, 2 * BOX), F32)]

            def with_potential(k, value):
                v = potential[k]
                re, im = value[0] * v, value[1] * v
                near[k, 0:8] = re
                near[k, 8:16] = im
                weight[0] = weight[0] + (value[0] * re + value[1] * im)

            dft64(pair(near), ALL_SET, tmp, with_potential, 1)
            weights[t] = weight[0]
            dft64(pair(near), ALL_SET, tmp, put_pair(near, slice(0, 16), F32), -1)
            grid_lanes(near, down_hi[...], down_lo[...], valid)
            squeeze(near, send_2.at[it, t])
            to_peers(
                me, lambda g: send_2.at[it, t, pl.ds(3 * g, 3)], came_2.at[it, t, mine3],
                s2.at[it, t], r2.at[it, t],
            )
            came_2[it, t, mine3] = send_2[it, t, mine3]
            return c

        lax.fori_loop(0, 3, space_tile, 0)

        def with_level(place, row):
            for t in range(3):
                rows = slice(16 * t, 16 * t + 16)
                image[it, place, rows] = (
                    row[rows] * (shift_weight * mask[place])
                    + level[place] * vec[it, place, rows]
                )

        corr = total_share(n)

        @pl.when(it == 1)
        def _():
            def moments(place, totals):
                b, ab, w = vec[0, place], image[0, place], vec[1, place]
                lift = jnp.concatenate([level[place]] * 3, axis=0)
                return tuple(x + y for x, y in zip(totals, (b * b, b * ab, ab * ab, lift * w * w)))

            zero = jnp.zeros((48, 2 * BOX), F32)
            totals = lax.fori_loop(0, KEPT, moments, (zero,) * 4)
            own = jnp.zeros((8, 2 * BOX), F32)
            for m, total in enumerate(totals):
                line = jnp.sum(total, axis=1, keepdims=True) * (1.0 / BOX**3)
                for t in range(3):
                    both = line[16 * t : 16 * t + 8] + line[16 * t + 8 : 16 * t + 16]
                    if m == 3:
                        both = both + jnp.sum(weights[t], axis=1, keepdims=True) * (1.0 / BOX**6)
                    own = jnp.where(lane == 4 * t + m, jnp.broadcast_to(both, own.shape), own)
            own = own + pltpu.roll(own, 4, 0)
            sums[...] = own
            all_sums[me] = own
            to_peers(me, lambda g: sums, all_sums.at[me], m_sem.at[0], m_sem.at[1])
            square = corr.astype(F32)
            square = jnp.sum(square * square, axis=1, keepdims=True) * (shift_weight / BOX**6)
            rest = jnp.zeros((8, 2 * BOX), F32)
            for t in range(3):
                four = square[4 * t : 4 * t + 4] + square[12 + 4 * t : 16 + 4 * t]
                eight = jnp.concatenate([four, four], axis=0)
                rest = jnp.where(lane == 4 * t + 3, jnp.broadcast_to(eight, rest.shape), rest)
            sums_here[...] = rest

        multiply(corr, panel, spread, product, SLOTS)
        lay_out(product, with_level)

        def far_tile(t, c):
            wait_all(send_2.at[it, t, most], came_2.at[it, t, most], s2.at[it, t], r2.at[it, t]).wait()
            start = pl.multiple_of(16 * t, 16)
            turn_squeezed(came_2.at[it, t], near)

            def to_near(n, value):
                near[kept_place(n), 0:8] = value[0]
                near[kept_place(n), 8:16] = value[1]

            dft64(pair(near), KEPT_SET, tmp, to_near, -1)
            for n in range(KEPT):
                for half, value in zip((0, 8), pair_to_natural(near, n)):
                    rows = pl.ds(start + half, 8)
                    total = image[it, n, rows, :] + value * mask[n, half : half + 8]
                    image[it, n, rows, :] = total
                    vec[it + 1, n, rows, :] = total - SHIFT * vec[it, n, rows, :]
            return c

        lax.fori_loop(0, 3, far_tile, 0)
        return carry

    lax.fori_loop(0, 2, apply, 0)

    first = pl.ds(0, 15)
    wait_all(all_sums.at[first], all_sums.at[first], m_sem.at[0], m_sem.at[1]).wait()
    m0 = sums_here[...] + all_sums[0]
    for g in range(1, 16):
        m0 = m0 + all_sums[g]
    m1, m2, m3 = (pltpu.roll(m0, 2 * BOX - n, 1) for n in (1, 2, 3))
    step0 = m0 / m1
    fresh = m0 - 2.0 * step0 * m1 + step0 * step0 * m2
    u = 1.0 + fresh / m0 - step0 * SHIFT
    curve = u * u * m1 - 2.0 * u * step0 * (m2 - SHIFT * m1) + step0 * step0 * m3
    step1 = fresh / curve
    low_part, high_part = step0 + step1 * u, step1 * step0
    for t in range(3):
        a = jnp.broadcast_to(low_part[:, 4 * t : 4 * t + 1], (8, 2 * BOX))
        e = jnp.broadcast_to(high_part[:, 4 * t : 4 * t + 1], (8, 2 * BOX))
        for half in (0, 8):
            rows = slice(16 * t + half, 16 * t + half + 8)
            b, ab = vec[0, :, rows, :], image[0, :, rows, :]
            response[:, rows, :] = a * b - e * vec[1, :, rows, :]
            residual[:, rows, :] = b - a * ab + e * image[1, :, rows, :]

    for p in range(4):
        ring_up(p).wait_send()
        ring_down(p).wait_send()
    for p in range(2):
        ring(3, 2, p, up, 8 + p).wait_send()
    for p in range(2, 4):
        ring(1, 2, p, down, 8 + p).wait_send()


def run(*args):
    grid_f = pltpu.VMEM((BOX, 16, 2 * BOX), F32)
    three_f = pltpu.VMEM((3, BOX, 16, 2 * BOX), F32)
    six_b = pltpu.VMEM((2, 3, 48, 16, 2 * BOX), BF16)
    natural = (KEPT, 48, 2 * BOX)
    dma = pltpu.SemaphoreType.DMA
    return pl.pallas_call(
        kernel,
        out_shape=(shape(natural), shape(natural)),
        in_specs=[far] + [vmem] * 3 + [smem] * 2 + [far] * 3,
        out_specs=(vmem, vmem),
        scratch_shapes=[
            pltpu.VMEM((BOX, 4 * BOX), F32),
            pltpu.VMEM((NPERT, BOX, 4 * BOX), F32),
            pltpu.VMEM((8, 4 * BOX, 4 * BOX), BF16),
            pltpu.VMEM((4, 64, BOX, 2 * BOX), BF16),
            pltpu.VMEM((4, BOX, 2 * BOX), F32),
            pltpu.VMEM((KEPT, 16, 2 * BOX), F32),
            pltpu.VMEM((KEPT, 16, 2 * BOX), F32),
            pltpu.VMEM((KEPT, 16, 2 * BOX), F32),
            pltpu.VMEM((NPERT, BOX, 8, 2 * BOX), F32),
            pltpu.VMEM((BOX, 8, 2 * BOX), F32),
            pltpu.VMEM((16 * STEP, 2 * BOX), F32),
            pltpu.VMEM((3, 8, 2 * BOX), F32),
            pltpu.VMEM((64 * STEP, 2 * BOX), F32),
            pltpu.VMEM((4, 4, ROWS, 64, 2 * BOX), BF16),
            grid_f, grid_f, grid_f,
            grid_f, grid_f, three_f, three_f, six_b, six_b, six_b, six_b,
            pltpu.VMEM((ROWS, 96, 2 * BOX), BF16),
            pltpu.VMEM((ROWS, 48, 2 * BOX), F32),
            pltpu.VMEM((3, 24, 256), BF16),
            pltpu.VMEM((3, 16, 24, 256), BF16),
            pltpu.VMEM((24, 128), BF16),
            pltpu.VMEM((16, 24, 128), BF16),
            pltpu.VMEM(natural, F32),
            pltpu.VMEM((3, *natural), F32),
            pltpu.VMEM((2, *natural), F32),
            pltpu.VMEM((8, 2 * BOX), F32),
            pltpu.VMEM((8, 2 * BOX), F32),
            pltpu.VMEM((16, 8, 2 * BOX), F32),
            dma((3,)), dma((4,)), dma((12,)), dma((4, 4)), dma((2,)), dma((3,)), dma((3,)),
            dma((2, 3)), dma((2, 3)), dma((2, 3)), dma((2, 3)), dma((4,)), dma((4,)), dma((2,)),
        ],
        compiler_params=pltpu.CompilerParams(
            vmem_limit_bytes=VMEM_LIMIT, collective_id=0, has_side_effects=True
        ),
    )(*args)


def place_body(response, residual, first, second, buffer, sem):
    pairs = ((0, response, first), (1, residual, second))

    def leave(w, out, t, q):
        part = pl.ds(12 * q + 4 * t, 4)
        return pltpu.make_async_copy(buffer.at[w, part], out.at[part], sem.at[w, t, q])

    for t in range(NPERT):
        for w, src, out in pairs:
            flat = src.reshape(KEPT * 48, 2 * BOX)
            for q in range(4):
                for p in range(4):
                    row = 16 * t + 8 * (p % 2) + 4 * (p // 2) + q
                    to = 12 * q + 4 * t + p
                    buffer[w, to, 0 : GCUT + 1] = flat[pl.ds(row, GCUT + 1, stride=48), :]
                    buffer[w, to, GCUT + 1 : BOX - GCUT] = jnp.zeros((BOX - KEPT, 2 * BOX), F32)
                    buffer[w, to, BOX - GCUT :] = flat[pl.ds(row + 48 * (GCUT + 1), GCUT, stride=48), :]
                leave(w, out, t, q).start()
    for t in range(NPERT):
        for w, _, out in pairs:
            for q in range(4):
                leave(w, out, t, q).wait()


def place(*values):
    out = shape((48, BOX, 2 * BOX))
    outs = pl.pallas_call(
        place_body,
        out_shape=(out, out),
        in_specs=[vmem] * 2,
        out_specs=(pl.BlockSpec(memory_space=pl.ANY),) * 2,
        scratch_shapes=[
            pltpu.VMEM((2, 48, BOX, 2 * BOX), F32),
            pltpu.SemaphoreType.DMA((2, NPERT, 4)),
        ],
        compiler_params=pltpu.CompilerParams(vmem_limit_bytes=16 * 1024 * 1024),
    )(*values)
    return tuple(v.reshape(4, NPERT, 4, BOX, 2 * BOX) for v in outs)


def on_device(psi_occ, energies, k_point, g_mask, v_local, dv):
    response, residual = run(
        psi_occ, g_mask, jnp.asarray(fold_table(), BF16), jnp.asarray(spread_table(), BF16),
        energies, k_point, v_local, dv, jnp.stack(lane_tables()),
    )

    return place(response, residual)


def solution(mesh):
    placed = (
        P(("pool", "band"), "ga", None, None),
        P(("pool", "band")),
        P("pool"),
        P(("pool", "ga"), None),
        P(None, "ga"),
        P(None, None, "ga"),
    )
    return jax.shard_map(
        on_device,
        mesh=mesh,
        in_specs=placed,
        out_specs=(
            P(("pool", "band"), None, "ga", None, None),
            P(("pool", "band"), None, "ga", None, None),
        ),
        check_vma=False,
    )
```

```python
import functools
import math

import jax
import jax.numpy as jnp
import numpy as np
from jax import lax
from jax.experimental import pallas as pl
from jax.experimental.pallas import tpu as pltpu
from jax.sharding import PartitionSpec as P

BOX = 64
GCUT = 21
KEPT = 2 * GCUT + 1
NPERT = 3
STRIDE = 16
SHIFT = 16.0
ROWS = 24

cell_length = 16.5
shift_weight = 8.0

kept_freqs = list(range(GCUT + 1)) + list(range(-GCUT, 0))
place_of = {f: i for i, f in enumerate(kept_freqs)}
F32 = jnp.float32
BF16 = jnp.bfloat16


def add(a, b):
    if a is None:
        return b
    if b is None:
        return a
    return (a[0] + b[0], a[1] + b[1])


def sub(a, b):
    if b is None:
        return a
    if a is None:
        return (-b[0], -b[1])
    return (a[0] - b[0], a[1] - b[1])


def times_phase(a, turns, sign):
    if a is None:
        return None
    turns = turns % 1.0
    re, im = a
    if turns == 0.0:
        return a
    if turns == 0.5:
        return (-re, -im)
    if turns in (0.25, 0.75):
        if (turns == 0.25) == (sign > 0):
            return (-im, re)
        return (im, -re)
    c, s = math.cos(2 * math.pi * turns), sign * math.sin(2 * math.pi * turns)
    if turns in (0.125, 0.375, 0.625, 0.875):
        h = abs(c)
        if (c > 0) == (s > 0):
            pair = ((re - im) * h, (re + im) * h)
        else:
            pair = ((re + im) * h, (im - re) * h)
        return pair if c > 0 else (-pair[0], -pair[1])
    return (re * c - im * s, im * c + re * s)


def small_dft(xs, sign):
    n = len(xs)
    if n == 1:
        return xs
    even, odd = small_dft(xs[0::2], sign), small_dft(xs[1::2], sign)
    turned = [times_phase(o, k / n, sign) for k, o in enumerate(odd)]
    return [add(e, o) for e, o in zip(even, turned)] + [sub(e, o) for e, o in zip(even, turned)]


def dft64(load, keep, tmp, store, sign):
    for n2 in range(8):
        out = small_dft([load(8 * n1 + n2) for n1 in range(8)], sign)
        for k1 in range(8):
            re, im = times_phase(out[k1], n2 * k1 / 64.0, sign)
            tmp[8 * n2 + k1, 0:8] = re
            tmp[8 * n2 + k1, 8:16] = im
    for k1 in range(8):
        if not any((k1 + 8 * k2) in keep for k2 in range(8)):
            continue
        out = small_dft([(tmp[8 * n2 + k1, 0:8], tmp[8 * n2 + k1, 8:16]) for n2 in range(8)], sign)
        for k2 in range(8):
            if (k1 + 8 * k2) in keep:
                store(k1 + 8 * k2, out[k2])


def corner_turn(block):
    front = lax.broadcasted_iota(jnp.int32, (8, 2 * BOX), 1) < BOX
    top = lax.broadcasted_iota(jnp.int32, (8, 2 * BOX), 0) < 4
    half = []
    for h in range(2):
        a, b = block[2 * h], block[2 * h + 1]
        half.append(
            (
                jnp.where(front, a, pltpu.roll(b, BOX, 1)),
                jnp.where(front, pltpu.roll(a, BOX, 1), b),
            )
        )
    out = [None] * 4
    for i in range(2):
        a, b = half[0][i], half[1][i]
        out[i] = jnp.where(top, a, pltpu.roll(b, 4, 0))
        out[2 + i] = jnp.where(top, pltpu.roll(a, 4, 0), b)
    return out


def turn_in(src, dst):
    for s in range(16):
        tiles = [src[4 * s + c].astype(F32) for c in range(4)]
        re = corner_turn([t[0:8] for t in tiles])
        im = corner_turn([t[8:16] for t in tiles])
        for c in range(4):
            dst[4 * s + c, 0:8] = re[c]
            dst[4 * s + c, 8:16] = im[c]


def pair(ref):
    return lambda n: (ref[n, 0:8], ref[n, 8:16])


def put_pair(ref, rows, dtype):
    def store(n, value):
        ref[n, rows] = jnp.concatenate([value[0], value[1]], axis=0).astype(dtype)

    return store


def split_dot(x, high, low):
    hi = x.astype(BF16)
    lo = (x - hi.astype(F32)).astype(BF16)
    dot = functools.partial(jnp.dot, preferred_element_type=F32)
    return dot(hi, high) + dot(lo, high) + dot(hi, low)


def lanes_forward(src, first_row, high, low, dst):
    a = src[:, pl.ds(first_row, 8), :].reshape(KEPT * 8, 2 * BOX)
    b = src[:, pl.ds(first_row + 8, 8), :].reshape(KEPT * 8, 2 * BOX)
    out = split_dot(jnp.concatenate([a, b], axis=1), high, low)
    dst[0:KEPT, 0:8, :] = out[:, : 2 * BOX].reshape(KEPT, 8, 2 * BOX)
    dst[0:KEPT, 8:16, :] = out[:, 2 * BOX :].reshape(KEPT, 8, 2 * BOX)


def lanes_back(src, high, low):
    x = jnp.concatenate(
        [
            src[0:KEPT, 0:8, :].reshape(KEPT * 8, 2 * BOX),
            src[0:KEPT, 8:16, :].reshape(KEPT * 8, 2 * BOX),
        ],
        axis=1,
    )
    out = split_dot(x, high, low)
    return (
        out[:, : 2 * BOX].reshape(KEPT, 8, 2 * BOX),
        out[:, 2 * BOX :].reshape(KEPT, 8, 2 * BOX),
    )


def lane_tables():
    index = np.arange(BOX)
    angle = (index[:, None] * index[None, :] % BOX) * (2.0 * np.pi / BOX)
    c, s, z = np.cos(angle), np.sin(angle), np.zeros((BOX, BOX))
    forward = np.block([[c, z, s, z], [-s, z, c, z], [z, c, z, s], [z, -s, z, c]])
    s = -s
    back = np.block([[c, s, z, z], [z, z, c, s], [-s, c, z, z], [z, z, -s, c]])
    grid = np.block([[c, z, -s, z], [z, c, z, -s], [s, z, c, z], [z, s, z, c]])
    out = []
    for w in (forward, back, grid, grid.T):
        w = jnp.asarray(w, F32)
        high = w.astype(BF16)
        out += [high, (w - high.astype(F32)).astype(BF16)]
    return out


kept_place = lambda n: n if n <= GCUT else (n - (BOX - KEPT) if n >= BOX - GCUT else None)
KEPT_SET = frozenset(f % BOX for f in kept_freqs)
ALL_SET = frozenset(range(BOX))


def load_kept(ref):
    def load(n):
        place = kept_place(n)
        return None if place is None else (ref[place, 0:8], ref[place, 8:16])

    return load


def forward_tile(src, first_row, high, low, near, tmp, store):
    lanes_forward(src, first_row, high, low, near)
    dft64(load_kept(near), ALL_SET, tmp, store, 1)


def back_tile(src, high, low, near, tmp):
    turn_in(src, near)

    def store(n, value):
        tmp2 = near
        tmp2[kept_place(n), 0:8] = value[0]
        tmp2[kept_place(n), 8:16] = value[1]

    dft64(pair(near), KEPT_SET, tmp, store, -1)
    return lanes_back(near, high, low)


def squeeze(src, dst):
    front = front_lanes((16, 2 * BOX))
    zero = jnp.zeros((16, 2 * BOX), BF16)
    for g in range(16):
        first, second, third, guest = (src[4 * g + c].astype(BF16) for c in range(4))
        dst[3 * g] = first + pltpu.roll(jnp.where(front, guest, zero), GCUT + 1, 1)
        dst[3 * g + 1] = second + pltpu.roll(jnp.where(front, zero, guest), 2 * BOX - GCUT, 1)
        dst[3 * g + 2] = third


def turn_squeezed(src, dst, valid=None):
    front = front_lanes((16, 2 * BOX))
    left = lax.broadcasted_iota(jnp.int32, (16, 2 * BOX), 1) < BOX
    top = lax.broadcasted_iota(jnp.int32, (8, 2 * BOX), 0) < 4
    for g in range(16):
        tiles = [src[3 * g + c] for c in range(3)]
        ahead = pltpu.roll(tiles[0], 2 * BOX - GCUT - 1, 1)
        tiles.append(jnp.where(front, ahead, pltpu.roll(tiles[1], GCUT, 1)))
        half = []
        for h in range(2):
            a, b = tiles[2 * h], tiles[2 * h + 1]
            half.append(
                (
                    jnp.where(left, a, pltpu.roll(b, BOX, 1)).astype(F32),
                    jnp.where(left, pltpu.roll(a, BOX, 1), b).astype(F32),
                )
            )
        for i in range(2):
            a, b = half[0][i], half[1][i]
            if valid is not None:
                a, b = a * valid, b * valid
            for rows in (slice(0, 8), slice(8, 16)):
                x, y = a[rows], b[rows]
                dst[4 * g + i, rows] = jnp.where(top, x, pltpu.roll(y, 4, 0))
                dst[4 * g + 2 + i, rows] = jnp.where(top, pltpu.roll(x, 4, 0), y)


def natural_to_pair(src, first_row, dst):
    front = lax.broadcasted_iota(jnp.int32, (8, 2 * BOX), 1) < BOX
    for n in range(KEPT):
        a, b = src[n, pl.ds(first_row, 8), :], src[n, pl.ds(first_row + 8, 8), :]
        dst[n, 0:8] = jnp.where(front, a, pltpu.roll(b, BOX, 1))
        dst[n, 8:16] = jnp.where(front, pltpu.roll(a, BOX, 1), b)


def pair_to_natural(src, n):
    front = lax.broadcasted_iota(jnp.int32, (8, 2 * BOX), 1) < BOX
    re, im = src[n, 0:8], src[n, 8:16]
    return jnp.where(front, re, pltpu.roll(im, BOX, 1)), jnp.where(front, pltpu.roll(re, BOX, 1), im)


def grid_lanes(ref, high, low, valid=None):
    x = [ref[:, h : h + 8, :].reshape(BOX * 8, 2 * BOX) for h in (0, 8)]
    x = jnp.concatenate(x, axis=1).astype(BF16)
    out = jnp.dot(x, high, preferred_element_type=F32) + jnp.dot(x, low, preferred_element_type=F32)
    for h, lanes in ((0, slice(0, 2 * BOX)), (8, slice(2 * BOX, 4 * BOX))):
        part = out[:, lanes].reshape(BOX, 8, 2 * BOX)
        ref[:, h : h + 8, :] = part if valid is None else part * valid[0:8]


def front_lanes(shape):
    return lax.broadcasted_iota(jnp.int32, shape, len(shape) - 1) % BOX < BOX // 2


def widest(f):
    return int(math.sqrt(GCUT**2 - max(abs(f) - 0.5, 0.0) ** 2) + 0.5)


def lay_rows():
    order = sorted(kept_freqs, key=lambda f: (abs(f), -f))
    hosts, others = order[:ROWS], order[ROWS:]
    room = [[widest(f) + 1, BOX - 1 - widest(f)] for f in hosts]
    pieces = sorted(
        [(widest(f) + 1, f, True) for f in others] + [(widest(f), f, False) for f in others],
        key=lambda piece: -piece[0],
    )
    guests, where = [[] for _ in hosts], {}
    for size, f, ahead in pieces:
        fits = [r for r in range(ROWS) if room[r][1] - room[r][0] + 1 >= size]
        r = min(fits, key=lambda n: (room[n][1] - room[n][0] + 1 - size, n))
        start = room[r][0]
        shift = start if ahead else start - (BOX - size)
        room[r][0] = start + size
        guests[r].append((f, ahead, shift % (2 * BOX)))
        where[f, ahead] = (r, shift % (2 * BOX))
    return hosts, guests, where


hosts, guests, where_laid = lay_rows()


def pack_row(get, r):
    value = get(hosts[r])
    front = front_lanes(value.shape)
    for f, ahead, shift in guests[r]:
        row = get(f)
        piece = jnp.where(front, row, 0.0) if ahead else jnp.where(front, 0.0, row)
        value = value + pltpu.roll(piece, shift, value.ndim - 1)
    return value


def unpack_row(get, f):
    if f in hosts:
        return get(hosts.index(f))
    (r, up), (n, down) = where_laid[f, True], where_laid[f, False]
    first, second = get(r), get(n)
    axis = first.ndim - 1
    return jnp.where(
        front_lanes(first.shape),
        pltpu.roll(first, (2 * BOX - up) % (2 * BOX), axis),
        pltpu.roll(second, (2 * BOX - down) % (2 * BOX), axis),
    )


def lane_sign(shape):
    return jnp.where(lax.broadcasted_iota(jnp.int32, shape, len(shape) - 1) < BOX, 1.0, -1.0)


def panel_rows(panel, slots, r, p):
    rows = [jnp.concatenate([panel[d, p, n] for d in slots], axis=0) for n in (r, r + 1)]
    return jnp.concatenate(rows, axis=1)


def pack_values(values, packed):
    sign = lane_sign((48, 2 * BOX))
    for r in range(ROWS):
        straight = pack_row(lambda f: values[place_of[f]], r)
        turned = pltpu.roll(straight, BOX, 1) * sign
        packed[r] = jnp.concatenate([straight, turned], axis=0).astype(BF16)


def correlate(packed, panel, fold, slots, planes=(0, 1, 2, 3)):
    count = 64 * len(slots)
    nt = (((1,), (1,)), ((), ()))
    total = {p: None for p in planes}
    for r in range(0, ROWS, 2):
        y = jnp.concatenate([packed[r], packed[r + 1]], axis=1)
        for p in planes:
            part = lax.dot_general(
                panel_rows(panel, slots, r, p), y, nt, preferred_element_type=F32
            )
            total[p] = part if total[p] is None else total[p] + part
    column = lax.broadcasted_iota(jnp.int32, (count, 96), 1) % 16 // 4
    chosen = jnp.zeros((count, 96), F32)
    for p in planes:
        chosen = jnp.where(column == 2 * (p % 2) + p // 2, total[p], chosen)
    hi = chosen.astype(BF16)
    lo = (chosen - hi.astype(F32)).astype(BF16)
    return lax.dot_general(fold, hi, nt, preferred_element_type=F32) + lax.dot_general(
        fold, lo, nt, preferred_element_type=F32
    )


def fold_table():
    f = np.zeros((2, 3, 4, 2, 3, 4, 4), np.float32)
    for a in range(2):
        for t in range(3):
            for q in range(4):
                f[a, t, q, a, t, :, q] = 1.0
    return f.reshape(24, 96)


def spread_table():
    f = np.zeros((4, 2, 3, 2, 2, 4, 2, 3, 4), np.float32)
    for p in range(4):
        for a in range(2):
            for t in range(3):
                for q in range(4):
                    f[p, a, t, p % 2, p // 2, q, a, t, q] = 1.0
    return f.reshape(384, 24)


def multiply(corr, panel, spread, product, slots, more=False):
    rows = jnp.dot(spread[...], corr, preferred_element_type=F32).astype(BF16)
    sign = -lane_sign((48, 2 * BOX))
    for r in range(0, ROWS, 2):
        total = None
        for p in range(4):
            part = jnp.dot(
                rows[96 * p : 96 * p + 96], panel_rows(panel, slots, r, p), preferred_element_type=F32
            )
            total = part if total is None else total + part
        for c in range(2):
            lanes = slice(2 * BOX * c, 2 * BOX * (c + 1))
            value = total[:48, lanes] + pltpu.roll(total[48:, lanes], BOX, 1) * sign
            product[r + c] = product[r + c] + value if more else value


def lay_out(product, finish):
    for f in kept_freqs:
        finish(place_of[f], unpack_row(lambda r: product[r], f))


VMEM_LIMIT = 62 * 1024 * 1024
MESH = pl.DeviceIdType.MESH
vmem = pl.BlockSpec(memory_space=pltpu.VMEM)
smem = pl.BlockSpec(memory_space=pltpu.SMEM)
far = pl.BlockSpec(memory_space=pltpu.HBM)
STEP = 72
SLOTS = (0, 1, 3, 2)


def shape(dims, dtype=F32):
    return jax.ShapeDtypeStruct(dims, dtype)


def remote(src, dst, send, recv, where):
    return pltpu.make_async_remote_copy(
        src_ref=src, dst_ref=dst, send_sem=send, recv_sem=recv, device_id=where, device_id_type=MESH
    )


def away(step):
    return min(step[0], 4 - step[0]) + min(step[1], 4 - step[1])


STEPS = sorted([(y, x) for y in range(4) for x in range(4) if (y, x) != (0, 0)], key=lambda s: -away(s))


def peers(me):
    for dy, dx in STEPS:
        yield 4 * lax.rem(me // 4 + dy, 4) + lax.rem(lax.rem(me, 4) + dx, 4)


def to_peers(me, src_of, dst, send, recv):
    for g in peers(me):
        remote(src_of(g), dst, send, recv, {"ga": g}).start()


def kernel(
    psi, g_mask, fold, spread, energies, k_point, far_v, far_dv, far_tables,
    response, residual,
    v_local, dv, tables, raw, mask_rows, mask, level, solved, changes, potential, solved_rows, weights, wide_rows, panel, near, tmp, space, send_a, came_a, send_b, came_b, send_1, send_2,
    came_1, came_2, packed, product, share, shares, far_share, far_shares, source, vec, image, sums, sums_here, all_sums,
    in_sem, raw_sem, ring_send, ring_recv, a_sem, b_send, b_recv, s1, r1, s2, r2, c_send, c_recv, m_sem,
):
    me = lax.axis_index("ga")
    z = lax.axis_index("band")
    up, down = lax.rem(z + 1, 4), lax.rem(z + 3, 4)

    barrier = pltpu.get_barrier_semaphore()

    for g in peers(me):
        pl.semaphore_signal(barrier, inc=1, device_id={"ga": g}, device_id_type=MESH)
    for other in (up, down):
        pl.semaphore_signal(barrier, inc=1, device_id={"band": other}, device_id_type=MESH)

    def raw_copy(p):
        return pltpu.make_async_copy(psi.at[:, p], raw.at[p], raw_sem.at[p])

    def late_copy(n):
        src, dst = ((far_tables, tables), (far_v, v_local), (far_dv, dv))[n]
        return pltpu.make_async_copy(src, dst, in_sem.at[n])

    for p in (0, 2, 1, 3):
        raw_copy(p).start()
    for n in range(3):
        late_copy(n).start()
    fwd_hi, fwd_lo, back_hi, back_lo, up_hi, up_lo, down_hi, down_lo = (tables.at[n] for n in range(8))

    front = lax.broadcasted_iota(jnp.int32, (4, 2 * BOX), 1) < BOX
    top = lax.broadcasted_iota(jnp.int32, (8, 2 * BOX), 0) < 4
    for c in range(BOX // 2):
        both = g_mask[:, 2 * BOX * c : 2 * BOX * (c + 1)].astype(F32)
        turned = pltpu.roll(both, BOX, 1)
        for n, rows in ((2 * c, jnp.where(front, both, turned)), (2 * c + 1, jnp.where(front, turned, both))):
            for p in range(4):
                mask_rows[p, n : n + 1] = rows[p : p + 1]

    def spread_rows(first, second):
        return jnp.where(top, jnp.broadcast_to(first, (8, 2 * BOX)), jnp.broadcast_to(second, (8, 2 * BOX)))

    def pack_plane(u, carry):
        p = 2 * lax.rem(u, 2) + u // 2
        raw_copy(p).wait()

        def widen(m, c):
            wide_rows[pl.ds(pl.multiple_of(STEP * m, 8), BOX), :] = raw[p, m].astype(F32)
            return c

        lax.fori_loop(0, 64, widen, 0)

        def get(f):
            n = f % BOX
            return wide_rows[pl.ds(n, 64, stride=STEP), :] * mask_rows[p, n : n + 1]

        for r in range(ROWS):
            panel[0, p, r] = pack_row(get, r).astype(BF16)
        return carry

    lax.fori_loop(0, 2, pack_plane, 0)
    pl.semaphore_wait(barrier, 17)

    def ring(src_slot, dst_slot, p, where, n):
        return remote(
            panel.at[src_slot, p], panel.at[dst_slot, p], ring_send.at[n], ring_recv.at[dst_slot, p],
            {"band": where},
        )

    def ring_up(p):
        return ring(0, 3, p, up, p)

    def ring_down(p):
        return ring(0, 1, p, down, 4 + p)

    ring_up(0).start()
    ring_down(2).start()
    lax.fori_loop(2, 4, pack_plane, 0)
    ring_up(1).start()
    ring_down(3).start()
    ring_up(2).start()
    ring_down(0).start()
    ring_up(3).start()
    ring_down(1).start()

    for i in range(2):
        for k in range(2):
            for q in range(4):
                solved_rows[pl.ds(STEP * (8 * i + 4 * k + q), BOX), :] = raw[2 * k + i, STRIDE * q].astype(F32)
    for f in kept_freqs:
        n = f % BOX
        for i in range(2):
            rows = mask_rows[i, n : n + 1], mask_rows[2 + i, n : n + 1]
            mask[place_of[f], 8 * i : 8 * i + 8] = spread_rows(*rows)
        solved[place_of[f]] = solved_rows[pl.ds(n, 16, stride=STEP), :] * mask[place_of[f]]
    for n in range(3):
        late_copy(n).wait()
    forward_tile(solved, 0, fwd_hi[...], fwd_lo[...], near, tmp, put_pair(send_a, slice(0, 16), F32))

    mine = pl.ds(4 * me, 4)
    to_peers(me, lambda g: send_a.at[pl.ds(4 * g, 4)], came_a.at[mine], a_sem.at[0], a_sem.at[1])
    came_a[mine] = send_a[mine]

    def spread_field(n, carry):
        line = v_local[pl.ds(n, 1), :]
        potential[n] = spread_rows(line[:, : 2 * BOX], line[:, 2 * BOX :])
        for p in range(NPERT):
            line = dv[p, pl.ds(n, 1), :]
            changes[p, n] = spread_rows(line[:, : 2 * BOX], line[:, 2 * BOX :])
        return carry

    lax.fori_loop(0, BOX, spread_field, 0)

    factor = 0.5 * (2.0 * math.pi / cell_length) ** 2
    row = lax.broadcasted_iota(jnp.int32, (8, 2 * BOX), 0)
    third = lax.broadcasted_iota(jnp.int32, (8, 2 * BOX), 1) % BOX
    third = jnp.where(third < BOX // 2, third, third - BOX).astype(F32)
    for i in range(2):
        first = 4 * me + 2 * (row // 4) + i
        first = jnp.where(first < BOX // 2, first, first - BOX).astype(F32)
        still = factor * ((first + k_point[0]) ** 2 + (third + k_point[2]) ** 2)
        for q in range(4):
            still = jnp.where(row % 4 == q, still - energies[q], still)
        for f in kept_freqs:
            here = mask[place_of[f], 8 * i : 8 * i + 8]
            rise = factor * (float(f) + k_point[1]) * (float(f) + k_point[1])
            level[place_of[f], 8 * i : 8 * i + 8] = (still + rise) * here
            mask[place_of[f], 8 * i : 8 * i + 8] = here * (1.0 / BOX**3)

    def wait_all(src, dst, send, recv):
        return remote(src, dst, send, recv, {"ga": lax.rem(me + 1, 16)})

    every = pl.ds(0, 60)
    wait_all(send_a.at[every], came_a.at[every], a_sem.at[0], a_sem.at[1]).wait()

    turn_in(came_a, near)

    def keep(n, value):
        space[n, 0:8] = value[0]
        space[n, 8:16] = value[1]

    dft64(pair(near), ALL_SET, tmp, keep, 1)

    def each_change(p, carry):
        def load(n):
            d = changes[p, n]
            return (space[n, 0:8] * d, space[n, 8:16] * d)

        dft64(load, ALL_SET, tmp, put_pair(send_b.at[p], slice(0, 16), F32), -1)
        to_peers(
            me, lambda g: send_b.at[p, pl.ds(4 * g, 4)], came_b.at[p, mine], b_send.at[p], b_recv.at[p]
        )
        came_b[p, mine] = send_b[p, mine]
        return carry

    lax.fori_loop(0, NPERT, each_change, 0)

    def pass_on(p_up, p_down):
        ring(0, 3, p_up, up, p_up).wait_recv()
        first = ring(3, 2, p_up, up, 8 + p_up)
        first.start()
        ring(0, 1, p_down, down, 4 + p_down).wait_recv()
        second = ring(1, 2, p_down, down, 8 + p_down)
        second.start()

    pass_on(0, 2)
    pass_on(1, 3)

    def back(came, dst_add):
        def each(t, carry):
            dst_add(t)
            return carry

        lax.fori_loop(0, 3, each, 0)

    def source_tile(t):
        wait_all(send_b.at[t, every], came_b.at[t, every], b_send.at[t], b_recv.at[t]).wait()
        start = pl.multiple_of(16 * t, 16)
        a, b = back_tile(came_b.at[t], back_hi[...], back_lo[...], near, tmp)
        source[:, pl.ds(start, 8), :] = a * mask[:, 0:8, :]
        source[:, pl.ds(start + 8, 8), :] = b * mask[:, 8:16, :]

    back(came_b, source_tile)

    def send_share(n, src):
        to_peers(me, lambda g: src, shares.at[n, me], c_send.at[n], c_recv.at[n])

    def total_share(n):
        first = pl.ds(0, 15)
        wait_all(shares.at[n, first], shares.at[n, first], c_send.at[n], c_recv.at[n]).wait()
        total = shares[n, 0].astype(F32)
        for g in range(1, 16):
            total = total + shares[n, g].astype(F32)
        return total.astype(BF16)

    pack_values(source, packed)
    for p in range(2, 4):
        ring(0, 3, p, up, p).wait_recv()
    for p in range(2):
        ring(0, 1, p, down, 4 + p).wait_recv()
    early = correlate(packed, panel, fold[...], SLOTS[:3]).astype(BF16)
    share[0] = jnp.concatenate([early, jnp.zeros((24, 64), BF16)], axis=1)
    shares[0, me] = share[0]
    send_share(0, share.at[0])
    ring(3, 2, 0, up, 8).wait_recv()
    ring(1, 2, 2, down, 10).wait_recv()
    late = correlate(packed, panel, fold[...], SLOTS[3:], (0, 2))
    multiply(total_share(0)[:, :192], panel, spread, product, SLOTS[:3])
    ring(3, 2, 1, up, 9).wait_recv()
    ring(1, 2, 3, down, 11).wait_recv()
    late = late + correlate(packed, panel, fold[...], SLOTS[3:], (1, 3))
    far_share[...] = jnp.concatenate([late.astype(BF16), jnp.zeros((24, 64), BF16)], axis=1)
    far_shares[me] = far_share[...]
    to_peers(me, lambda g: far_share, far_shares.at[me], c_send.at[3], c_recv.at[3])

    def first_row(place, row):
        for t in range(3):
            rows = slice(16 * t, 16 * t + 16)
            vec[0, place, rows] = row[rows] * mask[place] - source[place, rows]

    first = pl.ds(0, 15)
    wait_all(far_shares.at[first], far_shares.at[first], c_send.at[3], c_recv.at[3]).wait()
    total = far_shares[0].astype(F32)
    for g in range(1, 16):
        total = total + far_shares[g].astype(F32)
    multiply(total.astype(BF16)[:, :64], panel, spread, product, SLOTS[3:], True)
    lay_out(product, first_row)

    lane = lax.broadcasted_iota(jnp.int32, (8, 2 * BOX), 1)
    mine3, most = pl.ds(3 * me, 3), pl.ds(0, 45)
    third = lax.broadcasted_iota(jnp.int32, (16, 2 * BOX), 1) % BOX
    third = jnp.where(third < BOX // 2, third, third - BOX)
    side = jnp.minimum(jnp.maximum(4.0 * k_point[2], -1.0), 1.0)
    edge = jnp.where(third == GCUT, 0.5 - 0.5 * side, jnp.where(third == -GCUT, 0.5 + 0.5 * side, 0.0))
    valid = jnp.where(jnp.abs(third) < GCUT, 1.0, edge)

    def apply(it, carry):
        def near_tile(t, c):
            natural_to_pair(vec.at[it], pl.multiple_of(16 * t, 16), near)
            dft64(load_kept(near), ALL_SET, tmp, put_pair(space, slice(0, 16), F32), 1)
            squeeze(space, send_1.at[it, t])
            to_peers(
                me, lambda g: send_1.at[it, t, pl.ds(3 * g, 3)], came_1.at[it, t, mine3],
                s1.at[it, t], r1.at[it, t],
            )
            came_1[it, t, mine3] = send_1[it, t, mine3]
            return c

        lax.fori_loop(0, 3, near_tile, 0)

        pack_values(vec.at[it], packed)
        n = it + 1
        share[n] = correlate(packed, panel, fold[...], SLOTS).astype(BF16)
        shares[n, me] = share[n]
        send_share(n, share.at[n])

        def space_tile(t, c):
            wait_all(send_1.at[it, t, most], came_1.at[it, t, most], s1.at[it, t], r1.at[it, t]).wait()
            turn_squeezed(came_1.at[it, t], near, valid)
            grid_lanes(near, up_hi[...], up_lo[...])

            weight = [jnp.zeros((8, 2 * BOX), F32)]

            def with_potential(k, value):
                v = potential[k]
                re, im = value[0] * v, value[1] * v
                near[k, 0:8] = re
                near[k, 8:16] = im
                weight[0] = weight[0] + (value[0] * re + value[1] * im)

            dft64(pair(near), ALL_SET, tmp, with_potential, 1)
            weights[t] = weight[0]
            dft64(pair(near), ALL_SET, tmp, put_pair(near, slice(0, 16), F32), -1)
            grid_lanes(near, down_hi[...], down_lo[...], valid)
            squeeze(near, send_2.at[it, t])
            to_peers(
                me, lambda g: send_2.at[it, t, pl.ds(3 * g, 3)], came_2.at[it, t, mine3],
                s2.at[it, t], r2.at[it, t],
            )
            came_2[it, t, mine3] = send_2[it, t, mine3]
            return c

        lax.fori_loop(0, 3, space_tile, 0)

        def with_level(place, row):
            for t in range(3):
                rows = slice(16 * t, 16 * t + 16)
                image[it, place, rows] = (
                    row[rows] * (shift_weight * mask[place])
                    + level[place] * vec[it, place, rows]
                )

        corr = total_share(n)

        @pl.when(it == 1)
        def _():
            def moments(place, totals):
                b, ab, w = vec[0, place], image[0, place], vec[1, place]
                lift = jnp.concatenate([level[place]] * 3, axis=0)
                return tuple(x + y for x, y in zip(totals, (b * b, b * ab, ab * ab, lift * w * w)))

            zero = jnp.zeros((48, 2 * BOX), F32)
            totals = lax.fori_loop(0, KEPT, moments, (zero,) * 4)
            own = jnp.zeros((8, 2 * BOX), F32)
            for m, total in enumerate(totals):
                line = jnp.sum(total, axis=1, keepdims=True) * (1.0 / BOX**3)
                for t in range(3):
                    both = line[16 * t : 16 * t + 8] + line[16 * t + 8 : 16 * t + 16]
                    if m == 3:
                        both = both + jnp.sum(weights[t], axis=1, keepdims=True) * (1.0 / BOX**6)
                    own = jnp.where(lane == 4 * t + m, jnp.broadcast_to(both, own.shape), own)
            own = own + pltpu.roll(own, 4, 0)
            sums[...] = own
            all_sums[me] = own
            to_peers(me, lambda g: sums, all_sums.at[me], m_sem.at[0], m_sem.at[1])
            square = corr.astype(F32)
            square = jnp.sum(square * square, axis=1, keepdims=True) * (shift_weight / BOX**6)
            rest = jnp.zeros((8, 2 * BOX), F32)
            for t in range(3):
                four = square[4 * t : 4 * t + 4] + square[12 + 4 * t : 16 + 4 * t]
                eight = jnp.concatenate([four, four], axis=0)
                rest = jnp.where(lane == 4 * t + 3, jnp.broadcast_to(eight, rest.shape), rest)
            sums_here[...] = rest

        multiply(corr, panel, spread, product, SLOTS)
        lay_out(product, with_level)

        def far_tile(t, c):
            wait_all(send_2.at[it, t, most], came_2.at[it, t, most], s2.at[it, t], r2.at[it, t]).wait()
            start = pl.multiple_of(16 * t, 16)
            turn_squeezed(came_2.at[it, t], near)

            def to_near(n, value):
                near[kept_place(n), 0:8] = value[0]
                near[kept_place(n), 8:16] = value[1]

            dft64(pair(near), KEPT_SET, tmp, to_near, -1)
            for n in range(KEPT):
                for half, value in zip((0, 8), pair_to_natural(near, n)):
                    rows = pl.ds(start + half, 8)
                    total = image[it, n, rows, :] + value * mask[n, half : half + 8]
                    image[it, n, rows, :] = total
                    vec[it + 1, n, rows, :] = total - SHIFT * vec[it, n, rows, :]
            return c

        lax.fori_loop(0, 3, far_tile, 0)
        return carry

    lax.fori_loop(0, 2, apply, 0)

    first = pl.ds(0, 15)
    wait_all(all_sums.at[first], all_sums.at[first], m_sem.at[0], m_sem.at[1]).wait()
    m0 = sums_here[...] + all_sums[0]
    for g in range(1, 16):
        m0 = m0 + all_sums[g]
    m1, m2, m3 = (pltpu.roll(m0, 2 * BOX - n, 1) for n in (1, 2, 3))
    step0 = m0 / m1
    fresh = m0 - 2.0 * step0 * m1 + step0 * step0 * m2
    u = 1.0 + fresh / m0 - step0 * SHIFT
    curve = u * u * m1 - 2.0 * u * step0 * (m2 - SHIFT * m1) + step0 * step0 * m3
    step1 = fresh / curve
    low_part, high_part = step0 + step1 * u, step1 * step0
    for t in range(3):
        a = jnp.broadcast_to(low_part[:, 4 * t : 4 * t + 1], (8, 2 * BOX))
        e = jnp.broadcast_to(high_part[:, 4 * t : 4 * t + 1], (8, 2 * BOX))
        for half in (0, 8):
            rows = slice(16 * t + half, 16 * t + half + 8)
            b, ab = vec[0, :, rows, :], image[0, :, rows, :]
            response[:, rows, :] = a * b - e * vec[1, :, rows, :]
            residual[:, rows, :] = b - a * ab + e * image[1, :, rows, :]

    for p in range(4):
        ring_up(p).wait_send()
        ring_down(p).wait_send()
    for p in range(2):
        ring(3, 2, p, up, 8 + p).wait_send()
    for p in range(2, 4):
        ring(1, 2, p, down, 8 + p).wait_send()


def run(*args):
    grid_f = pltpu.VMEM((BOX, 16, 2 * BOX), F32)
    three_f = pltpu.VMEM((3, BOX, 16, 2 * BOX), F32)
    six_b = pltpu.VMEM((2, 3, 48, 16, 2 * BOX), BF16)
    natural = (KEPT, 48, 2 * BOX)
    dma = pltpu.SemaphoreType.DMA
    return pl.pallas_call(
        kernel,
        out_shape=(shape(natural), shape(natural)),
        in_specs=[far] + [vmem] * 3 + [smem] * 2 + [far] * 3,
        out_specs=(vmem, vmem),
        scratch_shapes=[
            pltpu.VMEM((BOX, 4 * BOX), F32),
            pltpu.VMEM((NPERT, BOX, 4 * BOX), F32),
            pltpu.VMEM((8, 4 * BOX, 4 * BOX), BF16),
            pltpu.VMEM((4, 64, BOX, 2 * BOX), BF16),
            pltpu.VMEM((4, BOX, 2 * BOX), F32),
            pltpu.VMEM((KEPT, 16, 2 * BOX), F32),
            pltpu.VMEM((KEPT, 16, 2 * BOX), F32),
            pltpu.VMEM((KEPT, 16, 2 * BOX), F32),
            pltpu.VMEM((NPERT, BOX, 8, 2 * BOX), F32),
            pltpu.VMEM((BOX, 8, 2 * BOX), F32),
            pltpu.VMEM((16 * STEP, 2 * BOX), F32),
            pltpu.VMEM((3, 8, 2 * BOX), F32),
            pltpu.VMEM((64 * STEP, 2 * BOX), F32),
            pltpu.VMEM((4, 4, ROWS, 64, 2 * BOX), BF16),
            grid_f, grid_f, grid_f,
            grid_f, grid_f, three_f, three_f, six_b, six_b, six_b, six_b,
            pltpu.VMEM((ROWS, 96, 2 * BOX), BF16),
            pltpu.VMEM((ROWS, 48, 2 * BOX), F32),
            pltpu.VMEM((3, 24, 256), BF16),
            pltpu.VMEM((3, 16, 24, 256), BF16),
            pltpu.VMEM((24, 128), BF16),
            pltpu.VMEM((16, 24, 128), BF16),
            pltpu.VMEM(natural, F32),
            pltpu.VMEM((3, *natural), F32),
            pltpu.VMEM((2, *natural), F32),
            pltpu.VMEM((8, 2 * BOX), F32),
            pltpu.VMEM((8, 2 * BOX), F32),
            pltpu.VMEM((16, 8, 2 * BOX), F32),
            dma((3,)), dma((4,)), dma((12,)), dma((4, 4)), dma((2,)), dma((3,)), dma((3,)),
            dma((2, 3)), dma((2, 3)), dma((2, 3)), dma((2, 3)), dma((4,)), dma((4,)), dma((2,)),
        ],
        compiler_params=pltpu.CompilerParams(
            vmem_limit_bytes=VMEM_LIMIT, collective_id=0, has_side_effects=True
        ),
    )(*args)


def place_body(response, residual, first, second, stage, buffer, in_sem, sem):
    pairs = ((0, response, first), (1, residual, second))

    def come(w, src, t):
        return pltpu.make_async_copy(
            src.at[:, pl.ds(16 * t, 16)], stage.at[w, t, :, pl.ds(0, 16)], in_sem.at[w, t]
        )

    def leave(w, out, t, q):
        part = pl.ds(12 * q + 4 * t, 4)
        return pltpu.make_async_copy(buffer.at[w, part], out.at[part], sem.at[w, t, q])

    for t in range(NPERT):
        for w, src, _ in pairs:
            come(w, src, t).start()
    for t in range(NPERT):
        for w, src, out in pairs:
            come(w, src, t).wait()
            flat = stage.at[w, t].reshape(KEPT * 24, 2 * BOX)
            for q in range(4):
                for p in range(4):
                    row = 8 * (p % 2) + 4 * (p // 2) + q
                    to = 12 * q + 4 * t + p
                    buffer[w, to, 0 : GCUT + 1] = flat[pl.ds(row, GCUT + 1, stride=24), :]
                    buffer[w, to, GCUT + 1 : BOX - GCUT] = jnp.zeros((BOX - KEPT, 2 * BOX), F32)
                    buffer[w, to, BOX - GCUT :] = flat[pl.ds(row + 24 * (GCUT + 1), GCUT, stride=24), :]
                leave(w, out, t, q).start()
    for t in range(NPERT):
        for w, _, out in pairs:
            for q in range(4):
                leave(w, out, t, q).wait()


def place(*values):
    out = shape((48, BOX, 2 * BOX))
    outs = pl.pallas_call(
        place_body,
        out_shape=(out, out),
        in_specs=[pl.BlockSpec(memory_space=pl.ANY)] * 2,
        out_specs=(pl.BlockSpec(memory_space=pl.ANY),) * 2,
        scratch_shapes=[
            pltpu.VMEM((2, NPERT, KEPT, 24, 2 * BOX), F32),
            pltpu.VMEM((2, 48, BOX, 2 * BOX), F32),
            pltpu.SemaphoreType.DMA((2, NPERT)),
            pltpu.SemaphoreType.DMA((2, NPERT, 4)),
        ],
        compiler_params=pltpu.CompilerParams(vmem_limit_bytes=VMEM_LIMIT),
    )(*values)
    return tuple(v.reshape(4, NPERT, 4, BOX, 2 * BOX) for v in outs)


def on_device(psi_occ, energies, k_point, g_mask, v_local, dv):
    response, residual = run(
        psi_occ, g_mask, jnp.asarray(fold_table(), BF16), jnp.asarray(spread_table(), BF16),
        energies, k_point, v_local, dv, jnp.stack(lane_tables()),
    )

    return place(response, residual)


def solution(mesh):
    placed = (
        P(("pool", "band"), "ga", None, None),
        P(("pool", "band")),
        P("pool"),
        P(("pool", "ga"), None),
        P(None, "ga"),
        P(None, None, "ga"),
    )
    return jax.shard_map(
        on_device,
        mesh=mesh,
        in_specs=placed,
        out_specs=(
            P(("pool", "band"), None, "ga", None, None),
            P(("pool", "band"), None, "ga", None, None),
        ),
        check_vma=False,
    )
```

```python
import functools
import math

import jax
import jax.numpy as jnp
import numpy as np
from jax import lax
from jax.experimental import pallas as pl
from jax.experimental.pallas import tpu as pltpu
from jax.sharding import PartitionSpec as P

BOX = 64
GCUT = 21
KEPT = 2 * GCUT + 1
NPERT = 3
STRIDE = 16
SHIFT = 16.0
ROWS = 24

cell_length = 16.5
shift_weight = 8.0

kept_freqs = list(range(GCUT + 1)) + list(range(-GCUT, 0))
place_of = {f: i for i, f in enumerate(kept_freqs)}
F32 = jnp.float32
BF16 = jnp.bfloat16


def add(a, b):
    if a is None:
        return b
    if b is None:
        return a
    return (a[0] + b[0], a[1] + b[1])


def sub(a, b):
    if b is None:
        return a
    if a is None:
        return (-b[0], -b[1])
    return (a[0] - b[0], a[1] - b[1])


def times_phase(a, turns, sign):
    if a is None:
        return None
    turns = turns % 1.0
    re, im = a
    if turns == 0.0:
        return a
    if turns == 0.5:
        return (-re, -im)
    if turns in (0.25, 0.75):
        if (turns == 0.25) == (sign > 0):
            return (-im, re)
        return (im, -re)
    c, s = math.cos(2 * math.pi * turns), sign * math.sin(2 * math.pi * turns)
    if turns in (0.125, 0.375, 0.625, 0.875):
        h = abs(c)
        if (c > 0) == (s > 0):
            pair = ((re - im) * h, (re + im) * h)
        else:
            pair = ((re + im) * h, (im - re) * h)
        return pair if c > 0 else (-pair[0], -pair[1])
    return (re * c - im * s, im * c + re * s)


def small_dft(xs, sign):
    n = len(xs)
    if n == 1:
        return xs
    even, odd = small_dft(xs[0::2], sign), small_dft(xs[1::2], sign)
    turned = [times_phase(o, k / n, sign) for k, o in enumerate(odd)]
    return [add(e, o) for e, o in zip(even, turned)] + [sub(e, o) for e, o in zip(even, turned)]


def dft64(load, keep, tmp, store, sign):
    for n2 in range(8):
        out = small_dft([load(8 * n1 + n2) for n1 in range(8)], sign)
        for k1 in range(8):
            re, im = times_phase(out[k1], n2 * k1 / 64.0, sign)
            tmp[8 * n2 + k1, 0:8] = re
            tmp[8 * n2 + k1, 8:16] = im
    for k1 in range(8):
        if not any((k1 + 8 * k2) in keep for k2 in range(8)):
            continue
        out = small_dft([(tmp[8 * n2 + k1, 0:8], tmp[8 * n2 + k1, 8:16]) for n2 in range(8)], sign)
        for k2 in range(8):
            if (k1 + 8 * k2) in keep:
                store(k1 + 8 * k2, out[k2])


def corner_turn(block):
    front = lax.broadcasted_iota(jnp.int32, (8, 2 * BOX), 1) < BOX
    top = lax.broadcasted_iota(jnp.int32, (8, 2 * BOX), 0) < 4
    half = []
    for h in range(2):
        a, b = block[2 * h], block[2 * h + 1]
        half.append(
            (
                jnp.where(front, a, pltpu.roll(b, BOX, 1)),
                jnp.where(front, pltpu.roll(a, BOX, 1), b),
            )
        )
    out = [None] * 4
    for i in range(2):
        a, b = half[0][i], half[1][i]
        out[i] = jnp.where(top, a, pltpu.roll(b, 4, 0))
        out[2 + i] = jnp.where(top, pltpu.roll(a, 4, 0), b)
    return out


def turn_in(src, dst):
    for s in range(16):
        tiles = [src[4 * s + c].astype(F32) for c in range(4)]
        re = corner_turn([t[0:8] for t in tiles])
        im = corner_turn([t[8:16] for t in tiles])
        for c in range(4):
            dst[4 * s + c, 0:8] = re[c]
            dst[4 * s + c, 8:16] = im[c]


def pair(ref):
    return lambda n: (ref[n, 0:8], ref[n, 8:16])


def put_pair(ref, rows, dtype):
    def store(n, value):
        ref[n, rows] = jnp.concatenate([value[0], value[1]], axis=0).astype(dtype)

    return store


def split_dot(x, high, low):
    hi = x.astype(BF16)
    lo = (x - hi.astype(F32)).astype(BF16)
    dot = functools.partial(jnp.dot, preferred_element_type=F32)
    return dot(hi, high) + dot(lo, high) + dot(hi, low)


def lanes_forward(src, first_row, high, low, dst):
    a = src[:, pl.ds(first_row, 8), :].reshape(KEPT * 8, 2 * BOX)
    b = src[:, pl.ds(first_row + 8, 8), :].reshape(KEPT * 8, 2 * BOX)
    out = split_dot(jnp.concatenate([a, b], axis=1), high, low)
    dst[0:KEPT, 0:8, :] = out[:, : 2 * BOX].reshape(KEPT, 8, 2 * BOX)
    dst[0:KEPT, 8:16, :] = out[:, 2 * BOX :].reshape(KEPT, 8, 2 * BOX)


def lanes_back(src, high, low):
    x = jnp.concatenate(
        [
            src[0:KEPT, 0:8, :].reshape(KEPT * 8, 2 * BOX),
            src[0:KEPT, 8:16, :].reshape(KEPT * 8, 2 * BOX),
        ],
        axis=1,
    )
    out = split_dot(x, high, low)
    return (
        out[:, : 2 * BOX].reshape(KEPT, 8, 2 * BOX),
        out[:, 2 * BOX :].reshape(KEPT, 8, 2 * BOX),
    )


def lane_tables():
    index = np.arange(BOX)
    angle = (index[:, None] * index[None, :] % BOX) * (2.0 * np.pi / BOX)
    c, s, z = np.cos(angle), np.sin(angle), np.zeros((BOX, BOX))
    forward = np.block([[c, z, s, z], [-s, z, c, z], [z, c, z, s], [z, -s, z, c]])
    s = -s
    back = np.block([[c, s, z, z], [z, z, c, s], [-s, c, z, z], [z, z, -s, c]])
    grid = np.block([[c, z, -s, z], [z, c, z, -s], [s, z, c, z], [z, s, z, c]])
    out = []
    for w in (forward, back, grid, grid.T):
        w = jnp.asarray(w, F32)
        high = w.astype(BF16)
        out += [high, (w - high.astype(F32)).astype(BF16)]
    return out


kept_place = lambda n: n if n <= GCUT else (n - (BOX - KEPT) if n >= BOX - GCUT else None)
KEPT_SET = frozenset(f % BOX for f in kept_freqs)
ALL_SET = frozenset(range(BOX))


def load_kept(ref):
    def load(n):
        place = kept_place(n)
        return None if place is None else (ref[place, 0:8], ref[place, 8:16])

    return load


def forward_tile(src, first_row, high, low, near, tmp, store):
    lanes_forward(src, first_row, high, low, near)
    dft64(load_kept(near), ALL_SET, tmp, store, 1)


def back_tile(src, high, low, near, tmp):
    turn_in(src, near)

    def store(n, value):
        tmp2 = near
        tmp2[kept_place(n), 0:8] = value[0]
        tmp2[kept_place(n), 8:16] = value[1]

    dft64(pair(near), KEPT_SET, tmp, store, -1)
    return lanes_back(near, high, low)


def squeeze(src, dst):
    front = front_lanes((16, 2 * BOX))
    zero = jnp.zeros((16, 2 * BOX), BF16)
    for g in range(16):
        first, second, third, guest = (src[4 * g + c].astype(BF16) for c in range(4))
        dst[3 * g] = first + pltpu.roll(jnp.where(front, guest, zero), GCUT + 1, 1)
        dst[3 * g + 1] = second + pltpu.roll(jnp.where(front, zero, guest), 2 * BOX - GCUT, 1)
        dst[3 * g + 2] = third


def turn_squeezed(src, dst, valid=None):
    front = front_lanes((16, 2 * BOX))
    left = lax.broadcasted_iota(jnp.int32, (16, 2 * BOX), 1) < BOX
    top = lax.broadcasted_iota(jnp.int32, (8, 2 * BOX), 0) < 4
    for g in range(16):
        tiles = [src[3 * g + c] for c in range(3)]
        ahead = pltpu.roll(tiles[0], 2 * BOX - GCUT - 1, 1)
        tiles.append(jnp.where(front, ahead, pltpu.roll(tiles[1], GCUT, 1)))
        half = []
        for h in range(2):
            a, b = tiles[2 * h], tiles[2 * h + 1]
            half.append(
                (
                    jnp.where(left, a, pltpu.roll(b, BOX, 1)).astype(F32),
                    jnp.where(left, pltpu.roll(a, BOX, 1), b).astype(F32),
                )
            )
        for i in range(2):
            a, b = half[0][i], half[1][i]
            if valid is not None:
                a, b = a * valid, b * valid
            for rows in (slice(0, 8), slice(8, 16)):
                x, y = a[rows], b[rows]
                dst[4 * g + i, rows] = jnp.where(top, x, pltpu.roll(y, 4, 0))
                dst[4 * g + 2 + i, rows] = jnp.where(top, pltpu.roll(x, 4, 0), y)


def natural_to_pair(src, first_row, dst):
    front = lax.broadcasted_iota(jnp.int32, (8, 2 * BOX), 1) < BOX
    for n in range(KEPT):
        a, b = src[n, pl.ds(first_row, 8), :], src[n, pl.ds(first_row + 8, 8), :]
        dst[n, 0:8] = jnp.where(front, a, pltpu.roll(b, BOX, 1))
        dst[n, 8:16] = jnp.where(front, pltpu.roll(a, BOX, 1), b)


def pair_to_natural(src, n):
    front = lax.broadcasted_iota(jnp.int32, (8, 2 * BOX), 1) < BOX
    re, im = src[n, 0:8], src[n, 8:16]
    return jnp.where(front, re, pltpu.roll(im, BOX, 1)), jnp.where(front, pltpu.roll(re, BOX, 1), im)


def grid_lanes(ref, high, low, valid=None):
    x = [ref[:, h : h + 8, :].reshape(BOX * 8, 2 * BOX) for h in (0, 8)]
    x = jnp.concatenate(x, axis=1).astype(BF16)
    both = jnp.concatenate([high, low], axis=0)
    out = jnp.dot(jnp.concatenate([x, x], axis=1), both, preferred_element_type=F32)
    for h, lanes in ((0, slice(0, 2 * BOX)), (8, slice(2 * BOX, 4 * BOX))):
        part = out[:, lanes].reshape(BOX, 8, 2 * BOX)
        ref[:, h : h + 8, :] = part if valid is None else part * valid[0:8]


def front_lanes(shape):
    return lax.broadcasted_iota(jnp.int32, shape, len(shape) - 1) % BOX < BOX // 2


def widest(f):
    return int(math.sqrt(GCUT**2 - max(abs(f) - 0.5, 0.0) ** 2) + 0.5)


def lay_rows():
    order = sorted(kept_freqs, key=lambda f: (abs(f), -f))
    hosts, others = order[:ROWS], order[ROWS:]
    room = [[widest(f) + 1, BOX - 1 - widest(f)] for f in hosts]
    pieces = sorted(
        [(widest(f) + 1, f, True) for f in others] + [(widest(f), f, False) for f in others],
        key=lambda piece: -piece[0],
    )
    guests, where = [[] for _ in hosts], {}
    for size, f, ahead in pieces:
        fits = [r for r in range(ROWS) if room[r][1] - room[r][0] + 1 >= size]
        r = min(fits, key=lambda n: (room[n][1] - room[n][0] + 1 - size, n))
        start = room[r][0]
        shift = start if ahead else start - (BOX - size)
        room[r][0] = start + size
        guests[r].append((f, ahead, shift % (2 * BOX)))
        where[f, ahead] = (r, shift % (2 * BOX))
    return hosts, guests, where


hosts, guests, where_laid = lay_rows()


def pack_row(get, r):
    value = get(hosts[r])
    front = front_lanes(value.shape)
    for f, ahead, shift in guests[r]:
        row = get(f)
        piece = jnp.where(front, row, 0.0) if ahead else jnp.where(front, 0.0, row)
        value = value + pltpu.roll(piece, shift, value.ndim - 1)
    return value


def unpack_row(get, f):
    if f in hosts:
        return get(hosts.index(f))
    (r, up), (n, down) = where_laid[f, True], where_laid[f, False]
    first, second = get(r), get(n)
    axis = first.ndim - 1
    return jnp.where(
        front_lanes(first.shape),
        pltpu.roll(first, (2 * BOX - up) % (2 * BOX), axis),
        pltpu.roll(second, (2 * BOX - down) % (2 * BOX), axis),
    )


def lane_sign(shape):
    return jnp.where(lax.broadcasted_iota(jnp.int32, shape, len(shape) - 1) < BOX, 1.0, -1.0)


def panel_rows(panel, slots, r, p):
    rows = [jnp.concatenate([panel[d, p, n] for d in slots], axis=0) for n in (r, r + 1)]
    return jnp.concatenate(rows, axis=1)


def pack_values(values, packed):
    sign = lane_sign((48, 2 * BOX))
    for r in range(ROWS):
        straight = pack_row(lambda f: values[place_of[f]], r)
        turned = pltpu.roll(straight, BOX, 1) * sign
        packed[r] = jnp.concatenate([straight, turned], axis=0).astype(BF16)


def correlate(packed, panel, fold, slots, planes=(0, 1, 2, 3)):
    count = 64 * len(slots)
    nt = (((1,), (1,)), ((), ()))
    total = {p: None for p in planes}
    for r in range(0, ROWS, 2):
        y = jnp.concatenate([packed[r], packed[r + 1]], axis=1)
        for p in planes:
            part = lax.dot_general(
                panel_rows(panel, slots, r, p), y, nt, preferred_element_type=F32
            )
            total[p] = part if total[p] is None else total[p] + part
    column = lax.broadcasted_iota(jnp.int32, (count, 96), 1) % 16 // 4
    chosen = jnp.zeros((count, 96), F32)
    for p in planes:
        chosen = jnp.where(column == 2 * (p % 2) + p // 2, total[p], chosen)
    hi = chosen.astype(BF16)
    lo = (chosen - hi.astype(F32)).astype(BF16)
    return lax.dot_general(fold, hi, nt, preferred_element_type=F32) + lax.dot_general(
        fold, lo, nt, preferred_element_type=F32
    )


def fold_table():
    f = np.zeros((2, 3, 4, 2, 3, 4, 4), np.float32)
    for a in range(2):
        for t in range(3):
            for q in range(4):
                f[a, t, q, a, t, :, q] = 1.0
    return f.reshape(24, 96)


def spread_table():
    f = np.zeros((4, 2, 3, 2, 2, 4, 2, 3, 4), np.float32)
    for p in range(4):
        for a in range(2):
            for t in range(3):
                for q in range(4):
                    f[p, a, t, p % 2, p // 2, q, a, t, q] = 1.0
    return f.reshape(384, 24)


def multiply(corr, panel, spread, product, slots, more=False):
    rows = jnp.dot(spread[...], corr, preferred_element_type=F32).astype(BF16)
    rows = jnp.concatenate([rows[96 * p : 96 * p + 96] for p in range(4)], axis=1)
    sign = -lane_sign((48, 2 * BOX))
    for r in range(0, ROWS, 2):
        bands = jnp.concatenate([panel_rows(panel, slots, r, p) for p in range(4)], axis=0)
        total = jnp.dot(rows, bands, preferred_element_type=F32)
        for c in range(2):
            lanes = slice(2 * BOX * c, 2 * BOX * (c + 1))
            value = total[:48, lanes] + pltpu.roll(total[48:, lanes], BOX, 1) * sign
            product[r + c] = product[r + c] + value if more else value


def lay_out(product, finish):
    for f in kept_freqs:
        finish(place_of[f], unpack_row(lambda r: product[r], f))


VMEM_LIMIT = 62 * 1024 * 1024
MESH = pl.DeviceIdType.MESH
vmem = pl.BlockSpec(memory_space=pltpu.VMEM)
smem = pl.BlockSpec(memory_space=pltpu.SMEM)
far = pl.BlockSpec(memory_space=pltpu.HBM)
STEP = 72
SLOTS = (0, 1, 3, 2)


def shape(dims, dtype=F32):
    return jax.ShapeDtypeStruct(dims, dtype)


def remote(src, dst, send, recv, where):
    return pltpu.make_async_remote_copy(
        src_ref=src, dst_ref=dst, send_sem=send, recv_sem=recv, device_id=where, device_id_type=MESH
    )


def away(step):
    return min(step[0], 4 - step[0]) + min(step[1], 4 - step[1])


STEPS = sorted([(y, x) for y in range(4) for x in range(4) if (y, x) != (0, 0)], key=lambda s: -away(s))


def peers(me):
    for dy, dx in STEPS:
        yield 4 * lax.rem(me // 4 + dy, 4) + lax.rem(lax.rem(me, 4) + dx, 4)


def to_peers(me, src_of, dst, send, recv):
    for g in peers(me):
        remote(src_of(g), dst, send, recv, {"ga": g}).start()


def kernel(
    psi, g_mask, fold, spread, energies, k_point, far_v, far_dv, far_tables,
    response, residual,
    v_local, dv, tables, raw, mask_rows, mask, level, solved, changes, potential, solved_rows, weights, wide_rows, panel, near, tmp, space, send_a, came_a, send_b, came_b, send_1, send_2,
    came_1, came_2, packed, product, share, shares, far_share, far_shares, source, vec, image, sums, sums_here, all_sums,
    in_sem, raw_sem, ring_send, ring_recv, a_sem, b_send, b_recv, s1, r1, s2, r2, c_send, c_recv, m_sem,
):
    me = lax.axis_index("ga")
    z = lax.axis_index("band")
    up, down = lax.rem(z + 1, 4), lax.rem(z + 3, 4)

    barrier = pltpu.get_barrier_semaphore()

    for g in peers(me):
        pl.semaphore_signal(barrier, inc=1, device_id={"ga": g}, device_id_type=MESH)
    for other in (up, down):
        pl.semaphore_signal(barrier, inc=1, device_id={"band": other}, device_id_type=MESH)

    def raw_copy(p):
        return pltpu.make_async_copy(psi.at[:, p], raw.at[p], raw_sem.at[p])

    def late_copy(n):
        src, dst = ((far_tables, tables), (far_v, v_local), (far_dv, dv))[n]
        return pltpu.make_async_copy(src, dst, in_sem.at[n])

    for p in (0, 2, 1, 3):
        raw_copy(p).start()
    for n in range(3):
        late_copy(n).start()
    fwd_hi, fwd_lo, back_hi, back_lo, up_hi, up_lo, down_hi, down_lo = (tables.at[n] for n in range(8))

    front = lax.broadcasted_iota(jnp.int32, (4, 2 * BOX), 1) < BOX
    top = lax.broadcasted_iota(jnp.int32, (8, 2 * BOX), 0) < 4
    for c in range(BOX // 2):
        both = g_mask[:, 2 * BOX * c : 2 * BOX * (c + 1)].astype(F32)
        turned = pltpu.roll(both, BOX, 1)
        for n, rows in ((2 * c, jnp.where(front, both, turned)), (2 * c + 1, jnp.where(front, turned, both))):
            for p in range(4):
                mask_rows[p, n : n + 1] = rows[p : p + 1]

    def spread_rows(first, second):
        return jnp.where(top, jnp.broadcast_to(first, (8, 2 * BOX)), jnp.broadcast_to(second, (8, 2 * BOX)))

    def pack_plane(u, carry):
        p = 2 * lax.rem(u, 2) + u // 2
        raw_copy(p).wait()

        def widen(m, c):
            wide_rows[pl.ds(pl.multiple_of(STEP * m, 8), BOX), :] = raw[p, m].astype(F32)
            return c

        lax.fori_loop(0, 64, widen, 0)

        def get(f):
            n = f % BOX
            return wide_rows[pl.ds(n, 64, stride=STEP), :] * mask_rows[p, n : n + 1]

        for r in range(ROWS):
            panel[0, p, r] = pack_row(get, r).astype(BF16)
        return carry

    lax.fori_loop(0, 2, pack_plane, 0)
    pl.semaphore_wait(barrier, 17)

    def ring(src_slot, dst_slot, p, where, n):
        return remote(
            panel.at[src_slot, p], panel.at[dst_slot, p], ring_send.at[n], ring_recv.at[dst_slot, p],
            {"band": where},
        )

    def ring_up(p):
        return ring(0, 3, p, up, p)

    def ring_down(p):
        return ring(0, 1, p, down, 4 + p)

    ring_up(0).start()
    ring_down(2).start()
    lax.fori_loop(2, 4, pack_plane, 0)
    ring_up(1).start()
    ring_down(3).start()
    ring_up(2).start()
    ring_down(0).start()
    ring_up(3).start()
    ring_down(1).start()

    for i in range(2):
        for k in range(2):
            for q in range(4):
                solved_rows[pl.ds(STEP * (8 * i + 4 * k + q), BOX), :] = raw[2 * k + i, STRIDE * q].astype(F32)
    for f in kept_freqs:
        n = f % BOX
        for i in range(2):
            rows = mask_rows[i, n : n + 1], mask_rows[2 + i, n : n + 1]
            mask[place_of[f], 8 * i : 8 * i + 8] = spread_rows(*rows)
        solved[place_of[f]] = solved_rows[pl.ds(n, 16, stride=STEP), :] * mask[place_of[f]]
    for n in range(3):
        late_copy(n).wait()
    forward_tile(solved, 0, fwd_hi[...], fwd_lo[...], near, tmp, put_pair(send_a, slice(0, 16), F32))

    mine = pl.ds(4 * me, 4)
    to_peers(me, lambda g: send_a.at[pl.ds(4 * g, 4)], came_a.at[mine], a_sem.at[0], a_sem.at[1])
    came_a[mine] = send_a[mine]

    def spread_field(n, carry):
        line = v_local[pl.ds(n, 1), :]
        potential[n] = spread_rows(line[:, : 2 * BOX], line[:, 2 * BOX :])
        for p in range(NPERT):
            line = dv[p, pl.ds(n, 1), :]
            changes[p, n] = spread_rows(line[:, : 2 * BOX], line[:, 2 * BOX :])
        return carry

    lax.fori_loop(0, BOX, spread_field, 0)

    factor = 0.5 * (2.0 * math.pi / cell_length) ** 2
    row = lax.broadcasted_iota(jnp.int32, (8, 2 * BOX), 0)
    third = lax.broadcasted_iota(jnp.int32, (8, 2 * BOX), 1) % BOX
    third = jnp.where(third < BOX // 2, third, third - BOX).astype(F32)
    for i in range(2):
        first = 4 * me + 2 * (row // 4) + i
        first = jnp.where(first < BOX // 2, first, first - BOX).astype(F32)
        still = factor * ((first + k_point[0]) ** 2 + (third + k_point[2]) ** 2)
        for q in range(4):
            still = jnp.where(row % 4 == q, still - energies[q], still)
        for f in kept_freqs:
            here = mask[place_of[f], 8 * i : 8 * i + 8]
            rise = factor * (float(f) + k_point[1]) * (float(f) + k_point[1])
            level[place_of[f], 8 * i : 8 * i + 8] = (still + rise) * here
            mask[place_of[f], 8 * i : 8 * i + 8] = here * (1.0 / BOX**3)

    def wait_all(src, dst, send, recv):
        return remote(src, dst, send, recv, {"ga": lax.rem(me + 1, 16)})

    every = pl.ds(0, 60)
    wait_all(send_a.at[every], came_a.at[every], a_sem.at[0], a_sem.at[1]).wait()

    turn_in(came_a, near)

    def keep(n, value):
        space[n, 0:8] = value[0]
        space[n, 8:16] = value[1]

    dft64(pair(near), ALL_SET, tmp, keep, 1)

    def each_change(p, carry):
        def load(n):
            d = changes[p, n]
            return (space[n, 0:8] * d, space[n, 8:16] * d)

        dft64(load, ALL_SET, tmp, put_pair(send_b.at[p], slice(0, 16), F32), -1)
        to_peers(
            me, lambda g: send_b.at[p, pl.ds(4 * g, 4)], came_b.at[p, mine], b_send.at[p], b_recv.at[p]
        )
        came_b[p, mine] = send_b[p, mine]
        return carry

    lax.fori_loop(0, NPERT, each_change, 0)

    def pass_on(p_up, p_down):
        ring(0, 3, p_up, up, p_up).wait_recv()
        first = ring(3, 2, p_up, up, 8 + p_up)
        first.start()
        ring(0, 1, p_down, down, 4 + p_down).wait_recv()
        second = ring(1, 2, p_down, down, 8 + p_down)
        second.start()

    pass_on(0, 2)
    pass_on(1, 3)

    def back(came, dst_add):
        def each(t, carry):
            dst_add(t)
            return carry

        lax.fori_loop(0, 3, each, 0)

    def source_tile(t):
        wait_all(send_b.at[t, every], came_b.at[t, every], b_send.at[t], b_recv.at[t]).wait()
        start = pl.multiple_of(16 * t, 16)
        a, b = back_tile(came_b.at[t], back_hi[...], back_lo[...], near, tmp)
        source[:, pl.ds(start, 8), :] = a * mask[:, 0:8, :]
        source[:, pl.ds(start + 8, 8), :] = b * mask[:, 8:16, :]

    back(came_b, source_tile)

    def send_share(n, src):
        to_peers(me, lambda g: src, shares.at[n, me], c_send.at[n], c_recv.at[n])

    def total_share(n):
        first = pl.ds(0, 15)
        wait_all(shares.at[n, first], shares.at[n, first], c_send.at[n], c_recv.at[n]).wait()
        total = shares[n, 0].astype(F32)
        for g in range(1, 16):
            total = total + shares[n, g].astype(F32)
        return total.astype(BF16)

    pack_values(source, packed)
    for p in range(2, 4):
        ring(0, 3, p, up, p).wait_recv()
    for p in range(2):
        ring(0, 1, p, down, 4 + p).wait_recv()
    early = correlate(packed, panel, fold[...], SLOTS[:3]).astype(BF16)
    share[0] = jnp.concatenate([early, jnp.zeros((24, 64), BF16)], axis=1)
    shares[0, me] = share[0]
    send_share(0, share.at[0])
    ring(3, 2, 0, up, 8).wait_recv()
    ring(1, 2, 2, down, 10).wait_recv()
    late = correlate(packed, panel, fold[...], SLOTS[3:], (0, 2))
    multiply(total_share(0)[:, :192], panel, spread, product, SLOTS[:3])
    ring(3, 2, 1, up, 9).wait_recv()
    ring(1, 2, 3, down, 11).wait_recv()
    late = late + correlate(packed, panel, fold[...], SLOTS[3:], (1, 3))
    far_share[...] = jnp.concatenate([late.astype(BF16), jnp.zeros((24, 64), BF16)], axis=1)
    far_shares[me] = far_share[...]
    to_peers(me, lambda g: far_share, far_shares.at[me], c_send.at[3], c_recv.at[3])

    def first_row(place, row):
        for t in range(3):
            rows = slice(16 * t, 16 * t + 16)
            vec[0, place, rows] = row[rows] * mask[place] - source[place, rows]

    first = pl.ds(0, 15)
    wait_all(far_shares.at[first], far_shares.at[first], c_send.at[3], c_recv.at[3]).wait()
    total = far_shares[0].astype(F32)
    for g in range(1, 16):
        total = total + far_shares[g].astype(F32)
    multiply(total.astype(BF16)[:, :64], panel, spread, product, SLOTS[3:], True)
    lay_out(product, first_row)

    lane = lax.broadcasted_iota(jnp.int32, (8, 2 * BOX), 1)
    mine3, most = pl.ds(3 * me, 3), pl.ds(0, 45)
    third = lax.broadcasted_iota(jnp.int32, (16, 2 * BOX), 1) % BOX
    third = jnp.where(third < BOX // 2, third, third - BOX)
    side = jnp.minimum(jnp.maximum(4.0 * k_point[2], -1.0), 1.0)
    edge = jnp.where(third == GCUT, 0.5 - 0.5 * side, jnp.where(third == -GCUT, 0.5 + 0.5 * side, 0.0))
    valid = jnp.where(jnp.abs(third) < GCUT, 1.0, edge)

    def apply(it, carry):
        def near_tile(t, c):
            natural_to_pair(vec.at[it], pl.multiple_of(16 * t, 16), near)
            dft64(load_kept(near), ALL_SET, tmp, put_pair(space, slice(0, 16), F32), 1)
            squeeze(space, send_1.at[it, t])
            to_peers(
                me, lambda g: send_1.at[it, t, pl.ds(3 * g, 3)], came_1.at[it, t, mine3],
                s1.at[it, t], r1.at[it, t],
            )
            came_1[it, t, mine3] = send_1[it, t, mine3]
            return c

        lax.fori_loop(0, 3, near_tile, 0)

        pack_values(vec.at[it], packed)
        n = it + 1
        share[n] = correlate(packed, panel, fold[...], SLOTS).astype(BF16)
        shares[n, me] = share[n]
        send_share(n, share.at[n])

        def space_tile(t, c):
            wait_all(send_1.at[it, t, most], came_1.at[it, t, most], s1.at[it, t], r1.at[it, t]).wait()
            turn_squeezed(came_1.at[it, t], near, valid)
            grid_lanes(near, up_hi[...], up_lo[...])

            weight = [jnp.zeros((8, 2 * BOX), F32)]

            def with_potential(k, value):
                v = potential[k]
                re, im = value[0] * v, value[1] * v
                near[k, 0:8] = re
                near[k, 8:16] = im
                weight[0] = weight[0] + (value[0] * re + value[1] * im)

            dft64(pair(near), ALL_SET, tmp, with_potential, 1)
            weights[t] = weight[0]
            dft64(pair(near), ALL_SET, tmp, put_pair(near, slice(0, 16), F32), -1)
            grid_lanes(near, down_hi[...], down_lo[...], valid)
            squeeze(near, send_2.at[it, t])
            to_peers(
                me, lambda g: send_2.at[it, t, pl.ds(3 * g, 3)], came_2.at[it, t, mine3],
                s2.at[it, t], r2.at[it, t],
            )
            came_2[it, t, mine3] = send_2[it, t, mine3]
            return c

        lax.fori_loop(0, 3, space_tile, 0)

        def with_level(place, row):
            for t in range(3):
                rows = slice(16 * t, 16 * t + 16)
                image[it, place, rows] = (
                    row[rows] * (shift_weight * mask[place])
                    + level[place] * vec[it, place, rows]
                )

        corr = total_share(n)

        @pl.when(it == 1)
        def _():
            def moments(place, totals):
                b, ab, w = vec[0, place], image[0, place], vec[1, place]
                lift = jnp.concatenate([level[place]] * 3, axis=0)
                return tuple(x + y for x, y in zip(totals, (b * b, b * ab, ab * ab, lift * w * w)))

            zero = jnp.zeros((48, 2 * BOX), F32)
            totals = lax.fori_loop(0, KEPT, moments, (zero,) * 4)
            own = jnp.zeros((8, 2 * BOX), F32)
            for m, total in enumerate(totals):
                line = jnp.sum(total, axis=1, keepdims=True) * (1.0 / BOX**3)
                for t in range(3):
                    both = line[16 * t : 16 * t + 8] + line[16 * t + 8 : 16 * t + 16]
                    if m == 3:
                        both = both + jnp.sum(weights[t], axis=1, keepdims=True) * (1.0 / BOX**6)
                    own = jnp.where(lane == 4 * t + m, jnp.broadcast_to(both, own.shape), own)
            own = own + pltpu.roll(own, 4, 0)
            sums[...] = own
            all_sums[me] = own
            to_peers(me, lambda g: sums, all_sums.at[me], m_sem.at[0], m_sem.at[1])
            square = corr.astype(F32)
            square = jnp.sum(square * square, axis=1, keepdims=True) * (shift_weight / BOX**6)
            rest = jnp.zeros((8, 2 * BOX), F32)
            for t in range(3):
                four = square[4 * t : 4 * t + 4] + square[12 + 4 * t : 16 + 4 * t]
                eight = jnp.concatenate([four, four], axis=0)
                rest = jnp.where(lane == 4 * t + 3, jnp.broadcast_to(eight, rest.shape), rest)
            sums_here[...] = rest

        multiply(corr, panel, spread, product, SLOTS)
        lay_out(product, with_level)

        def far_tile(t, c):
            wait_all(send_2.at[it, t, most], came_2.at[it, t, most], s2.at[it, t], r2.at[it, t]).wait()
            start = pl.multiple_of(16 * t, 16)
            turn_squeezed(came_2.at[it, t], near)

            def to_near(n, value):
                near[kept_place(n), 0:8] = value[0]
                near[kept_place(n), 8:16] = value[1]

            dft64(pair(near), KEPT_SET, tmp, to_near, -1)
            for n in range(KEPT):
                for half, value in zip((0, 8), pair_to_natural(near, n)):
                    rows = pl.ds(start + half, 8)
                    total = image[it, n, rows, :] + value * mask[n, half : half + 8]
                    image[it, n, rows, :] = total
                    vec[it + 1, n, rows, :] = total - SHIFT * vec[it, n, rows, :]
            return c

        lax.fori_loop(0, 3, far_tile, 0)
        return carry

    lax.fori_loop(0, 2, apply, 0)

    first = pl.ds(0, 15)
    wait_all(all_sums.at[first], all_sums.at[first], m_sem.at[0], m_sem.at[1]).wait()
    m0 = sums_here[...] + all_sums[0]
    for g in range(1, 16):
        m0 = m0 + all_sums[g]
    m1, m2, m3 = (pltpu.roll(m0, 2 * BOX - n, 1) for n in (1, 2, 3))
    step0 = m0 / m1
    fresh = m0 - 2.0 * step0 * m1 + step0 * step0 * m2
    u = 1.0 + fresh / m0 - step0 * SHIFT
    curve = u * u * m1 - 2.0 * u * step0 * (m2 - SHIFT * m1) + step0 * step0 * m3
    step1 = fresh / curve
    low_part, high_part = step0 + step1 * u, step1 * step0
    for t in range(3):
        a = jnp.broadcast_to(low_part[:, 4 * t : 4 * t + 1], (8, 2 * BOX))
        e = jnp.broadcast_to(high_part[:, 4 * t : 4 * t + 1], (8, 2 * BOX))
        for half in (0, 8):
            rows = slice(16 * t + half, 16 * t + half + 8)
            b, ab = vec[0, :, rows, :], image[0, :, rows, :]
            response[:, rows, :] = a * b - e * vec[1, :, rows, :]
            residual[:, rows, :] = b - a * ab + e * image[1, :, rows, :]

    for p in range(4):
        ring_up(p).wait_send()
        ring_down(p).wait_send()
    for p in range(2):
        ring(3, 2, p, up, 8 + p).wait_send()
    for p in range(2, 4):
        ring(1, 2, p, down, 8 + p).wait_send()


def run(*args):
    grid_f = pltpu.VMEM((BOX, 16, 2 * BOX), F32)
    three_f = pltpu.VMEM((3, BOX, 16, 2 * BOX), F32)
    six_b = pltpu.VMEM((2, 3, 48, 16, 2 * BOX), BF16)
    natural = (KEPT, 48, 2 * BOX)
    dma = pltpu.SemaphoreType.DMA
    return pl.pallas_call(
        kernel,
        out_shape=(shape(natural), shape(natural)),
        in_specs=[far] + [vmem] * 3 + [smem] * 2 + [far] * 3,
        out_specs=(vmem, vmem),
        scratch_shapes=[
            pltpu.VMEM((BOX, 4 * BOX), F32),
            pltpu.VMEM((NPERT, BOX, 4 * BOX), F32),
            pltpu.VMEM((8, 4 * BOX, 4 * BOX), BF16),
            pltpu.VMEM((4, 64, BOX, 2 * BOX), BF16),
            pltpu.VMEM((4, BOX, 2 * BOX), F32),
            pltpu.VMEM((KEPT, 16, 2 * BOX), F32),
            pltpu.VMEM((KEPT, 16, 2 * BOX), F32),
            pltpu.VMEM((KEPT, 16, 2 * BOX), F32),
            pltpu.VMEM((NPERT, BOX, 8, 2 * BOX), F32),
            pltpu.VMEM((BOX, 8, 2 * BOX), F32),
            pltpu.VMEM((16 * STEP, 2 * BOX), F32),
            pltpu.VMEM((3, 8, 2 * BOX), F32),
            pltpu.VMEM((64 * STEP, 2 * BOX), F32),
            pltpu.VMEM((4, 4, ROWS, 64, 2 * BOX), BF16),
            grid_f, grid_f, grid_f,
            grid_f, grid_f, three_f, three_f, six_b, six_b, six_b, six_b,
            pltpu.VMEM((ROWS, 96, 2 * BOX), BF16),
            pltpu.VMEM((ROWS, 48, 2 * BOX), F32),
            pltpu.VMEM((3, 24, 256), BF16),
            pltpu.VMEM((3, 16, 24, 256), BF16),
            pltpu.VMEM((24, 128), BF16),
            pltpu.VMEM((16, 24, 128), BF16),
            pltpu.VMEM(natural, F32),
            pltpu.VMEM((3, *natural), F32),
            pltpu.VMEM((2, *natural), F32),
            pltpu.VMEM((8, 2 * BOX), F32),
            pltpu.VMEM((8, 2 * BOX), F32),
            pltpu.VMEM((16, 8, 2 * BOX), F32),
            dma((3,)), dma((4,)), dma((12,)), dma((4, 4)), dma((2,)), dma((3,)), dma((3,)),
            dma((2, 3)), dma((2, 3)), dma((2, 3)), dma((2, 3)), dma((4,)), dma((4,)), dma((2,)),
        ],
        compiler_params=pltpu.CompilerParams(
            vmem_limit_bytes=VMEM_LIMIT, collective_id=0, has_side_effects=True
        ),
    )(*args)


def place_body(response, residual, first, second, stage, buffer, in_sem, sem):
    pairs = ((0, response, first), (1, residual, second))

    def come(w, src, t):
        return pltpu.make_async_copy(
            src.at[:, pl.ds(16 * t, 16)], stage.at[w, t, pl.ds(0, KEPT), pl.ds(0, 16)], in_sem.at[w, t]
        )

    def leave(w, out, t, q):
        part = pl.ds(12 * q + 4 * t, 4)
        return pltpu.make_async_copy(buffer.at[w, part], out.at[part], sem.at[w, t, q])

    for t in range(NPERT):
        for w, src, _ in pairs:
            come(w, src, t).start()
    for t in range(NPERT):
        for w, src, out in pairs:
            come(w, src, t).wait()
            flat = stage.at[w, t].reshape(48 * 24, 2 * BOX)
            for q in range(4):
                for p in range(4):
                    row = 8 * (p % 2) + 4 * (p // 2) + q
                    to = 12 * q + 4 * t + p
                    buffer[w, to, 0 : GCUT + 1] = flat[pl.ds(row, GCUT + 1, stride=24), :]
                    buffer[w, to, GCUT + 1 : BOX - GCUT] = jnp.zeros((BOX - KEPT, 2 * BOX), F32)
                    buffer[w, to, BOX - GCUT :] = flat[pl.ds(row + 24 * (GCUT + 1), GCUT, stride=24), :]
                leave(w, out, t, q).start()
    for t in range(NPERT):
        for w, _, out in pairs:
            for q in range(4):
                leave(w, out, t, q).wait()


def place(*values):
    out = shape((48, BOX, 2 * BOX))
    outs = pl.pallas_call(
        place_body,
        out_shape=(out, out),
        in_specs=[pl.BlockSpec(memory_space=pl.ANY)] * 2,
        out_specs=(pl.BlockSpec(memory_space=pl.ANY),) * 2,
        scratch_shapes=[
            pltpu.VMEM((2, NPERT, 48, 24, 2 * BOX), F32),
            pltpu.VMEM((2, 48, BOX, 2 * BOX), F32),
            pltpu.SemaphoreType.DMA((2, NPERT)),
            pltpu.SemaphoreType.DMA((2, NPERT, 4)),
        ],
        compiler_params=pltpu.CompilerParams(vmem_limit_bytes=VMEM_LIMIT),
    )(*values)
    return tuple(v.reshape(4, NPERT, 4, BOX, 2 * BOX) for v in outs)


def on_device(psi_occ, energies, k_point, g_mask, v_local, dv):
    response, residual = run(
        psi_occ, g_mask, jnp.asarray(fold_table(), BF16), jnp.asarray(spread_table(), BF16),
        energies, k_point, v_local, dv, jnp.stack(lane_tables()),
    )

    return place(response, residual)


def solution(mesh):
    placed = (
        P(("pool", "band"), "ga", None, None),
        P(("pool", "band")),
        P("pool"),
        P(("pool", "ga"), None),
        P(None, "ga"),
        P(None, None, "ga"),
    )
    return jax.shard_map(
        on_device,
        mesh=mesh,
        in_specs=placed,
        out_specs=(
            P(("pool", "band"), None, "ga", None, None),
            P(("pool", "band"), None, "ga", None, None),
        ),
        check_vma=False,
    )
```
